32 devices in a mesh: blk: 4 (over x, core), tp: 8 (over z, y).
Axes of the slice: x: 2, y: 2, z: 4, core: 2. Of those that a mesh axis runs over, the one named last changes fastest.
Arguments:
- residual_in: bfloat16 [2048, 5120], P('blk'), may hold values from -6 to 6
- norm_gain: bfloat16 [5120], replicated, may hold values from 0.099609375 to 1.8984375
- w_query: bfloat16 [5120, 4096], P(('blk', 'tp')), may hold values from -0.5 to 0.5
- w_key_value: bfloat16 [5120, 2048], P(('blk', 'tp')), may hold values from -0.5 to 0.5
- query_bias: bfloat16 [4096], replicated, may hold values from -3 to 3
- key_value_bias: bfloat16 [2048], replicated, may hold values from -3 to 3
- w_output: bfloat16 [4096, 5120], P(None, ('blk', 'tp')), may hold values from -0.09375 to 0.09375
- device_map: int32 [32], replicated, may hold values from 0 to 31, each once
- positions: int32 [2048], P('blk'), may hold values from 0 to 4094, as said below
- segments: int32 [2048], P('blk'), may hold values from 0 to 1, as said below
Outputs:
- output: bfloat16 [2048, 5120], P('blk', 'tp')
The draws below stay inside these ranges and needn't reach their ends.
Inputs may be any that keep to these rules, and one draw needn't show every extreme that they name: `segments`: ids never fall; both ids 0 and 1 occur; the shorter prompt holds a quarter of 512 up to 511 tokens. `positions`: a token's index within its prompt plus an offset shared by the whole prompt; the longer prompt's last token stands at 4094. `device_map`: each of 0 to 31 once.
All inputs are finite; a program needn't handle non-finite values.
Results may differ from the reference program's by a relative error of at most 0.012.
Values may be sent and summed in bfloat16 or wider, within the bound.
A program may use at most 128 MiB of HBM per device.

```python
import jax
import jax.numpy as jnp
from jax import lax

D = 5120
HEADS = 32
KVH = 8
HD = 128
TOK_DEV = 512
LEN = 2048
QW = 4096
KVW = 2048
TRAINER_ROWS = 160
DEVICES = 32


def weight_pair(key):
    base_key = jax.random.fold_in(key, 11)
    query_key, pair_key = jax.random.split(base_key, 2)
    query_raw = jnp.clip(jax.random.normal(query_key, (D, KVH, HEADS // KVH, HD), jnp.float32), -6.0, 6.0)
    pairs_raw = jnp.clip(jax.random.normal(pair_key, (D, KVH, 2, HD), jnp.float32), -6.0, 6.0)
    fan_scale = D ** (-0.5)
    query_scaled = jnp.clip(query_raw.reshape(D, HEADS * HD) * fan_scale, -0.5, 0.5)
    pairs_scaled = jnp.clip(pairs_raw.reshape(D, 2 * KVH * HD) * fan_scale, -0.5, 0.5)
    return (query_scaled.astype(jnp.bfloat16), pairs_scaled.astype(jnp.bfloat16))


def prompt_layout(key):
    base_key = jax.random.fold_in(key, 23)
    short_key, order_key, offset_key = jax.random.split(base_key, 3)
    short_len = jax.random.randint(short_key, (), TOK_DEV // 4, TOK_DEV)
    first_short = jax.random.randint(order_key, (), 0, 2)
    boundary = jnp.where(first_short == 1, short_len, LEN - short_len)
    index_all = jnp.arange(LEN, dtype=jnp.int32)
    segment_ids = (index_all >= boundary).astype(jnp.int32)
    short_offset = jax.random.randint(offset_key, (), 0, 2048)
    long_offset = short_len + 2047
    offset_zero = jnp.where(first_short == 1, short_offset, long_offset)
    offset_one = jnp.where(first_short == 1, long_offset, short_offset)
    starts = jnp.where(segment_ids == 1, boundary, 0)
    shifted = jnp.where(segment_ids == 1, offset_one, offset_zero)
    return (segment_ids, (index_all - starts + shifted).astype(jnp.int32))


def draw_w_query(key, part):
    return weight_pair(key)[0]


def draw_w_key_value(key, part):
    return weight_pair(key)[1]


def draw_segments(key, part):
    return prompt_layout(key)[0]


def draw_positions(key, part):
    return prompt_layout(key)[1]


def level_of(own_key, extent, cuts, low, high):
    level, own = 1.0, jax.random.fold_in(own_key, 6)
    for position, shards_of in cuts:
        steps = jnp.exp(jax.random.uniform(jax.random.fold_in(own, position), (shards_of,), jnp.float32, low / len(cuts), high / len(cuts)))
        level = level * jnp.repeat(steps, extent[position] // shards_of).reshape([-1 if axis == position else 1 for axis in range(len(extent))])
    return level


def noise(key, extent, scale, limit, cuts=(), held_as=jnp.bfloat16):
    result = scale * jax.random.normal(key, extent, jnp.float32)
    if cuts:
        result = result * level_of(key, extent, cuts, -0.22, 0.18)
    return jnp.clip(result, -limit, limit).astype(held_as)


def setup_inputs(seed: int = 0) -> dict:
    splits = jax.random.split(jax.random.key(seed), 11)
    residual_in = noise(splits[0], (LEN, D), 1.0, 6.0, ((0, 4),))
    norm_gain = jnp.clip(1.0 + 0.18 * jax.random.normal(splits[1], (D,), jnp.float32), 0.099609375, 1.8984375).astype(jnp.bfloat16)
    w_query = draw_w_query(jax.random.fold_in(splits[10], 71), 0)
    w_key_value = draw_w_key_value(jax.random.fold_in(splits[10], 71), 0)
    query_bias = noise(splits[4], (QW,), 0.5, 3.0)
    key_value_bias = noise(splits[5], (KVW,), 0.5, 3.0)
    w_output = noise(splits[6], (QW, D), QW ** -0.5, 0.09375, ((1, 32),))
    device_map = jax.random.permutation(splits[7], DEVICES).astype(jnp.int32)
    positions = draw_positions(jax.random.fold_in(splits[10], 71), 0)
    segments = draw_segments(jax.random.fold_in(splits[10], 71), 0)
    return {"residual_in": residual_in, "norm_gain": norm_gain, "w_query": w_query, "w_key_value": w_key_value, "query_bias": query_bias, "key_value_bias": key_value_bias, "w_output": w_output, "device_map": device_map, "positions": positions, "segments": segments}


NORM_FLOOR = 0.0625
ROPE_BASE = 1000000.0
NEGATIVE_FILL = -1e+30

def rope_tables(positions, head_width):
    half_width = head_width // 2
    frequency = ROPE_BASE ** (-(jnp.arange(half_width, dtype=jnp.float32) * 2.0) / head_width)
    angles = positions.astype(jnp.float32)[:, None] * frequency[None, :]
    angles = jnp.concatenate([angles, angles], axis=1)
    return (jnp.cos(angles), jnp.sin(angles))

def rotate(values, cosine_table, sine_table):
    half_width = values.shape[-1] // 2
    turned = jnp.concatenate([-values[..., half_width:], values[..., :half_width]], axis=-1)
    return values * cosine_table[:, None, :] + turned * sine_table[:, None, :]

def reference(residual_in, norm_gain, w_query, w_key_value, query_bias, key_value_bias, w_output, device_map, positions, segments):
    floats = residual_in.astype(jnp.float32)
    square = jnp.maximum(lax.optimization_barrier(jnp.mean(floats * floats, axis=1, keepdims=True)), NORM_FLOOR)
    normed = (floats * lax.rsqrt(square) * norm_gain.astype(jnp.float32)).astype(jnp.bfloat16)
    ordered = jnp.take(normed.reshape(LEN, DEVICES, TRAINER_ROWS), device_map, axis=1).reshape(LEN, D)
    queries = jnp.dot(ordered, w_query, preferred_element_type=jnp.float32) + query_bias.astype(jnp.float32)
    key_value = jnp.dot(ordered, w_key_value, preferred_element_type=jnp.float32) + key_value_bias.astype(jnp.float32)
    cosine_table, sine_table = rope_tables(positions, HD)
    query_rot = rotate(queries.reshape(LEN, HEADS, HD), cosine_table, sine_table).astype(jnp.bfloat16)
    paired = key_value.reshape(LEN, KVH, 2, HD)
    key_rot = rotate(paired[:, :, 0, :], cosine_table, sine_table).astype(jnp.bfloat16)
    values = paired[:, :, 1, :].astype(jnp.bfloat16)
    per_group = HEADS // KVH
    query_rows = min(512, LEN)
    attend_scale = HD ** (-0.5)
    key_index = jnp.arange(LEN, dtype=jnp.int32)

    def one_block(block_number):
        block_start = (block_number * query_rows).astype(jnp.int32)
        query_block = lax.dynamic_slice_in_dim(query_rot, block_start, query_rows, 0)
        query_segment = lax.dynamic_slice_in_dim(segments, block_start, query_rows, 0)
        row_index = block_start + jnp.arange(query_rows, dtype=jnp.int32)
        visible = (key_index[None, :] <= row_index[:, None]) & (segments[None, :] == query_segment[:, None])

        def one_group(group_number):
            group_start = (group_number * per_group).astype(jnp.int32)
            query_group = lax.dynamic_slice_in_dim(query_block, group_start, per_group, 1).astype(jnp.float32)
            key_group = lax.dynamic_index_in_dim(key_rot, group_number, 1, keepdims=False).astype(jnp.float32)
            value_group = lax.dynamic_index_in_dim(values, group_number, 1, keepdims=False).astype(jnp.float32)
            scores = jnp.einsum('qhd,kd->hqk', query_group, key_group, precision=lax.Precision.HIGHEST) * attend_scale
            masked = jnp.where(visible[None], scores, NEGATIVE_FILL)
            row_peak = lax.optimization_barrier(jnp.max(masked, axis=2, keepdims=True))
            raw_weights = jnp.where(visible[None], jnp.exp(masked - row_peak), 0.0)
            weights = lax.optimization_barrier(raw_weights.astype(jnp.bfloat16)).astype(jnp.float32)
            context = jnp.einsum('hqk,kd->hqd', weights, value_group, precision=lax.Precision.HIGHEST)
            context = context / lax.optimization_barrier(jnp.sum(raw_weights, axis=2, keepdims=True))
            return context.astype(jnp.bfloat16)
        grouped = lax.map(one_group, jnp.arange(KVH, dtype=jnp.int32))
        return grouped.transpose(2, 0, 1, 3).reshape(query_rows, QW)
    blocks_out = lax.map(one_block, jnp.arange(LEN // query_rows, dtype=jnp.int32))
    context = blocks_out.reshape(LEN, QW)
    mixed = jnp.dot(context, w_output, preferred_element_type=jnp.float32)
    return (residual_in.astype(jnp.float32) + mixed).astype(jnp.bfloat16)
```

```python
import functools

import jax
import jax.numpy as jnp
import numpy as np
from jax import lax
from jax.experimental import pallas as pl
from jax.experimental.pallas import tpu as pltpu
from jax.sharding import PartitionSpec as P

D = 5120
KVH = 8
HD = 128


NORM_FLOOR = 0.0625
ROPE_BASE = 1000000.0
NEGATIVE_FILL = -1e30


def for_sending(x):
    return jax.tree.map(lambda a: a.astype(jnp.bfloat16) if a.dtype == jnp.float32 else a, x)


def from_partner(block, axis, bit):
    count = lax.axis_size(axis)
    route = []
    for low in range(count):
        high = low | 1 << bit
        if high != low and high < count:
            route += [(low, high), (high, low)]
    return lax.ppermute(block, axis, route)


def rope_tables(positions, head_width):
    half_width = head_width // 2
    frequency = ROPE_BASE ** (-(jnp.arange(half_width, dtype=jnp.float32) * 2.0) / head_width)
    angles = positions.astype(jnp.float32)[:, None] * frequency[None, :]
    angles = jnp.concatenate([angles, angles], axis=1)
    return (jnp.cos(angles), jnp.sin(angles))


def rotate(values, cosine_table, sine_table):
    half_width = values.shape[-1] // 2
    turned = jnp.concatenate([-values[..., half_width:], values[..., :half_width]], axis=-1)
    return values * cosine_table[:, None, :] + turned * sine_table[:, None, :]


def join_pair(mine_cols, partner, is_lower):
    return jnp.where(
        is_lower,
        jnp.concatenate([mine_cols, partner], axis=1),
        jnp.concatenate([partner, mine_cols], axis=1),
    )


def per_device(
    residual_in,
    norm_gain,
    w_query,
    w_key_value,
    query_bias,
    key_value_bias,
    w_output,
    device_map,
    positions,
    segments,
):
    tp_count = lax.axis_size("tp")
    tp_index = lax.axis_index("tp")
    blk_index = lax.axis_index("blk")
    local_tokens = residual_in.shape[0]
    shard_rows = w_query.shape[0]
    kv_group = tp_count // KVH
    floats = residual_in.astype(jnp.float32)
    square = jnp.maximum(jnp.mean(floats * floats, axis=1, keepdims=True), NORM_FLOOR)
    normed = (floats * lax.rsqrt(square) * norm_gain.astype(jnp.float32)).astype(jnp.bfloat16)
    ordered = jnp.take(
        normed.reshape(local_tokens, device_map.shape[0], shard_rows), device_map, axis=1
    ).reshape(local_tokens, D)
    moved_query, moved_pairs = (
        lax.all_to_all(w_query, "tp", split_axis=1, concat_axis=0, tiled=True),
        lax.all_to_all(w_key_value, "tp", split_axis=1, concat_axis=0, tiled=True),
    )
    for bit_level in range(kv_group.bit_length() - 1):
        partner = from_partner(for_sending(moved_pairs), "tp", bit_level).astype(moved_pairs.dtype)
        moved_pairs = join_pair(moved_pairs, partner, tp_index >> bit_level & 1 == 0)
    queries = jnp.dot(
        ordered,
        lax.all_gather(moved_query, "blk", axis=0, tiled=True),
        preferred_element_type=jnp.float32,
    )
    key_value = jnp.dot(
        ordered,
        lax.all_gather(moved_pairs, "blk", axis=0, tiled=True),
        preferred_element_type=jnp.float32,
    )
    query_width = queries.shape[1]
    heads_here = query_width // HD
    kv_head = tp_index // kv_group
    queries = queries + lax.dynamic_slice_in_dim(
        query_bias, tp_index * query_width, query_width
    ).astype(jnp.float32)
    key_value = key_value + lax.dynamic_slice_in_dim(
        key_value_bias, kv_head * 2 * HD, 2 * HD
    ).astype(jnp.float32)
    cosine_table, sine_table = rope_tables(positions, HD)
    query_rot = rotate(
        queries.reshape(local_tokens, heads_here, HD), cosine_table, sine_table
    ).astype(jnp.bfloat16)
    key_rot = rotate(key_value[:, None, :HD], cosine_table, sine_table)[:, 0, :].astype(
        jnp.bfloat16
    )
    values = key_value[:, HD:].astype(jnp.bfloat16)
    attend_scale = HD ** (-0.5)
    row_index = blk_index * local_tokens + jnp.arange(local_tokens, dtype=jnp.int32)
    initial = (
        jnp.full((heads_here, local_tokens), NEGATIVE_FILL, jnp.float32),
        jnp.zeros((heads_here, local_tokens), jnp.float32),
        jnp.zeros((heads_here, local_tokens, HD), jnp.float32),
    )
    key_piece = lax.all_gather(key_rot, "blk", axis=0, tiled=True)
    value_piece = lax.all_gather(values, "blk", axis=0, tiled=True)
    segment_piece = lax.all_gather(segments, "blk", axis=0, tiled=True)
    piece_rows = key_piece.shape[0]
    key_block_rows = 512

    def one_block(block_number, state_now):
        run_peak, run_mass, context = state_now
        block_start = block_number * key_block_rows
        key_block = lax.dynamic_slice_in_dim(key_piece, block_start, key_block_rows, 0)
        value_block = lax.dynamic_slice_in_dim(value_piece, block_start, key_block_rows, 0)
        segment_block = lax.dynamic_slice_in_dim(segment_piece, block_start, key_block_rows, 0)
        scores = (
            jnp.einsum("qhd,kd->hqk", query_rot, key_block, preferred_element_type=jnp.float32)
            * attend_scale
        )
        key_index = block_start + jnp.arange(key_block_rows, dtype=jnp.int32)
        visible = (key_index[None, :] <= row_index[:, None]) & (
            segment_block[None, :] == segments[:, None]
        )
        masked = jnp.where(visible[None], scores, NEGATIVE_FILL)
        new_peak = jnp.maximum(run_peak, jnp.max(masked, axis=2))
        factor = jnp.exp(run_peak - new_peak)
        raw_weights = jnp.where(visible[None], jnp.exp(masked - new_peak[:, :, None]), 0.0)
        run_mass = run_mass * factor + jnp.sum(raw_weights, axis=2)
        context = context * factor[:, :, None] + jnp.einsum(
            "hqk,kd->hqd",
            raw_weights.astype(jnp.bfloat16),
            value_block,
            preferred_element_type=jnp.float32,
        )
        return (new_peak, run_mass, context)

    run_peak, run_mass, context = lax.fori_loop(0, piece_rows // key_block_rows, one_block, initial)
    context_flat = (
        (context / run_mass[:, :, None])
        .transpose(1, 0, 2)
        .reshape(local_tokens, query_width)
        .astype(jnp.bfloat16)
    )
    width_out = D // tp_count
    moved_out = lax.all_to_all(w_output, "tp", split_axis=0, concat_axis=1, tiled=True)
    row_terms = jnp.dot(
        context_flat,
        lax.all_gather(moved_out, "blk", axis=1, tiled=True),
        preferred_element_type=jnp.float32,
    )
    summed = lax.psum_scatter(
        row_terms.astype(jnp.bfloat16), "tp", scatter_dimension=1, tiled=True
    ).astype(jnp.float32)
    residual_part = lax.dynamic_slice_in_dim(residual_in, tp_index * width_out, width_out, 1)
    return (residual_part.astype(jnp.float32) + summed).astype(jnp.bfloat16)


MESH = pl.DeviceIdType.MESH
BF = jnp.bfloat16
F32 = jnp.float32


def flip(i, mask):
    out = i
    for bit in range(mask.bit_length()):
        if mask >> bit & 1:
            out = out + (1 << bit) * (1 - 2 * ((i // (1 << bit)) % 2))
    return out


def fused_kernel(nb, nt, dm_ref, x_hbm, wq_hbm, wkv_hbm, gain_ref, bq_ref, bkv_ref, wo_hbm, inv_ref,
                 pos_ref, seg_ref, out_ref, x_ref, xo, gq, gkv, wo, kv_all, seg_all, qacc,
                 kvacc, qrot, ctx_all, oacc, gain32, bq32, bkv32, cos_t, sin_t, segq_ref,
                 x_sem, loc_sem, kv1s, kv1r, kvxs, kvxr, kvcs, kvcr, q1s, q1r, qxs, qxr, qcs, qcr,
                 w1s, w1r, wxs, wxr, wcs, wcr, es, er, gs, gr, azs, azr, ays, ayr, wrel, rr, r2s):
    b = lax.axis_index("blk")
    t = lax.axis_index("tp")
    n_tok, width = x_ref.shape
    rows = wq_hbm.shape[0]
    qc, kc = gq.shape[2], gkv.shape[2]
    oc = wo.shape[1]
    bx, bc = flip(b, 2), flip(b, 1)

    barrier = pltpu.get_barrier_semaphore()
    peers = [(b, flip(t, k)) for k in range(1, nt)] + [(flip(b, k), t) for k in range(1, nb)]
    for peer in peers:
        pl.semaphore_signal(barrier, inc=1, device_id=peer, device_id_type=MESH)
    x_in = pltpu.make_async_copy(x_hbm, x_ref, x_sem)
    x_in.start()
    gain32[...] = gain_ref[...].astype(F32)
    bq32[...] = bq_ref[...].astype(F32)
    bkv32[...] = bkv_ref[...].astype(F32)
    pl.semaphore_wait(barrier, len(peers))

    def remote(src, dst, ss, rs, dev):
        return pltpu.make_async_remote_copy(src_ref=src, dst_ref=dst, send_sem=ss, recv_sem=rs,
                                            device_id=dev, device_id_type=MESH)

    def slot(bb, k):
        return bb * nt + flip(t, k)

    def stage_one(hbm, buf, width, k, ss, rs, local):
        cols = pl.ds(pl.multiple_of(flip(t, k) * width, 128), width)
        mine = buf.at[b * nt + t]
        if k == 0:
            return pltpu.make_async_copy(hbm.at[:, cols], mine, local)
        return remote(hbm.at[:, cols], mine, ss.at[k], rs.at[k], (b, flip(t, k)))

    def stage_one_in(buf, hbm, width, k, ss, rs, local):
        if k == 0:
            return stage_one(hbm, buf, width, 0, ss, rs, local)
        piece = buf.at[slot(b, k)]
        return remote(piece, piece, ss.at[k], rs.at[k], (b, flip(t, k)))

    def forward(buf, bb, k, ss, rs, i, dev):
        piece = buf.at[slot(bb, k)]
        return remote(piece, piece, ss.at[i], rs.at[i], dev)

    kv_set = (wkv_hbm, gkv, kc, kv1s, kv1r, kvxs, kvxr, kvcs, kvcr, loc_sem.at[0])
    q_set = (wq_hbm, gq, qc, q1s, q1r, qxs, qxr, qcs, qcr, loc_sem.at[1])

    order = [0] + sorted(range(1, nt), key=lambda k: (k * 5 + 4) % nt)

    def start_one(ws):
        hbm, buf, width, s1, r1, xs, xr, cs, cr, loc = ws
        for k in order:
            stage_one(hbm, buf, width, k, s1, r1, loc).start()

    def gather_step(ws, i):
        k = order[i]
        hbm, buf, width, s1, r1, xs, xr, cs, cr, loc = ws
        arrived = stage_one_in(buf, hbm, width, k, s1, r1, loc)
        if k == 0:
            arrived.wait()
        else:
            arrived.wait_recv()
        forward(buf, b, k, xs, xr, k, (bx, t)).start()
        forward(buf, b, k, cs, cr, k, (bc, t)).start()

    def gather_cross(ws, i):
        k = order[i]
        hbm, buf, width, s1, r1, xs, xr, cs, cr, loc = ws
        forward(buf, bx, k, xs, xr, k, (bx, t)).wait_recv()
        forward(buf, bx, k, cs, cr, nt + k, (bc, t)).start()

    def gather_last(ws, i):
        k = order[i]
        hbm, buf, width, s1, r1, xs, xr, cs, cr, loc = ws
        forward(buf, bc, k, cs, cr, k, (bc, t)).wait_recv()
        forward(buf, flip(b, 3), k, cs, cr, nt + k, (bc, t)).wait_recv()

    def gather_sent(ws):
        hbm, buf, width, s1, r1, xs, xr, cs, cr, loc = ws
        for k in range(nt):
            if k:
                stage_one(hbm, buf, width, k, s1, r1, loc).wait_send()
            forward(buf, b, k, xs, xr, k, (bx, t)).wait_send()
            forward(buf, b, k, cs, cr, k, (bc, t)).wait_send()
            forward(buf, bx, k, cs, cr, nt + k, (bc, t)).wait_send()

    def multiply(buf, acc, i):
        k = order[i]

        def one(j, _):
            s = slot(j, k)
            acc[...] += jnp.dot(xo[dm_ref[s]], buf[s], preferred_element_type=F32)
            return 0
        lax.fori_loop(0, nb, one, 0)

    start_one(kv_set)
    start_one(q_set)

    x_in.wait()
    tile = n_tok // nt

    def norm_tile(i):
        toks = slice(i * tile, (i + 1) * tile)
        v = x_ref[toks, :].astype(F32)
        scale = lax.rsqrt(jnp.maximum(jnp.mean(v * v, axis=1, keepdims=True), NORM_FLOOR))

        def spread(g, _):
            per = 4 * rows // 128
            gain = jnp.concatenate([gain32[pl.ds(g * per + i, 1), :] for i in range(per)], axis=1)
            u = x_ref[toks, pl.ds(pl.multiple_of(g * 4 * rows, 128), 4 * rows)].astype(F32)
            u = (u * scale * gain).astype(BF)
            for i in range(4):
                xo[g * 4 + i, toks, :] = u[:, i * rows:(i + 1) * rows]
            return 0

        lax.fori_loop(0, nb * nt // 4, spread, 0)

    def tables():
        pos = jnp.broadcast_to(pos_ref[...].astype(F32), (HD, n_tok)).T
        angles = pos * inv_ref[...]
        cos_t[...] = jnp.cos(angles)
        sign = jnp.where(lax.broadcasted_iota(jnp.int32, (1, HD), 1) < HD // 2, -1.0, 1.0)
        sin_t[...] = jnp.sin(angles) * sign
        segq_ref[...] = jnp.broadcast_to(seg_ref[...].astype(F32), (HD, n_tok)).T[:, :1].astype(jnp.int32)

    for k in range(nt):
        norm_tile(k)
        gather_step(kv_set, k)
        if k:
            gather_cross(kv_set, k - 1)
    tables()
    gather_cross(kv_set, nt - 1)

    for e in range(2):
        kvacc[:, e * HD:(e + 1) * HD] = jnp.broadcast_to(bkv32[pl.ds(t * 2 + e, 1), :], (n_tok, HD))
    for k in range(nt):
        gather_last(kv_set, k)
        multiply(gkv, kvacc, k)
        if k % 2:
            gather_step(q_set, k // 2)
            if k > 1:
                gather_cross(q_set, k // 2 - 1)

    def rope(u):
        return u * cos_t[...] + pltpu.roll(u, HD // 2, 1) * sin_t[...]

    kv_all[b, :, :HD] = rope(kvacc[:, :HD]).astype(BF)
    kv_all[b, :, HD:] = kvacc[:, HD:].astype(BF)
    seg_all[b] = seg_ref[...]

    for d in range(1, nb):
        @pl.when(b + d < nb)
        def _():
            dst = (b + d, t)
            remote(kv_all.at[b], kv_all.at[b], es.at[d], er.at[d], dst).start()
            remote(seg_all.at[b], seg_all.at[b], gs.at[d], gr.at[d], dst).start()

    for e in range(qc // HD):
        qacc[:, e * HD:(e + 1) * HD] = jnp.broadcast_to(
            bq32[pl.ds(t * (qc // HD) + e, 1), :], (n_tok, HD))
    flat, flat_x = b * nt + t, bx * nt + t
    t_dst, k_mine = flat // nb, flat % nb
    t_via, k_via = flat_x // nb, flat_x % nb
    prim = (t * nb) // nt
    k_own = t - (t * nb - prim * nt)
    half = nt // 2

    def wpiece(k, ch):
        return wo.at[ch, pl.ds(pl.multiple_of(k * rows, 16), rows), :]

    def wsrc(ch):
        return wo_hbm.at[:, pl.ds(ch * qc, qc)]

    def straight(ch):
        return remote(wsrc(ch), wpiece(k_mine, ch), w1s.at[ch], w1r.at[k_mine, ch], (b, t_dst))

    def to_relay(i):
        return remote(wsrc(half + i), wrel.at[i], w1s.at[half + i], rr.at[i], (bx, t))

    def from_relay(i):
        return remote(wrel.at[i], wpiece(k_via, half + i), r2s.at[i], w1r.at[k_via, half + i], (b, t_via))

    def wfwd(k, ch, ss, rs, dev):
        return remote(wpiece(k, ch), wpiece(k, ch), ss.at[k, ch], rs.at[k, ch], dev)

    def w_start():
        for i in range(half):
            to_relay(i).start()

        @pl.when(t_dst != t)
        def _():
            for ch in range(half):
                straight(ch).start()

        @pl.when(t_dst == t)
        def _():
            for ch in range(half):
                pltpu.make_async_copy(wsrc(ch), wpiece(k_mine, ch), w1s.at[ch]).start()

    def w_relay():
        for i in range(half):
            to_relay(i).wait_recv()

            @pl.when(t_via != t)
            def _():
                from_relay(i).start()

            @pl.when(t_via == t)
            def _():
                pltpu.make_async_copy(wrel.at[i], wpiece(k_via, half + i), r2s.at[i]).start()

    def w_direct(i, k):
        for role, where in ((0, prim), (1, flip(prim, 2))):
            ch = role * half + i

            @pl.when((b == where) & (k != k_own))
            def _():
                src = (b, t * nb + k - prim * nt)
                remote(wpiece(k, ch), wpiece(k, ch), w1s.at[ch], w1r.at[k, ch], src).wait_recv()

            @pl.when((b == where) & (k == k_own))
            def _():
                if role == 0:
                    pltpu.make_async_copy(wsrc(ch), wpiece(k, ch), w1s.at[ch]).wait()
                else:
                    pltpu.make_async_copy(wrel.at[i], wpiece(k, ch), r2s.at[i]).wait()

            @pl.when(b == where)
            def _():
                wfwd(k, ch, wxs, wxr, (bx, t)).start()
                wfwd(k, ch, wcs, wcr, (bc, t)).start()

    def w_crossed(i, k):
        for role, where in ((0, prim), (1, flip(prim, 2))):
            ch = (1 - role) * half + i

            @pl.when(b == where)
            def _():
                wfwd(k, ch, wxs, wxr, (bx, t)).wait_recv()
                wfwd(k, ch, wcs, wcr, (bc, t)).start()

    w_start()
    first = nt // 2
    for k in range(first, nt + 2):
        if k < nt:
            gather_step(q_set, k)
        if k - 1 < nt:
            gather_cross(q_set, k - 1)
        done = range(0, first - 1) if k == first else (k - 2,)
        for e in done:
            gather_last(q_set, e)
            multiply(gq, qacc, e)

    w_relay()

    for h in range(qc // HD):
        cols = slice(h * HD, (h + 1) * HD)
        qrot[:, cols] = rope(qacc[:, cols]).astype(BF)

    for d in range(1, nb):
        @pl.when(b >= d)
        def _():
            remote(kv_all.at[b - d], kv_all.at[b - d], es.at[d], er.at[d], (b - d, t)).wait_recv()
            remote(seg_all.at[b - d], seg_all.at[b - d], gs.at[d], gr.at[d], (b - d, t)).wait_recv()

    qrows = 256
    scale = HD ** (-0.5)

    def attend(h, part):
        r0 = part * qrows
        qh = qrot[r0:r0 + qrows, h * HD:(h + 1) * HD]
        sq = segq_ref[r0:r0 + qrows, :]
        ri = b * n_tok + r0 + lax.broadcasted_iota(jnp.int32, (qrows, n_tok), 0)
        ci = lax.broadcasted_iota(jnp.int32, (qrows, n_tok), 1)

        def block(j, st):
            m, l, c = st
            kb = kv_all[j]
            s = lax.dot_general(qh, kb[:, :HD], (((1,), (1,)), ((), ())),
                                preferred_element_type=F32) * scale
            vis = (ci + j * n_tok <= ri) & (seg_all[j] == sq)
            s = jnp.where(vis, s, NEGATIVE_FILL)
            m2 = jnp.maximum(m, jnp.max(s, axis=1, keepdims=True))
            f = jnp.exp(m - m2)
            p = jnp.where(vis, jnp.exp(s - m2), 0.0)
            l = l * f + jnp.sum(p, axis=1, keepdims=True)
            c = c * f + jnp.dot(p.astype(BF), kb[:, HD:], preferred_element_type=F32)
            return (m2, l, c)

        init = (jnp.full((qrows, 1), NEGATIVE_FILL, F32), jnp.zeros((qrows, 1), F32),
                jnp.zeros((qrows, HD), F32))
        m, l, c = lax.fori_loop(0, b + 1, block, init)
        return (c / l).astype(BF)

    n_pair = ctx_all.shape[1]

    def az(tt, p, dz, dev):
        piece = ctx_all.at[tt, p]
        return remote(piece, piece, azs.at[p, dz], azr.at[p, dz], dev)

    def ay(tt, p, dz, dev):
        piece = ctx_all.at[tt, p]
        return remote(piece, piece, ays.at[p, dz], ayr.at[p, dz], dev)

    direct = [(i, k) for i in range(half) for k in range(nb)]
    crossed = list(direct)
    for p in range(n_pair):
        for hh in range(2):
            for part in range(n_tok // qrows):
                ctx_all[t, p, part * qrows:(part + 1) * qrows, hh * HD:(hh + 1) * HD] = attend(
                    2 * p + hh, part)
                for e in range(2):
                    w_direct(*direct.pop(0))
        for dz in range(1, nt // 2):
            az(t, p, dz, (b, flip(t, 2 * dz))).start()
        ay(t, p, 0, (b, flip(t, 1))).start()

    while direct:
        w_direct(*direct.pop(0))

    for p in range(n_pair):
        for dz in range(1, nt // 2):
            az(flip(t, 2 * dz), p, dz, (b, flip(t, 2 * dz))).wait_recv()
            ay(flip(t, 2 * dz), p, dz, (b, flip(t, 1))).start()

    for piece in crossed:
        w_crossed(*piece)
    for ch in range(nt):
        for k in range(nb):
            @pl.when((b != prim) & (b != flip(prim, 2)))
            def _():
                wfwd(k, ch, wcs, wcr, (bc, t)).wait_recv()

    oacc[...] = x_ref[:, pl.ds(pl.multiple_of(t * oc, 128), oc)].astype(F32)

    def project(tt, p):
        cw = ctx_all.shape[3]
        oacc[...] += lax.dot_general(ctx_all[tt, p], wo[tt, :, p * cw:(p + 1) * cw],
                                     (((1,), (1,)), ((), ())), preferred_element_type=F32)

    for p in range(n_pair):
        for dz in range(nt // 2):
            project(flip(t, 2 * dz), p)
    for p in range(n_pair):
        for dz in range(nt // 2):
            other = flip(t, 2 * dz + 1)
            ay(other, p, dz, (b, flip(t, 1))).wait_recv()
            project(other, p)
    out_ref[...] = oacc[...].astype(BF)

    gather_sent(kv_set)
    gather_sent(q_set)
    for d in range(1, nb):
        @pl.when(b + d < nb)
        def _():
            dst = (b + d, t)
            remote(kv_all.at[b], kv_all.at[b], es.at[d], er.at[d], dst).wait_send()
            remote(seg_all.at[b], seg_all.at[b], gs.at[d], gr.at[d], dst).wait_send()
    for i in range(half):
        to_relay(i).wait_send()

        @pl.when(t_dst != t)
        def _():
            straight(i).wait_send()

        @pl.when(t_via != t)
        def _():
            from_relay(i).wait_send()
        for k in range(nb):
            for role, where in ((0, prim), (1, flip(prim, 2))):
                @pl.when(b == where)
                def _():
                    wfwd(k, role * half + i, wxs, wxr, (bx, t)).wait_send()
                    wfwd(k, i, wcs, wcr, (bc, t)).wait_send()
                    wfwd(k, half + i, wcs, wcr, (bc, t)).wait_send()
    for p in range(n_pair):
        for dz in range(nt // 2):
            if dz:
                az(t, p, dz, (b, flip(t, 2 * dz))).wait_send()
            ay(flip(t, 2 * dz), p, dz, (b, flip(t, 1))).wait_send()


def fused(nb, nt, residual_in, norm_gain, w_query, w_key_value, query_bias, key_value_bias, w_output,
          device_map, positions, segments):
    n_tok, width = residual_in.shape
    rows = w_query.shape[0]
    qc, kc, oc = w_query.shape[1] // nt, w_key_value.shape[1] // nt, width // nt
    n = nb * nt
    inv = ROPE_BASE ** (-(np.arange(HD // 2, dtype=np.float64) * 2.0) / HD)
    inv = np.concatenate([inv, inv]).astype(np.float32)[None, :]
    any_, vm = pl.BlockSpec(memory_space=pl.ANY), pl.BlockSpec(memory_space=pltpu.VMEM)
    dma = pltpu.SemaphoreType.DMA
    return pl.pallas_call(
        functools.partial(fused_kernel, nb, nt),
        out_shape=jax.ShapeDtypeStruct((n_tok, oc), BF),
        in_specs=[pl.BlockSpec(memory_space=pltpu.SMEM), any_, any_, any_, vm, vm, vm, any_, vm, vm, vm],
        out_specs=vm,
        scratch_shapes=[
            pltpu.VMEM((n_tok, width), BF),
            pltpu.VMEM((n, n_tok, rows), BF),
            pltpu.VMEM((n, rows, qc), BF),
            pltpu.VMEM((n, rows, kc), BF),
            pltpu.VMEM((nt, oc, qc), BF),
            pltpu.VMEM((nb, n_tok, kc), BF),
            pltpu.VMEM((nb, 1, n_tok), jnp.int32),
            pltpu.VMEM((n_tok, qc), F32),
            pltpu.VMEM((n_tok, kc), F32),
            pltpu.VMEM((n_tok, qc), BF),
            pltpu.VMEM((nt, qc // (2 * HD), n_tok, 2 * HD), BF),
            pltpu.VMEM((n_tok, oc), F32),
            pltpu.VMEM((width // 128, 128), F32), pltpu.VMEM((qc * nt // HD, HD), F32),
            pltpu.VMEM((kc * nt // HD, HD), F32), pltpu.VMEM((n_tok, HD), F32),
            pltpu.VMEM((n_tok, HD), F32), pltpu.VMEM((n_tok, 1), jnp.int32),
            dma, dma((3,)),
            dma((nt,)), dma((nt,)), dma((nt,)), dma((nt,)), dma((2 * nt,)), dma((2 * nt,)),
            dma((nt,)), dma((nt,)), dma((nt,)), dma((nt,)), dma((2 * nt,)), dma((2 * nt,)),
            dma((nt,)), dma((nb, nt)), dma((nb, nt)), dma((nb, nt)), dma((nb, nt)), dma((nb, nt)),
            dma((nb,)), dma((nb,)), dma((nb,)), dma((nb,)),
            dma((2, nt // 2)), dma((2, nt // 2)), dma((2, nt // 2)), dma((2, nt // 2)),
            pltpu.VMEM((nt // 2, rows, qc), BF), dma((nt // 2,)), dma((nt // 2,)),
        ],
        compiler_params=pltpu.CompilerParams(
            collective_id=0, has_side_effects=True, vmem_limit_bytes=63 * 1024 * 1024),
    )(device_map, residual_in, w_query, w_key_value, norm_gain.reshape(-1, 128), query_bias.reshape(-1, HD),
      key_value_bias.reshape(-1, HD), w_output.T, jnp.asarray(inv), positions[None, :], segments[None, :])


def route(shape, *args):
    nb, nt = shape["blk"], shape["tp"]
    n_tok, width = args[0].shape
    rows = args[2].shape[0]
    qc, kc, oc = args[2].shape[1] // nt, args[3].shape[1] // nt, width // nt
    fits = (nb == 4 and nt == KVH and rows % 32 == 0 and rows <= 160 and qc == 4 * HD and kc == 2 * HD
            and oc == nb * rows and oc % 128 == 0 and width % 128 == 0 and n_tok % 256 == 0)
    if fits:
        return fused(nb, nt, *args)
    return per_device(*args)


def solution(mesh):
    in_specs = (
        P("blk", None),
        P(),
        P(("blk", "tp"), None),
        P(("blk", "tp"), None),
        P(),
        P(),
        P(None, ("blk", "tp")),
        P(),
        P("blk"),
        P("blk"),
    )
    out_specs = P("blk", "tp")
    return jax.shard_map(
        functools.partial(route, dict(mesh.shape)), mesh=mesh, in_specs=in_specs, out_specs=out_specs, check_vma=False
    )
```

```python
import functools

import jax
import jax.numpy as jnp
import numpy as np
from jax import lax
from jax.experimental import pallas as pl
from jax.experimental.pallas import tpu as pltpu
from jax.sharding import PartitionSpec as P

D = 5120
KVH = 8
HD = 128


NORM_FLOOR = 0.0625
ROPE_BASE = 1000000.0
NEGATIVE_FILL = -1e30


def for_sending(x):
    return jax.tree.map(lambda a: a.astype(jnp.bfloat16) if a.dtype == jnp.float32 else a, x)


def from_partner(block, axis, bit):
    count = lax.axis_size(axis)
    route = []
    for low in range(count):
        high = low | 1 << bit
        if high != low and high < count:
            route += [(low, high), (high, low)]
    return lax.ppermute(block, axis, route)


def rope_tables(positions, head_width):
    half_width = head_width // 2
    frequency = ROPE_BASE ** (-(jnp.arange(half_width, dtype=jnp.float32) * 2.0) / head_width)
    angles = positions.astype(jnp.float32)[:, None] * frequency[None, :]
    angles = jnp.concatenate([angles, angles], axis=1)
    return (jnp.cos(angles), jnp.sin(angles))


def rotate(values, cosine_table, sine_table):
    half_width = values.shape[-1] // 2
    turned = jnp.concatenate([-values[..., half_width:], values[..., :half_width]], axis=-1)
    return values * cosine_table[:, None, :] + turned * sine_table[:, None, :]


def join_pair(mine_cols, partner, is_lower):
    return jnp.where(
        is_lower,
        jnp.concatenate([mine_cols, partner], axis=1),
        jnp.concatenate([partner, mine_cols], axis=1),
    )


def per_device(
    residual_in,
    norm_gain,
    w_query,
    w_key_value,
    query_bias,
    key_value_bias,
    w_output,
    device_map,
    positions,
    segments,
):
    tp_count = lax.axis_size("tp")
    tp_index = lax.axis_index("tp")
    blk_index = lax.axis_index("blk")
    local_tokens = residual_in.shape[0]
    shard_rows = w_query.shape[0]
    kv_group = tp_count // KVH
    floats = residual_in.astype(jnp.float32)
    square = jnp.maximum(jnp.mean(floats * floats, axis=1, keepdims=True), NORM_FLOOR)
    normed = (floats * lax.rsqrt(square) * norm_gain.astype(jnp.float32)).astype(jnp.bfloat16)
    ordered = jnp.take(
        normed.reshape(local_tokens, device_map.shape[0], shard_rows), device_map, axis=1
    ).reshape(local_tokens, D)
    moved_query, moved_pairs = (
        lax.all_to_all(w_query, "tp", split_axis=1, concat_axis=0, tiled=True),
        lax.all_to_all(w_key_value, "tp", split_axis=1, concat_axis=0, tiled=True),
    )
    for bit_level in range(kv_group.bit_length() - 1):
        partner = from_partner(for_sending(moved_pairs), "tp", bit_level).astype(moved_pairs.dtype)
        moved_pairs = join_pair(moved_pairs, partner, tp_index >> bit_level & 1 == 0)
    queries = jnp.dot(
        ordered,
        lax.all_gather(moved_query, "blk", axis=0, tiled=True),
        preferred_element_type=jnp.float32,
    )
    key_value = jnp.dot(
        ordered,
        lax.all_gather(moved_pairs, "blk", axis=0, tiled=True),
        preferred_element_type=jnp.float32,
    )
    query_width = queries.shape[1]
    heads_here = query_width // HD
    kv_head = tp_index // kv_group
    queries = queries + lax.dynamic_slice_in_dim(
        query_bias, tp_index * query_width, query_width
    ).astype(jnp.float32)
    key_value = key_value + lax.dynamic_slice_in_dim(
        key_value_bias, kv_head * 2 * HD, 2 * HD
    ).astype(jnp.float32)
    cosine_table, sine_table = rope_tables(positions, HD)
    query_rot = rotate(
        queries.reshape(local_tokens, heads_here, HD), cosine_table, sine_table
    ).astype(jnp.bfloat16)
    key_rot = rotate(key_value[:, None, :HD], cosine_table, sine_table)[:, 0, :].astype(
        jnp.bfloat16
    )
    values = key_value[:, HD:].astype(jnp.bfloat16)
    attend_scale = HD ** (-0.5)
    row_index = blk_index * local_tokens + jnp.arange(local_tokens, dtype=jnp.int32)
    initial = (
        jnp.full((heads_here, local_tokens), NEGATIVE_FILL, jnp.float32),
        jnp.zeros((heads_here, local_tokens), jnp.float32),
        jnp.zeros((heads_here, local_tokens, HD), jnp.float32),
    )
    key_piece = lax.all_gather(key_rot, "blk", axis=0, tiled=True)
    value_piece = lax.all_gather(values, "blk", axis=0, tiled=True)
    segment_piece = lax.all_gather(segments, "blk", axis=0, tiled=True)
    piece_rows = key_piece.shape[0]
    key_block_rows = 512

    def one_block(block_number, state_now):
        run_peak, run_mass, context = state_now
        block_start = block_number * key_block_rows
        key_block = lax.dynamic_slice_in_dim(key_piece, block_start, key_block_rows, 0)
        value_block = lax.dynamic_slice_in_dim(value_piece, block_start, key_block_rows, 0)
        segment_block = lax.dynamic_slice_in_dim(segment_piece, block_start, key_block_rows, 0)
        scores = (
            jnp.einsum("qhd,kd->hqk", query_rot, key_block, preferred_element_type=jnp.float32)
            * attend_scale
        )
        key_index = block_start + jnp.arange(key_block_rows, dtype=jnp.int32)
        visible = (key_index[None, :] <= row_index[:, None]) & (
            segment_block[None, :] == segments[:, None]
        )
        masked = jnp.where(visible[None], scores, NEGATIVE_FILL)
        new_peak = jnp.maximum(run_peak, jnp.max(masked, axis=2))
        factor = jnp.exp(run_peak - new_peak)
        raw_weights = jnp.where(visible[None], jnp.exp(masked - new_peak[:, :, None]), 0.0)
        run_mass = run_mass * factor + jnp.sum(raw_weights, axis=2)
        context = context * factor[:, :, None] + jnp.einsum(
            "hqk,kd->hqd",
            raw_weights.astype(jnp.bfloat16),
            value_block,
            preferred_element_type=jnp.float32,
        )
        return (new_peak, run_mass, context)

    run_peak, run_mass, context = lax.fori_loop(0, piece_rows // key_block_rows, one_block, initial)
    context_flat = (
        (context / run_mass[:, :, None])
        .transpose(1, 0, 2)
        .reshape(local_tokens, query_width)
        .astype(jnp.bfloat16)
    )
    width_out = D // tp_count
    moved_out = lax.all_to_all(w_output, "tp", split_axis=0, concat_axis=1, tiled=True)
    row_terms = jnp.dot(
        context_flat,
        lax.all_gather(moved_out, "blk", axis=1, tiled=True),
        preferred_element_type=jnp.float32,
    )
    summed = lax.psum_scatter(
        row_terms.astype(jnp.bfloat16), "tp", scatter_dimension=1, tiled=True
    ).astype(jnp.float32)
    residual_part = lax.dynamic_slice_in_dim(residual_in, tp_index * width_out, width_out, 1)
    return (residual_part.astype(jnp.float32) + summed).astype(jnp.bfloat16)


MESH = pl.DeviceIdType.MESH
BF = jnp.bfloat16
F32 = jnp.float32


def flip(i, mask):
    out = i
    for bit in range(mask.bit_length()):
        if mask >> bit & 1:
            out = out + (1 << bit) * (1 - 2 * ((i // (1 << bit)) % 2))
    return out


def fused_kernel(nb, nt, dm_ref, x_hbm, wq_hbm, wkv_hbm, gain_ref, bq_ref, bkv_ref, wo_hbm, inv_ref,
                 pos_ref, seg_ref, out_ref, x_ref, xo, gq, gkv, wo, kv_all, seg_all, qacc,
                 kvacc, qrot, ctx_all, oacc, gain32, bq32, bkv32, cos_t, sin_t, segq_ref,
                 x_sem, loc_sem, kv1s, kv1r, kvxs, kvxr, kvcs, kvcr, q1s, q1r, qxs, qxr, qcs, qcr,
                 w1s, w1r, wxs, wxr, wcs, wcr, es, er, gs, gr, azs, azr, ays, ayr, wrel, rr, r2s):
    b = lax.axis_index("blk")
    t = lax.axis_index("tp")
    n_tok, width = x_ref.shape
    rows = wq_hbm.shape[0]
    qc, kc = gq.shape[2], gkv.shape[2]
    oc = wo.shape[1]
    bx, bc = flip(b, 2), flip(b, 1)

    barrier = pltpu.get_barrier_semaphore()
    peers = [(b, flip(t, k)) for k in range(1, nt)] + [(flip(b, k), t) for k in range(1, nb)]
    peers += [(bx, flip(t, 1))]
    for peer in peers:
        pl.semaphore_signal(barrier, inc=1, device_id=peer, device_id_type=MESH)
    x_in = pltpu.make_async_copy(x_hbm, x_ref, x_sem)
    x_in.start()
    gain32[...] = gain_ref[...].astype(F32)
    bq32[...] = bq_ref[...].astype(F32)
    bkv32[...] = bkv_ref[...].astype(F32)
    with jax.named_scope("barrier"):
        pl.semaphore_wait(barrier, len(peers))

    def remote(src, dst, ss, rs, dev):
        return pltpu.make_async_remote_copy(src_ref=src, dst_ref=dst, send_sem=ss, recv_sem=rs,
                                            device_id=dev, device_id_type=MESH)

    def slot(bb, k):
        return bb * nt + flip(t, k)

    def stage_one(hbm, buf, width, k, ss, rs, local):
        cols = pl.ds(pl.multiple_of(flip(t, k) * width, 128), width)
        mine = buf.at[b * nt + t]
        if k == 0:
            return pltpu.make_async_copy(hbm.at[:, cols], mine, local)
        return remote(hbm.at[:, cols], mine, ss.at[k], rs.at[k], (b, flip(t, k)))

    def stage_one_in(buf, hbm, width, k, ss, rs, local):
        if k == 0:
            return stage_one(hbm, buf, width, 0, ss, rs, local)
        piece = buf.at[slot(b, k)]
        return remote(piece, piece, ss.at[k], rs.at[k], (b, flip(t, k)))

    def forward(buf, bb, k, ss, rs, i, dev):
        piece = buf.at[slot(bb, k)]
        return remote(piece, piece, ss.at[i], rs.at[i], dev)

    kv_set = (wkv_hbm, gkv, kc, kv1s, kv1r, kvxs, kvxr, kvcs, kvcr, loc_sem.at[0])
    q_set = (wq_hbm, gq, qc, q1s, q1r, qxs, qxr, qcs, qcr, loc_sem.at[1])

    order = [0, 1, 2, 4, 3, 6, 5, 7]

    def across(ws, k):
        hbm, buf, width, s1, r1, xs, xr, cs, cr, loc = ws
        cols = pl.ds(pl.multiple_of(flip(t, k) * width, 128), width)
        return remote(hbm.at[:, cols], buf.at[b * nt + t], xs.at[k], xr.at[k], (bx, flip(t, k)))

    def start_one(ws, k):
        hbm, buf, width, s1, r1, xs, xr, cs, cr, loc = ws
        stage_one(hbm, buf, width, k, s1, r1, loc).start()
        if k < 2:
            across(ws, k).start()

    def gather_step(ws, i):
        k = order[i]
        hbm, buf, width, s1, r1, xs, xr, cs, cr, loc = ws
        arrived = stage_one_in(buf, hbm, width, k, s1, r1, loc)
        if k == 0:
            arrived.wait()
        else:
            arrived.wait_recv()
        if k > 1:
            forward(buf, b, k, xs, xr, k, (bx, t)).start()
        forward(buf, b, k, cs, cr, k, (bc, t)).start()

    def gather_cross(ws, i):
        k = order[i]
        hbm, buf, width, s1, r1, xs, xr, cs, cr, loc = ws
        forward(buf, bx, k, xs, xr, k, (bx, t)).wait_recv()
        forward(buf, bx, k, cs, cr, nt + k, (bc, t)).start()

    def gather_last(ws, i):
        k = order[i]
        hbm, buf, width, s1, r1, xs, xr, cs, cr, loc = ws
        forward(buf, bc, k, cs, cr, k, (bc, t)).wait_recv()
        forward(buf, flip(b, 3), k, cs, cr, nt + k, (bc, t)).wait_recv()

    def gather_sent(ws):
        hbm, buf, width, s1, r1, xs, xr, cs, cr, loc = ws
        for k in range(nt):
            if k:
                stage_one(hbm, buf, width, k, s1, r1, loc).wait_send()
            if k < 2:
                across(ws, k).wait_send()
            else:
                forward(buf, b, k, xs, xr, k, (bx, t)).wait_send()
            forward(buf, b, k, cs, cr, k, (bc, t)).wait_send()
            forward(buf, bx, k, cs, cr, nt + k, (bc, t)).wait_send()

    def multiply(buf, acc, i):
        k = order[i]

        def one(j, _):
            s = slot(j, k)
            acc[...] += jnp.dot(xo[dm_ref[s]], buf[s], preferred_element_type=F32)
            return 0
        lax.fori_loop(0, nb, one, 0)

    issue = [0,2,4,1,6,3,5,7]
    for k in issue:
        start_one(kv_set, k)

    x_in.wait()
    tile = n_tok // nt

    def norm_tile(i):
        toks = slice(i * tile, (i + 1) * tile)
        v = x_ref[toks, :].astype(F32)
        scale = lax.rsqrt(jnp.maximum(jnp.mean(v * v, axis=1, keepdims=True), NORM_FLOOR))

        def spread(g, _):
            per = 4 * rows // 128
            gain = jnp.concatenate([gain32[pl.ds(g * per + i, 1), :] for i in range(per)], axis=1)
            u = x_ref[toks, pl.ds(pl.multiple_of(g * 4 * rows, 128), 4 * rows)].astype(F32)
            u = (u * scale * gain).astype(BF)
            for i in range(4):
                xo[g * 4 + i, toks, :] = u[:, i * rows:(i + 1) * rows]
            return 0

        lax.fori_loop(0, nb * nt // 4, spread, 0)

    def tables():
        pos = jnp.broadcast_to(pos_ref[...].astype(F32), (HD, n_tok)).T
        angles = pos * inv_ref[...]
        cos_t[...] = jnp.cos(angles)
        sign = jnp.where(lax.broadcasted_iota(jnp.int32, (1, HD), 1) < HD // 2, -1.0, 1.0)
        sin_t[...] = jnp.sin(angles) * sign
        segq_ref[...] = jnp.broadcast_to(seg_ref[...].astype(F32), (HD, n_tok)).T[:, :1].astype(jnp.int32)

    for k in range(nt):
        with jax.named_scope(f"norm{k}"):
            norm_tile(k)
        with jax.named_scope(f"kvstep{k}"):
            gather_step(kv_set, k)
        if k >= 2:
            start_one(q_set, issue[k - 2])
        if k:
            with jax.named_scope(f"kvcross{k}"):
                gather_cross(kv_set, k - 1)
    for k in range(nt - 2, nt):
        start_one(q_set, issue[k])
    with jax.named_scope("tables"):
        tables()
    with jax.named_scope("kvcross8"):
        gather_cross(kv_set, nt - 1)

    for e in range(2):
        kvacc[:, e * HD:(e + 1) * HD] = jnp.broadcast_to(bkv32[pl.ds(t * 2 + e, 1), :], (n_tok, HD))
    for k in range(4):
        with jax.named_scope(f"qstep{k}"):
            gather_step(q_set, k)
        if k:
            with jax.named_scope(f"qcross{k}"):
                gather_cross(q_set, k - 1)
    for e in range(qc // HD):
        qacc[:, e * HD:(e + 1) * HD] = jnp.broadcast_to(
            bq32[pl.ds(t * (qc // HD) + e, 1), :], (n_tok, HD))
    for e in range(nt):
        gather_last(kv_set, e)
        with jax.named_scope(f"kvmul{e}"):
            multiply(gkv, kvacc, e)
        if e % 2 and 4 + e // 2 < nt:
            k = 4 + e // 2
            with jax.named_scope(f"qstep{k}"):
                gather_step(q_set, k)
            with jax.named_scope(f"qcross{k}"):
                gather_cross(q_set, k - 1)
            if e > 1:
                gather_last(q_set, e // 2 - 1)
                multiply(gq, qacc, e // 2 - 1)

    def rope(u):
        return u * cos_t[...] + pltpu.roll(u, HD // 2, 1) * sin_t[...]

    kv_all[b, :, :HD] = rope(kvacc[:, :HD]).astype(BF)
    kv_all[b, :, HD:] = kvacc[:, HD:].astype(BF)
    seg_all[b] = seg_ref[...]

    def keys(slot_b, sem, dev):
        return (remote(kv_all.at[slot_b], kv_all.at[slot_b], es.at[sem], er.at[sem], dev),
                remote(seg_all.at[slot_b], seg_all.at[slot_b], gs.at[sem], gr.at[sem], dev))

    low = b < nb // 2
    even = b % 2 == 0

    @pl.when(low)
    def _():
        for c in keys(b, 0, (bx, t)):
            c.start()

    @pl.when(even)
    def _():
        for c in keys(b, 1, (bc, t)):
            c.start()

    flat, flat_x = b * nt + t, bx * nt + t
    t_dst, k_mine = flat // nb, flat % nb
    t_via, k_via = flat_x // nb, flat_x % nb
    prim = (t * nb) // nt
    k_own = t - (t * nb - prim * nt)
    half = nt // 2

    def wpiece(k, ch):
        return wo.at[ch, pl.ds(pl.multiple_of(k * rows, 16), rows), :]

    def wsrc(ch):
        return wo_hbm.at[:, pl.ds(ch * qc, qc)]

    def straight(ch):
        return remote(wsrc(ch), wpiece(k_mine, ch), w1s.at[ch], w1r.at[k_mine, ch], (b, t_dst))

    def to_relay(i):
        return remote(wsrc(half + i), wrel.at[i], w1s.at[half + i], rr.at[i], (bx, t))

    def from_relay(i):
        return remote(wrel.at[i], wpiece(k_via, half + i), r2s.at[i], w1r.at[k_via, half + i], (b, t_via))

    def wfwd(k, ch, ss, rs, dev):
        return remote(wpiece(k, ch), wpiece(k, ch), ss.at[k, ch], rs.at[k, ch], dev)

    def w_start():
        for i in range(half):
            to_relay(i).start()

        @pl.when(t_dst != t)
        def _():
            for ch in range(half):
                straight(ch).start()

        @pl.when(t_dst == t)
        def _():
            for ch in range(half):
                pltpu.make_async_copy(wsrc(ch), wpiece(k_mine, ch), w1s.at[ch]).start()

    def w_relay():
        for i in range(half):
            to_relay(i).wait_recv()

            @pl.when(t_via != t)
            def _():
                from_relay(i).start()

            @pl.when(t_via == t)
            def _():
                pltpu.make_async_copy(wrel.at[i], wpiece(k_via, half + i), r2s.at[i]).start()

    def w_direct(i, k):
        for role, where in ((0, prim), (1, flip(prim, 2))):
            ch = role * half + i

            @pl.when((b == where) & (k != k_own))
            def _():
                src = (b, t * nb + k - prim * nt)
                remote(wpiece(k, ch), wpiece(k, ch), w1s.at[ch], w1r.at[k, ch], src).wait_recv()

            @pl.when((b == where) & (k == k_own))
            def _():
                if role == 0:
                    pltpu.make_async_copy(wsrc(ch), wpiece(k, ch), w1s.at[ch]).wait()
                else:
                    pltpu.make_async_copy(wrel.at[i], wpiece(k, ch), r2s.at[i]).wait()

            @pl.when(b == where)
            def _():
                wfwd(k, ch, wxs, wxr, (bx, t)).start()
                wfwd(k, ch, wcs, wcr, (bc, t)).start()

    def w_crossed(i, k):
        for role, where in ((0, prim), (1, flip(prim, 2))):
            ch = (1 - role) * half + i

            @pl.when(b == where)
            def _():
                wfwd(k, ch, wxs, wxr, (bx, t)).wait_recv()
                wfwd(k, ch, wcs, wcr, (bc, t)).start()

    for k in range(8, nt):
        with jax.named_scope(f"qstep{k}"):
            gather_step(q_set, k)
        with jax.named_scope(f"qcross{k}"):
            gather_cross(q_set, k - 1)
    w_start()
    for e in range(nt // 2 - 1, nt):
        if e == nt - 3:
            with jax.named_scope("qcross8"):
                gather_cross(q_set, nt - 1)
        with jax.named_scope(f"qlast{e}"):
            gather_last(q_set, e)
        with jax.named_scope(f"qmul{e}"):
            multiply(gq, qacc, e)

    with jax.named_scope("wrelay"):
        w_relay()

    for h in range(qc // HD):
        cols = slice(h * HD, (h + 1) * HD)
        qrot[:, cols] = rope(qacc[:, cols]).astype(BF)

    @pl.when(b >= nb // 2)
    def _():
        for c in keys(bx, 0, (bx, t)):
            c.wait_recv()
        for c in keys(bx, 2, (bc, t)):
            c.start()
        for c in keys(flip(b, 3), 2, (bc, t)):
            c.wait_recv()

    @pl.when(b % 2 == 1)
    def _():
        for c in keys(bc, 1, (bc, t)):
            c.wait_recv()

    qrows = 256
    scale = HD ** (-0.5)

    def attend(h, part):
        r0 = part * qrows
        qh = qrot[r0:r0 + qrows, h * HD:(h + 1) * HD]
        sq = segq_ref[r0:r0 + qrows, :]
        ri = b * n_tok + r0 + lax.broadcasted_iota(jnp.int32, (qrows, n_tok), 0)
        ci = lax.broadcasted_iota(jnp.int32, (qrows, n_tok), 1)

        def block(j, st):
            m, l, c = st
            kb = kv_all[j]
            s = lax.dot_general(qh, kb[:, :HD], (((1,), (1,)), ((), ())),
                                preferred_element_type=F32) * scale
            vis = (ci + j * n_tok <= ri) & (seg_all[j] == sq)
            s = jnp.where(vis, s, NEGATIVE_FILL)
            m2 = jnp.maximum(m, jnp.max(s, axis=1, keepdims=True))
            f = jnp.exp(m - m2)
            p = jnp.where(vis, jnp.exp(s - m2), 0.0)
            l = l * f + jnp.sum(p, axis=1, keepdims=True)
            c = c * f + jnp.dot(p.astype(BF), kb[:, HD:], preferred_element_type=F32)
            return (m2, l, c)

        init = (jnp.full((qrows, 1), NEGATIVE_FILL, F32), jnp.zeros((qrows, 1), F32),
                jnp.zeros((qrows, HD), F32))
        m, l, c = lax.fori_loop(0, b + 1, block, init)
        return (c / l).astype(BF)

    n_pair = ctx_all.shape[1]

    def az(tt, p, dz, dev):
        piece = ctx_all.at[tt, p]
        return remote(piece, piece, azs.at[p, dz], azr.at[p, dz], dev)

    def ay(tt, p, dz, dev):
        piece = ctx_all.at[tt, p]
        return remote(piece, piece, ays.at[p, dz], ayr.at[p, dz], dev)

    direct = [(i, k) for i in range(half) for k in range(nb)]
    crossed = list(direct)
    for p in range(n_pair):
        for hh in range(2):
            for part in range(n_tok // qrows):
              with jax.named_scope(f"att{p}{hh}{part}"):
                ctx_all[t, p, part * qrows:(part + 1) * qrows, hh * HD:(hh + 1) * HD] = attend(
                    2 * p + hh, part)
                for e in range(2):
                    w_direct(*direct.pop(0))
        for dz in range(1, nt // 2):
            az(t, p, dz, (b, flip(t, 2 * dz))).start()
        ay(t, p, 0, (b, flip(t, 1))).start()

    with jax.named_scope("wdirrest"):
      while direct:
        w_direct(*direct.pop(0))

    for p in range(n_pair):
        for dz in range(1, nt // 2):
          with jax.named_scope(f"az{p}{dz}"):
            az(flip(t, 2 * dz), p, dz, (b, flip(t, 2 * dz))).wait_recv()
            ay(flip(t, 2 * dz), p, dz, (b, flip(t, 1))).start()

    for piece in crossed:
        w_crossed(*piece)
    for ch in range(nt):
        for k in range(nb):
            @pl.when((b != prim) & (b != flip(prim, 2)))
            def _():
                wfwd(k, ch, wcs, wcr, (bc, t)).wait_recv()

    oacc[...] = x_ref[:, pl.ds(pl.multiple_of(t * oc, 128), oc)].astype(F32)

    def project(tt, p):
        cw = ctx_all.shape[3]
        oacc[...] += lax.dot_general(ctx_all[tt, p], wo[tt, :, p * cw:(p + 1) * cw],
                                     (((1,), (1,)), ((), ())), preferred_element_type=F32)

    for p in range(n_pair):
        for dz in range(nt // 2):
            project(flip(t, 2 * dz), p)
    for p in range(n_pair):
        for dz in range(nt // 2):
            other = flip(t, 2 * dz + 1)
            ay(other, p, dz, (b, flip(t, 1))).wait_recv()
            project(other, p)
    out_ref[...] = oacc[...].astype(BF)

    gather_sent(kv_set)
    gather_sent(q_set)

    @pl.when(low)
    def _():
        for c in keys(b, 0, (bx, t)):
            c.wait_send()

    @pl.when(even)
    def _():
        for c in keys(b, 1, (bc, t)):
            c.wait_send()

    @pl.when(b >= nb // 2)
    def _():
        for c in keys(bx, 2, (bc, t)):
            c.wait_send()

    for i in range(half):
        to_relay(i).wait_send()

        @pl.when(t_dst != t)
        def _():
            straight(i).wait_send()

        @pl.when(t_via != t)
        def _():
            from_relay(i).wait_send()
        for k in range(nb):
            for role, where in ((0, prim), (1, flip(prim, 2))):
                @pl.when(b == where)
                def _():
                    wfwd(k, role * half + i, wxs, wxr, (bx, t)).wait_send()
                    wfwd(k, i, wcs, wcr, (bc, t)).wait_send()
                    wfwd(k, half + i, wcs, wcr, (bc, t)).wait_send()
    for p in range(n_pair):
        for dz in range(nt // 2):
            if dz:
                az(t, p, dz, (b, flip(t, 2 * dz))).wait_send()
            ay(flip(t, 2 * dz), p, dz, (b, flip(t, 1))).wait_send()


def fused(nb, nt, residual_in, norm_gain, w_query, w_key_value, query_bias, key_value_bias, w_output,
          device_map, positions, segments):
    n_tok, width = residual_in.shape
    rows = w_query.shape[0]
    qc, kc, oc = w_query.shape[1] // nt, w_key_value.shape[1] // nt, width // nt
    n = nb * nt
    inv = ROPE_BASE ** (-(np.arange(HD // 2, dtype=np.float64) * 2.0) / HD)
    inv = np.concatenate([inv, inv]).astype(np.float32)[None, :]
    any_, vm = pl.BlockSpec(memory_space=pl.ANY), pl.BlockSpec(memory_space=pltpu.VMEM)
    dma = pltpu.SemaphoreType.DMA
    return pl.pallas_call(
        functools.partial(fused_kernel, nb, nt),
        out_shape=jax.ShapeDtypeStruct((n_tok, oc), BF),
        in_specs=[pl.BlockSpec(memory_space=pltpu.SMEM), any_, any_, any_, vm, vm, vm, any_, vm, vm, vm],
        out_specs=vm,
        scratch_shapes=[
            pltpu.VMEM((n_tok, width), BF),
            pltpu.VMEM((n, n_tok, rows), BF),
            pltpu.VMEM((n, rows, qc), BF),
            pltpu.VMEM((n, rows, kc), BF),
            pltpu.VMEM((nt, oc, qc), BF),
            pltpu.VMEM((nb, n_tok, kc), BF),
            pltpu.VMEM((nb, 1, n_tok), jnp.int32),
            pltpu.VMEM((n_tok, qc), F32),
            pltpu.VMEM((n_tok, kc), F32),
            pltpu.VMEM((n_tok, qc), BF),
            pltpu.VMEM((nt, qc // (2 * HD), n_tok, 2 * HD), BF),
            pltpu.VMEM((n_tok, oc), F32),
            pltpu.VMEM((width // 128, 128), F32), pltpu.VMEM((qc * nt // HD, HD), F32),
            pltpu.VMEM((kc * nt // HD, HD), F32), pltpu.VMEM((n_tok, HD), F32),
            pltpu.VMEM((n_tok, HD), F32), pltpu.VMEM((n_tok, 1), jnp.int32),
            dma, dma((3,)),
            dma((nt,)), dma((nt,)), dma((nt,)), dma((nt,)), dma((2 * nt,)), dma((2 * nt,)),
            dma((nt,)), dma((nt,)), dma((nt,)), dma((nt,)), dma((2 * nt,)), dma((2 * nt,)),
            dma((nt,)), dma((nb, nt)), dma((nb, nt)), dma((nb, nt)), dma((nb, nt)), dma((nb, nt)),
            dma((nb,)), dma((nb,)), dma((nb,)), dma((nb,)),
            dma((2, nt // 2)), dma((2, nt // 2)), dma((2, nt // 2)), dma((2, nt // 2)),
            pltpu.VMEM((nt // 2, rows, qc), BF), dma((nt // 2,)), dma((nt // 2,)),
        ],
        compiler_params=pltpu.CompilerParams(
            collective_id=0, has_side_effects=True, vmem_limit_bytes=63 * 1024 * 1024),
    )(device_map, residual_in, w_query, w_key_value, norm_gain.reshape(-1, 128), query_bias.reshape(-1, HD),
      key_value_bias.reshape(-1, HD), w_output.T, jnp.asarray(inv), positions[None, :], segments[None, :])


def route(shape, *args):
    nb, nt = shape["blk"], shape["tp"]
    n_tok, width = args[0].shape
    rows = args[2].shape[0]
    qc, kc, oc = args[2].shape[1] // nt, args[3].shape[1] // nt, width // nt
    fits = (nb == 4 and nt == KVH and rows % 32 == 0 and rows <= 160 and qc == 4 * HD and kc == 2 * HD
            and oc == nb * rows and oc % 128 == 0 and width % 128 == 0 and n_tok % 256 == 0)
    if fits:
        return fused(nb, nt, *args)
    return per_device(*args)


def solution(mesh):
    in_specs = (
        P("blk", None),
        P(),
        P(("blk", "tp"), None),
        P(("blk", "tp"), None),
        P(),
        P(),
        P(None, ("blk", "tp")),
        P(),
        P("blk"),
        P("blk"),
    )
    out_specs = P("blk", "tp")
    return jax.shard_map(
        functools.partial(route, dict(mesh.shape)), mesh=mesh, in_specs=in_specs, out_specs=out_specs, check_vma=False
    )
```

```python
import functools

import jax
import jax.numpy as jnp
import numpy as np
from jax import lax
from jax.experimental import pallas as pl
from jax.experimental.pallas import tpu as pltpu
from jax.sharding import PartitionSpec as P

D = 5120
KVH = 8
HD = 128


NORM_FLOOR = 0.0625
ROPE_BASE = 1000000.0
NEGATIVE_FILL = -1e30
LOG2E = 1.4426950408889634


def for_sending(x):
    return jax.tree.map(lambda a: a.astype(jnp.bfloat16) if a.dtype == jnp.float32 else a, x)


def from_partner(block, axis, bit):
    count = lax.axis_size(axis)
    route = []
    for low in range(count):
        high = low | 1 << bit
        if high != low and high < count:
            route += [(low, high), (high, low)]
    return lax.ppermute(block, axis, route)


def rope_tables(positions, head_width):
    half_width = head_width // 2
    frequency = ROPE_BASE ** (-(jnp.arange(half_width, dtype=jnp.float32) * 2.0) / head_width)
    angles = positions.astype(jnp.float32)[:, None] * frequency[None, :]
    angles = jnp.concatenate([angles, angles], axis=1)
    return (jnp.cos(angles), jnp.sin(angles))


def rotate(values, cosine_table, sine_table):
    half_width = values.shape[-1] // 2
    turned = jnp.concatenate([-values[..., half_width:], values[..., :half_width]], axis=-1)
    return values * cosine_table[:, None, :] + turned * sine_table[:, None, :]


def join_pair(mine_cols, partner, is_lower):
    return jnp.where(
        is_lower,
        jnp.concatenate([mine_cols, partner], axis=1),
        jnp.concatenate([partner, mine_cols], axis=1),
    )


def per_device(
    residual_in,
    norm_gain,
    w_query,
    w_key_value,
    query_bias,
    key_value_bias,
    w_output,
    device_map,
    positions,
    segments,
):
    tp_count = lax.axis_size("tp")
    tp_index = lax.axis_index("tp")
    blk_index = lax.axis_index("blk")
    local_tokens = residual_in.shape[0]
    shard_rows = w_query.shape[0]
    kv_group = tp_count // KVH
    floats = residual_in.astype(jnp.float32)
    square = jnp.maximum(jnp.mean(floats * floats, axis=1, keepdims=True), NORM_FLOOR)
    normed = (floats * lax.rsqrt(square) * norm_gain.astype(jnp.float32)).astype(jnp.bfloat16)
    ordered = jnp.take(
        normed.reshape(local_tokens, device_map.shape[0], shard_rows), device_map, axis=1
    ).reshape(local_tokens, D)
    moved_query, moved_pairs = (
        lax.all_to_all(w_query, "tp", split_axis=1, concat_axis=0, tiled=True),
        lax.all_to_all(w_key_value, "tp", split_axis=1, concat_axis=0, tiled=True),
    )
    for bit_level in range(kv_group.bit_length() - 1):
        partner = from_partner(for_sending(moved_pairs), "tp", bit_level).astype(moved_pairs.dtype)
        moved_pairs = join_pair(moved_pairs, partner, tp_index >> bit_level & 1 == 0)
    queries = jnp.dot(
        ordered,
        lax.all_gather(moved_query, "blk", axis=0, tiled=True),
        preferred_element_type=jnp.float32,
    )
    key_value = jnp.dot(
        ordered,
        lax.all_gather(moved_pairs, "blk", axis=0, tiled=True),
        preferred_element_type=jnp.float32,
    )
    query_width = queries.shape[1]
    heads_here = query_width // HD
    kv_head = tp_index // kv_group
    queries = queries + lax.dynamic_slice_in_dim(
        query_bias, tp_index * query_width, query_width
    ).astype(jnp.float32)
    key_value = key_value + lax.dynamic_slice_in_dim(
        key_value_bias, kv_head * 2 * HD, 2 * HD
    ).astype(jnp.float32)
    cosine_table, sine_table = rope_tables(positions, HD)
    query_rot = rotate(
        queries.reshape(local_tokens, heads_here, HD), cosine_table, sine_table
    ).astype(jnp.bfloat16)
    key_rot = rotate(key_value[:, None, :HD], cosine_table, sine_table)[:, 0, :].astype(
        jnp.bfloat16
    )
    values = key_value[:, HD:].astype(jnp.bfloat16)
    attend_scale = HD ** (-0.5)
    row_index = blk_index * local_tokens + jnp.arange(local_tokens, dtype=jnp.int32)
    initial = (
        jnp.full((heads_here, local_tokens), NEGATIVE_FILL, jnp.float32),
        jnp.zeros((heads_here, local_tokens), jnp.float32),
        jnp.zeros((heads_here, local_tokens, HD), jnp.float32),
    )
    key_piece = lax.all_gather(key_rot, "blk", axis=0, tiled=True)
    value_piece = lax.all_gather(values, "blk", axis=0, tiled=True)
    segment_piece = lax.all_gather(segments, "blk", axis=0, tiled=True)
    piece_rows = key_piece.shape[0]
    key_block_rows = 512

    def one_block(block_number, state_now):
        run_peak, run_mass, context = state_now
        block_start = block_number * key_block_rows
        key_block = lax.dynamic_slice_in_dim(key_piece, block_start, key_block_rows, 0)
        value_block = lax.dynamic_slice_in_dim(value_piece, block_start, key_block_rows, 0)
        segment_block = lax.dynamic_slice_in_dim(segment_piece, block_start, key_block_rows, 0)
        scores = (
            jnp.einsum("qhd,kd->hqk", query_rot, key_block, preferred_element_type=jnp.float32)
            * attend_scale
        )
        key_index = block_start + jnp.arange(key_block_rows, dtype=jnp.int32)
        visible = (key_index[None, :] <= row_index[:, None]) & (
            segment_block[None, :] == segments[:, None]
        )
        masked = jnp.where(visible[None], scores, NEGATIVE_FILL)
        new_peak = jnp.maximum(run_peak, jnp.max(masked, axis=2))
        factor = jnp.exp(run_peak - new_peak)
        raw_weights = jnp.where(visible[None], jnp.exp(masked - new_peak[:, :, None]), 0.0)
        run_mass = run_mass * factor + jnp.sum(raw_weights, axis=2)
        context = context * factor[:, :, None] + jnp.einsum(
            "hqk,kd->hqd",
            raw_weights.astype(jnp.bfloat16),
            value_block,
            preferred_element_type=jnp.float32,
        )
        return (new_peak, run_mass, context)

    run_peak, run_mass, context = lax.fori_loop(0, piece_rows // key_block_rows, one_block, initial)
    context_flat = (
        (context / run_mass[:, :, None])
        .transpose(1, 0, 2)
        .reshape(local_tokens, query_width)
        .astype(jnp.bfloat16)
    )
    width_out = D // tp_count
    moved_out = lax.all_to_all(w_output, "tp", split_axis=0, concat_axis=1, tiled=True)
    row_terms = jnp.dot(
        context_flat,
        lax.all_gather(moved_out, "blk", axis=1, tiled=True),
        preferred_element_type=jnp.float32,
    )
    summed = lax.psum_scatter(
        row_terms.astype(jnp.bfloat16), "tp", scatter_dimension=1, tiled=True
    ).astype(jnp.float32)
    residual_part = lax.dynamic_slice_in_dim(residual_in, tp_index * width_out, width_out, 1)
    return (residual_part.astype(jnp.float32) + summed).astype(jnp.bfloat16)


MESH = pl.DeviceIdType.MESH
BF = jnp.bfloat16
F32 = jnp.float32


def flip(i, mask):
    out = i
    for bit in range(mask.bit_length()):
        if mask >> bit & 1:
            out = out + (1 << bit) * (1 - 2 * ((i // (1 << bit)) % 2))
    return out


def fused_kernel(nb, nt, dm_ref, x_hbm, wq_hbm, wkv_hbm, gain_ref, bq_ref, bkv_ref, wo_hbm, inv_ref,
                 pos_ref, seg_ref, out_ref, x_ref, xo, gq, gkv, wo, kv_all, seg_all, qacc,
                 kvacc, qrot, ctx_all, oacc, gain32, bq32, bkv32, cos_t, sin_t, segq_ref,
                 masks, psend, prec, pss, prs,
                 x_sem, loc_sem, kv1s, kv1r, kvxs, kvxr, kvcs, kvcr, q1s, q1r, qxs, qxr, qcs, qcr,
                 w1s, w1r, wxs, wxr, wcs, wcr, es, er, gs, gr, azs, azr, ays, ayr, wrel, rs, rr, r2s):
    b = lax.axis_index("blk")
    t = lax.axis_index("tp")
    n_tok, width = x_ref.shape
    rows = wq_hbm.shape[0]
    qc, kc = gq.shape[2], gkv.shape[2]
    oc = wo.shape[1]
    bx, bc = flip(b, 2), flip(b, 1)

    barrier = pltpu.get_barrier_semaphore()
    peers = [(b, flip(t, k)) for k in range(1, nt)] + [(flip(b, k), t) for k in range(1, nb)]
    peers += [(bx, flip(t, 1))]
    for peer in peers:
        pl.semaphore_signal(barrier, inc=1, device_id=peer, device_id_type=MESH)
    x_in = pltpu.make_async_copy(x_hbm, x_ref, x_sem)
    x_in.start()
    gain32[...] = gain_ref[...].astype(F32)
    bq32[...] = bq_ref[...].astype(F32)
    bkv32[...] = bkv_ref[...].astype(F32)
    with jax.named_scope("barrier"):
        pl.semaphore_wait(barrier, len(peers))

    def remote(src, dst, ss, rs, dev):
        return pltpu.make_async_remote_copy(src_ref=src, dst_ref=dst, send_sem=ss, recv_sem=rs,
                                            device_id=dev, device_id_type=MESH)

    def slot(bb, k):
        return bb * nt + flip(t, k)

    def stage_one(hbm, buf, width, k, ss, rs, local):
        cols = pl.ds(pl.multiple_of(flip(t, k) * width, 128), width)
        mine = buf.at[b * nt + t]
        if k == 0:
            return pltpu.make_async_copy(hbm.at[:, cols], mine, local)
        return remote(hbm.at[:, cols], mine, ss.at[k], rs.at[k], (b, flip(t, k)))

    def stage_one_in(buf, hbm, width, k, ss, rs, local):
        if k == 0:
            return stage_one(hbm, buf, width, 0, ss, rs, local)
        piece = buf.at[slot(b, k)]
        return remote(piece, piece, ss.at[k], rs.at[k], (b, flip(t, k)))

    def forward(buf, bb, k, ss, rs, i, dev):
        piece = buf.at[slot(bb, k)]
        return remote(piece, piece, ss.at[i], rs.at[i], dev)

    kv_set = (wkv_hbm, gkv, kc, kv1s, kv1r, kvxs, kvxr, kvcs, kvcr, loc_sem.at[0])
    q_set = (wq_hbm, gq, qc, q1s, q1r, qxs, qxr, qcs, qcr, loc_sem.at[1])

    order = [0, 1, 2, 4, 3, 6, 5, 7]

    def across(ws, k):
        hbm, buf, width, s1, r1, xs, xr, cs, cr, loc = ws
        cols = pl.ds(pl.multiple_of(flip(t, k) * width, 128), width)
        return remote(hbm.at[:, cols], buf.at[b * nt + t], xs.at[k], xr.at[k], (bx, flip(t, k)))

    def start_one(ws, k):
        hbm, buf, width, s1, r1, xs, xr, cs, cr, loc = ws
        stage_one(hbm, buf, width, k, s1, r1, loc).start()
        if k < 2:
            across(ws, k).start()

    def gather_step(ws, i):
        k = order[i]
        hbm, buf, width, s1, r1, xs, xr, cs, cr, loc = ws
        arrived = stage_one_in(buf, hbm, width, k, s1, r1, loc)
        if k == 0:
            arrived.wait()
        else:
            arrived.wait_recv()
        if k > 1:
            forward(buf, b, k, xs, xr, k, (bx, t)).start()
        forward(buf, b, k, cs, cr, k, (bc, t)).start()

    def gather_cross(ws, i):
        k = order[i]
        hbm, buf, width, s1, r1, xs, xr, cs, cr, loc = ws
        forward(buf, bx, k, xs, xr, k, (bx, t)).wait_recv()
        forward(buf, bx, k, cs, cr, nt + k, (bc, t)).start()

    def gather_last(ws, i):
        k = order[i]
        hbm, buf, width, s1, r1, xs, xr, cs, cr, loc = ws
        forward(buf, bc, k, cs, cr, k, (bc, t)).wait_recv()
        forward(buf, flip(b, 3), k, cs, cr, nt + k, (bc, t)).wait_recv()

    def gather_sent(ws):
        hbm, buf, width, s1, r1, xs, xr, cs, cr, loc = ws
        for k in range(nt):
            if k:
                stage_one(hbm, buf, width, k, s1, r1, loc).wait_send()
            if k < 2:
                across(ws, k).wait_send()
            else:
                forward(buf, b, k, xs, xr, k, (bx, t)).wait_send()
            forward(buf, b, k, cs, cr, k, (bc, t)).wait_send()
            forward(buf, bx, k, cs, cr, nt + k, (bc, t)).wait_send()

    def multiply(buf, acc, i):
        k = order[i]

        def one(j, _):
            s = slot(j, k)
            acc[...] += jnp.dot(xo[dm_ref[s]], buf[s], preferred_element_type=F32)
            return 0
        lax.fori_loop(0, nb, one, 0)

    issue = [0,2,4,1,6,3,5,7]
    for k in issue:
        start_one(kv_set, k)

    x_in.wait()
    tile = n_tok // nt

    def norm_tile(i):
        toks = slice(i * tile, (i + 1) * tile)
        v = x_ref[toks, :].astype(F32)
        scale = lax.rsqrt(jnp.maximum(jnp.mean(v * v, axis=1, keepdims=True), NORM_FLOOR))

        def spread(g, _):
            per = 4 * rows // 128
            gain = jnp.concatenate([gain32[pl.ds(g * per + i, 1), :] for i in range(per)], axis=1)
            u = x_ref[toks, pl.ds(pl.multiple_of(g * 4 * rows, 128), 4 * rows)].astype(F32)
            u = (u * scale * gain).astype(BF)
            for i in range(4):
                xo[g * 4 + i, toks, :] = u[:, i * rows:(i + 1) * rows]
            return 0

        lax.fori_loop(0, nb * nt // 4, spread, 0)

    def tables():
        pos = jnp.broadcast_to(pos_ref[...].astype(F32), (HD, n_tok)).T
        angles = pos * inv_ref[...]
        cos_t[...] = jnp.cos(angles)
        sign = jnp.where(lax.broadcasted_iota(jnp.int32, (1, HD), 1) < HD // 2, -1.0, 1.0)
        sin_t[...] = jnp.sin(angles) * sign
        segq_ref[...] = jnp.broadcast_to(seg_ref[...].astype(F32), (HD, n_tok)).T[:, :1].astype(jnp.int32)

    for k in range(nt):
        with jax.named_scope(f"norm{k}"):
            norm_tile(k)
        with jax.named_scope(f"kvstep{k}"):
            gather_step(kv_set, k)
        if k >= 2:
            start_one(q_set, issue[k - 2])
        if k:
            with jax.named_scope(f"kvcross{k}"):
                gather_cross(kv_set, k - 1)
    for k in range(nt - 2, nt):
        start_one(q_set, issue[k])
    with jax.named_scope("tables"):
        tables()
    with jax.named_scope("kvcross8"):
        gather_cross(kv_set, nt - 1)

    for e in range(2):
        kvacc[:, e * HD:(e + 1) * HD] = jnp.broadcast_to(bkv32[pl.ds(t * 2 + e, 1), :], (n_tok, HD))
    for k in range(4):
        with jax.named_scope(f"qstep{k}"):
            gather_step(q_set, k)
        if k:
            with jax.named_scope(f"qcross{k}"):
                gather_cross(q_set, k - 1)
    for e in range(qc // HD):
        qacc[:, e * HD:(e + 1) * HD] = jnp.broadcast_to(
            bq32[pl.ds(t * (qc // HD) + e, 1), :], (n_tok, HD))
    for e in range(nt):
        gather_last(kv_set, e)
        with jax.named_scope(f"kvmul{e}"):
            multiply(gkv, kvacc, e)
        if e % 2 and 4 + e // 2 < nt:
            k = 4 + e // 2
            with jax.named_scope(f"qstep{k}"):
                gather_step(q_set, k)
            with jax.named_scope(f"qcross{k}"):
                gather_cross(q_set, k - 1)
            if e > 1:
                gather_last(q_set, e // 2 - 1)
                multiply(gq, qacc, e // 2 - 1)

    def rope(u):
        return u * cos_t[...] + pltpu.roll(u, HD // 2, 1) * sin_t[...]

    kv_all[b, :, :HD] = rope(kvacc[:, :HD]).astype(BF)
    kv_all[b, :, HD:] = kvacc[:, HD:].astype(BF)
    seg_all[b] = seg_ref[...]

    def keys(slot_b, sem, dev):
        return (remote(kv_all.at[slot_b], kv_all.at[slot_b], es.at[sem], er.at[sem], dev),
                remote(seg_all.at[slot_b], seg_all.at[slot_b], gs.at[sem], gr.at[sem], dev))

    low = b < nb // 2
    even = b % 2 == 0

    @pl.when(low)
    def _():
        for c in keys(b, 0, (bx, t)):
            c.start()

    @pl.when(even)
    def _():
        for c in keys(b, 1, (bc, t)):
            c.start()

    zi, yy = t // (nt // 2), t % 2
    k_mine = t % nb
    even_core = b % 2

    def wsrc(c):
        return wo_hbm.at[:, pl.ds(pl.multiple_of(c * 2 * qc, 128), 2 * qc)]

    def wpiece(slot, k):
        return wo.at[slot, pl.ds(pl.multiple_of(k * rows, 16), rows), :]

    def mine_or_next(side, owner):
        col = owner * 2 + t // nb
        return (even_core, col) if side == 0 else (1 - even_core, flip(col, 2))

    def straight(side):
        c, dest = mine_or_next(side, b)
        return dest, wsrc(c), wpiece(even_core, k_mine), w1s.at[side]

    def to_relay(side):
        c, _ = mine_or_next(side, bx)
        return remote(wsrc(2 + c), wrel.at[side], rs.at[side], rr.at[side], (bx, t))

    def from_relay(side):
        _, dest = mine_or_next(side, bx)
        return dest, wrel.at[side], wpiece(2 + even_core, k_mine), r2s.at[side]

    def deliver(what):
        dest, src, dst, ss = what

        @pl.when(dest != t)
        def _():
            remote(src, dst, ss, w1r.at[k_mine], (b, dest)).start()

        @pl.when(dest == t)
        def _():
            pltpu.make_async_copy(src, dst, w1r.at[k_mine]).start()

    def delivered(what):
        dest, src, dst, ss = what

        @pl.when(dest != t)
        def _():
            remote(src, dst, ss, w1r.at[k_mine], (b, dest)).wait_send()

    def w_start():
        for side in range(2):
            to_relay(side).start()
        for side in range(2):
            deliver(straight(side))

    def w_relay():
        for side in range(2):
            to_relay(side).wait_recv()
            deliver(from_relay(side))

    def whalf(bb, k):
        return wpiece(2 * ((bb // 2 + zi) % 2) + bb % 2, k)

    def w_x(bb, k):
        return remote(whalf(bb, k), whalf(bb, k), wxs.at[k], wxr.at[k], (bx, t))

    def w_c(bb, i, k):
        return remote(whalf(bb, k), whalf(bb, k), wcs.at[i, k], wcr.at[i, k], (bc, t))

    def w_home(k):
        remote(whalf(b, k), whalf(b, k), w1s.at[0], w1r.at[k], (bx, t)).wait_recv()
        w_x(b, k).start()
        w_c(b, 0, k).start()

    def w_cross(k):
        w_x(bx, k).wait_recv()
        w_c(bx, 1, k).start()

    def w_last(k):
        w_c(bc, 0, k).wait_recv()
        w_c(flip(b, 3), 1, k).wait_recv()

    for k in range(8, nt):
        with jax.named_scope(f"qstep{k}"):
            gather_step(q_set, k)
        with jax.named_scope(f"qcross{k}"):
            gather_cross(q_set, k - 1)
    w_start()
    for e in range(nt // 2 - 1, nt):
        if e == nt - 3:
            with jax.named_scope("qcross8"):
                gather_cross(q_set, nt - 1)
        with jax.named_scope(f"qlast{e}"):
            gather_last(q_set, e)
        with jax.named_scope(f"qmul{e}"):
            multiply(gq, qacc, e)

    for h in range(qc // HD):
        cols = slice(h * HD, (h + 1) * HD)
        qrot[:, cols] = rope(qacc[:, cols]).astype(BF)

    @pl.when(b >= nb // 2)
    def _():
        for c in keys(bx, 0, (bx, t)):
            c.wait_recv()
        for c in keys(bx, 2, (bc, t)):
            c.start()
        for c in keys(flip(b, 3), 2, (bc, t)):
            c.wait_recv()

    @pl.when(b % 2 == 1)
    def _():
        for c in keys(bc, 1, (bc, t)):
            c.wait_recv()

    n_part = ctx_all.shape[1]
    qrows = n_tok // n_part
    scale = HD ** (-0.5) * LOG2E
    across_qk = (((1,), (1,)), ((), ()))

    def mask_part(part):
        r0 = part * qrows
        sq = segq_ref[r0:r0 + qrows, :]
        seen = r0 + qrows
        ri = r0 + lax.broadcasted_iota(jnp.int32, (qrows, seen), 0)
        ci = lax.broadcasted_iota(jnp.int32, (qrows, seen), 1)
        vis = (ci <= ri) & (seg_all[b][:, :seen] == sq)
        masks[nb - 1, :, :seen] = jnp.where(vis, 0.0, NEGATIVE_FILL)

        def earlier(j, _):
            masks[j] = jnp.where(seg_all[j] == sq, jnp.zeros((qrows, n_tok), F32), NEGATIVE_FILL)
            return 0

        lax.fori_loop(0, b, earlier, 0)

    def attend(h, part):
        r0 = part * qrows
        seen = r0 + qrows
        qh = qrot[r0:r0 + qrows, h * HD:(h + 1) * HD]

        def scored(kb, mask):
            return lax.dot_general(qh, kb, across_qk, preferred_element_type=F32) * scale + mask

        s = scored(kv_all[b, :seen, :HD], masks[nb - 1, :, :seen])
        m = jnp.max(s, axis=1, keepdims=True)
        p = jnp.exp2(s - m)
        l = jnp.sum(p, axis=1, keepdims=True)
        c = jnp.dot(p.astype(BF), kv_all[b, :seen, HD:], preferred_element_type=F32)

        def block(j, st):
            m, l, c = st
            s = scored(kv_all[j, :, :HD], masks[j])
            m2 = jnp.maximum(m, jnp.max(s, axis=1, keepdims=True))
            f = jnp.exp2(m - m2)
            p = jnp.exp2(s - m2)
            l = l * f + jnp.sum(p, axis=1, keepdims=True)
            c = c * f + jnp.dot(p.astype(BF), kv_all[j, :, HD:], preferred_element_type=F32)
            return (m2, l, c)

        m, l, c = lax.fori_loop(0, b, block, (m, l, c))
        return (c / l).astype(BF)

    def cpiece(z_half, y_side, part):
        return ctx_all.at[z_half, part, :, pl.ds(pl.multiple_of(y_side * qc, 128), qc)]

    def az(z_half, part):
        piece = cpiece(z_half, yy, part)
        return remote(piece, piece, azs.at[part], azr.at[part], (b, flip(t, nt // 2)))

    def ay(z_half, y_side, part, i):
        piece = cpiece(z_half, y_side, part)
        return remote(piece, piece, ays.at[part, i], ayr.at[part, i], (b, flip(t, 1)))

    def relay_ctx(part):
        az(1 - zi, part).wait_recv()
        ay(1 - zi, yy, part, 1).start()

    def partial(part, slot_side):
        acc = None
        for zh in range(2):
            one = lax.dot_general(ctx_all[zh, part], wo[2 * zh + slot_side], across_qk,
                                  preferred_element_type=F32)
            acc = one if acc is None else acc + one
        return acc

    z_low = (t // 2) % 2

    def pcopy(part):
        return remote(psend.at[part], prec.at[part], pss.at[part], prs.at[part], (b, flip(t, 2)))

    def project(part):
        psend[part] = partial(part, 1 - z_low).astype(BF)
        pcopy(part).start()
        toks = slice(part * qrows, (part + 1) * qrows)
        resid = x_ref[toks, pl.ds(pl.multiple_of(t * oc, 128), oc)].astype(F32)
        oacc[toks, :] = resid + partial(part, z_low)

    for part in range(n_part):
        with jax.named_scope(f"mask{part}"):
            mask_part(part)
        for h in range(qc // HD):
            with jax.named_scope(f"att{part}{h}"):
                col = pl.ds(pl.multiple_of(yy * qc + h * HD, 128), HD)
                ctx_all[zi, part, :, col] = attend(h, part)
            if part == 0 and h == 1:
                with jax.named_scope("wrelay"):
                    w_relay()
        az(zi, part).start()
        ay(zi, yy, part, 0).start()

    with jax.named_scope("ctxrelay0"):
        relay_ctx(0)
    for k in range(nb):
        with jax.named_scope(f"whome{k}"):
            w_home(k)
        if k:
            with jax.named_scope(f"wcross{k - 1}"):
                w_cross(k - 1)
    with jax.named_scope("ctxrelay1"):
        relay_ctx(1)
    with jax.named_scope(f"wcross{nb - 1}"):
        w_cross(nb - 1)
    for k in range(nb):
        with jax.named_scope(f"wlast{k}"):
            w_last(k)
    for part in range(n_part):
        with jax.named_scope(f"ctxy{part}"):
            ay(zi, 1 - yy, part, 0).wait_recv()
            ay(1 - zi, 1 - yy, part, 1).wait_recv()
        with jax.named_scope(f"project{part}"):
            project(part)
    for part in range(n_part):
        with jax.named_scope(f"prec{part}"):
            pcopy(part).wait_recv()
        toks = slice(part * qrows, (part + 1) * qrows)
        out_ref[toks, :] = (oacc[toks, :] + prec[part].astype(F32)).astype(BF)

    gather_sent(kv_set)
    gather_sent(q_set)

    @pl.when(low)
    def _():
        for c in keys(b, 0, (bx, t)):
            c.wait_send()

    @pl.when(even)
    def _():
        for c in keys(b, 1, (bc, t)):
            c.wait_send()

    @pl.when(b >= nb // 2)
    def _():
        for c in keys(bx, 2, (bc, t)):
            c.wait_send()

    for side in range(2):
        to_relay(side).wait_send()
        delivered(straight(side))
        delivered(from_relay(side))
    for k in range(nb):
        w_x(b, k).wait_send()
        w_c(b, 0, k).wait_send()
        w_c(bx, 1, k).wait_send()
    for part in range(n_part):
        az(zi, part).wait_send()
        ay(zi, yy, part, 0).wait_send()
        ay(1 - zi, yy, part, 1).wait_send()
        pcopy(part).wait_send()


def fused(nb, nt, residual_in, norm_gain, w_query, w_key_value, query_bias, key_value_bias, w_output,
          device_map, positions, segments):
    n_tok, width = residual_in.shape
    rows = w_query.shape[0]
    qc, kc, oc = w_query.shape[1] // nt, w_key_value.shape[1] // nt, width // nt
    n = nb * nt
    inv = ROPE_BASE ** (-(np.arange(HD // 2, dtype=np.float64) * 2.0) / HD)
    inv = np.concatenate([inv, inv]).astype(np.float32)[None, :]
    any_, vm = pl.BlockSpec(memory_space=pl.ANY), pl.BlockSpec(memory_space=pltpu.VMEM)
    dma = pltpu.SemaphoreType.DMA
    return pl.pallas_call(
        functools.partial(fused_kernel, nb, nt),
        out_shape=jax.ShapeDtypeStruct((n_tok, oc), BF),
        in_specs=[pl.BlockSpec(memory_space=pltpu.SMEM), any_, any_, any_, vm, vm, vm, any_, vm, vm, vm],
        out_specs=vm,
        scratch_shapes=[
            pltpu.VMEM((n_tok, width), BF),
            pltpu.VMEM((n, n_tok, rows), BF),
            pltpu.VMEM((n, rows, qc), BF),
            pltpu.VMEM((n, rows, kc), BF),
            pltpu.VMEM((nb, oc, 2 * qc), BF),
            pltpu.VMEM((nb, n_tok, kc), BF),
            pltpu.VMEM((nb, 1, n_tok), jnp.int32),
            pltpu.VMEM((n_tok, qc), F32),
            pltpu.VMEM((n_tok, kc), F32),
            pltpu.VMEM((n_tok, qc), BF),
            pltpu.VMEM((2, 2, n_tok // 2, 2 * qc), BF),
            pltpu.VMEM((n_tok, oc), F32),
            pltpu.VMEM((width // 128, 128), F32), pltpu.VMEM((qc * nt // HD, HD), F32),
            pltpu.VMEM((kc * nt // HD, HD), F32), pltpu.VMEM((n_tok, HD), F32),
            pltpu.VMEM((n_tok, HD), F32), pltpu.VMEM((n_tok, 1), jnp.int32),
            pltpu.VMEM((nb, n_tok // 2, n_tok), F32), pltpu.VMEM((2, n_tok // 2, oc), BF),
            pltpu.VMEM((2, n_tok // 2, oc), BF), dma((2,)), dma((2,)),
            dma, dma((3,)),
            dma((nt,)), dma((nt,)), dma((nt,)), dma((nt,)), dma((2 * nt,)), dma((2 * nt,)),
            dma((nt,)), dma((nt,)), dma((nt,)), dma((nt,)), dma((2 * nt,)), dma((2 * nt,)),
            dma((2,)), dma((nb,)), dma((nb,)), dma((nb,)), dma((2, nb)), dma((2, nb)),
            dma((nb,)), dma((nb,)), dma((nb,)), dma((nb,)),
            dma((2,)), dma((2,)), dma((2, 2)), dma((2, 2)),
            pltpu.VMEM((2, rows, 2 * qc), BF), dma((2,)), dma((2,)), dma((2,)),
        ],
        compiler_params=pltpu.CompilerParams(
            collective_id=0, has_side_effects=True, vmem_limit_bytes=63 * 1024 * 1024),
    )(device_map, residual_in, w_query, w_key_value, norm_gain.reshape(-1, 128), query_bias.reshape(-1, HD),
      key_value_bias.reshape(-1, HD), w_output.T, jnp.asarray(inv), positions[None, :], segments[None, :])


def route(shape, *args):
    nb, nt = shape["blk"], shape["tp"]
    n_tok, width = args[0].shape
    rows = args[2].shape[0]
    qc, kc, oc = args[2].shape[1] // nt, args[3].shape[1] // nt, width // nt
    fits = (nb == 4 and nt == KVH and rows % 32 == 0 and rows <= 160 and qc == 4 * HD and kc == 2 * HD
            and oc == nb * rows and oc % 128 == 0 and width % 128 == 0 and n_tok % 256 == 0)
    if fits:
        return fused(nb, nt, *args)
    return per_device(*args)


def solution(mesh):
    in_specs = (
        P("blk", None),
        P(),
        P(("blk", "tp"), None),
        P(("blk", "tp"), None),
        P(),
        P(),
        P(None, ("blk", "tp")),
        P(),
        P("blk"),
        P("blk"),
    )
    out_specs = P("blk", "tp")
    return jax.shard_map(
        functools.partial(route, dict(mesh.shape)), mesh=mesh, in_specs=in_specs, out_specs=out_specs, check_vma=False
    )
```

```python
import functools

import jax
import jax.numpy as jnp
import numpy as np
from jax import lax
from jax.experimental import pallas as pl
from jax.experimental.pallas import tpu as pltpu
from jax.sharding import PartitionSpec as P

D = 5120
KVH = 8
HD = 128


NORM_FLOOR = 0.0625
ROPE_BASE = 1000000.0
NEGATIVE_FILL = -1e30
LOG2E = 1.4426950408889634


def for_sending(x):
    return jax.tree.map(lambda a: a.astype(jnp.bfloat16) if a.dtype == jnp.float32 else a, x)


def from_partner(block, axis, bit):
    count = lax.axis_size(axis)
    route = []
    for low in range(count):
        high = low | 1 << bit
        if high != low and high < count:
            route += [(low, high), (high, low)]
    return lax.ppermute(block, axis, route)


def rope_tables(positions, head_width):
    half_width = head_width // 2
    frequency = ROPE_BASE ** (-(jnp.arange(half_width, dtype=jnp.float32) * 2.0) / head_width)
    angles = positions.astype(jnp.float32)[:, None] * frequency[None, :]
    angles = jnp.concatenate([angles, angles], axis=1)
    return (jnp.cos(angles), jnp.sin(angles))


def rotate(values, cosine_table, sine_table):
    half_width = values.shape[-1] // 2
    turned = jnp.concatenate([-values[..., half_width:], values[..., :half_width]], axis=-1)
    return values * cosine_table[:, None, :] + turned * sine_table[:, None, :]


def join_pair(mine_cols, partner, is_lower):
    return jnp.where(
        is_lower,
        jnp.concatenate([mine_cols, partner], axis=1),
        jnp.concatenate([partner, mine_cols], axis=1),
    )


def per_device(
    residual_in,
    norm_gain,
    w_query,
    w_key_value,
    query_bias,
    key_value_bias,
    w_output,
    device_map,
    positions,
    segments,
):
    tp_count = lax.axis_size("tp")
    tp_index = lax.axis_index("tp")
    blk_index = lax.axis_index("blk")
    local_tokens = residual_in.shape[0]
    shard_rows = w_query.shape[0]
    kv_group = tp_count // KVH
    floats = residual_in.astype(jnp.float32)
    square = jnp.maximum(jnp.mean(floats * floats, axis=1, keepdims=True), NORM_FLOOR)
    normed = (floats * lax.rsqrt(square) * norm_gain.astype(jnp.float32)).astype(jnp.bfloat16)
    ordered = jnp.take(
        normed.reshape(local_tokens, device_map.shape[0], shard_rows), device_map, axis=1
    ).reshape(local_tokens, D)
    moved_query, moved_pairs = (
        lax.all_to_all(w_query, "tp", split_axis=1, concat_axis=0, tiled=True),
        lax.all_to_all(w_key_value, "tp", split_axis=1, concat_axis=0, tiled=True),
    )
    for bit_level in range(kv_group.bit_length() - 1):
        partner = from_partner(for_sending(moved_pairs), "tp", bit_level).astype(moved_pairs.dtype)
        moved_pairs = join_pair(moved_pairs, partner, tp_index >> bit_level & 1 == 0)
    queries = jnp.dot(
        ordered,
        lax.all_gather(moved_query, "blk", axis=0, tiled=True),
        preferred_element_type=jnp.float32,
    )
    key_value = jnp.dot(
        ordered,
        lax.all_gather(moved_pairs, "blk", axis=0, tiled=True),
        preferred_element_type=jnp.float32,
    )
    query_width = queries.shape[1]
    heads_here = query_width // HD
    kv_head = tp_index // kv_group
    queries = queries + lax.dynamic_slice_in_dim(
        query_bias, tp_index * query_width, query_width
    ).astype(jnp.float32)
    key_value = key_value + lax.dynamic_slice_in_dim(
        key_value_bias, kv_head * 2 * HD, 2 * HD
    ).astype(jnp.float32)
    cosine_table, sine_table = rope_tables(positions, HD)
    query_rot = rotate(
        queries.reshape(local_tokens, heads_here, HD), cosine_table, sine_table
    ).astype(jnp.bfloat16)
    key_rot = rotate(key_value[:, None, :HD], cosine_table, sine_table)[:, 0, :].astype(
        jnp.bfloat16
    )
    values = key_value[:, HD:].astype(jnp.bfloat16)
    attend_scale = HD ** (-0.5)
    row_index = blk_index * local_tokens + jnp.arange(local_tokens, dtype=jnp.int32)
    initial = (
        jnp.full((heads_here, local_tokens), NEGATIVE_FILL, jnp.float32),
        jnp.zeros((heads_here, local_tokens), jnp.float32),
        jnp.zeros((heads_here, local_tokens, HD), jnp.float32),
    )
    key_piece = lax.all_gather(key_rot, "blk", axis=0, tiled=True)
    value_piece = lax.all_gather(values, "blk", axis=0, tiled=True)
    segment_piece = lax.all_gather(segments, "blk", axis=0, tiled=True)
    piece_rows = key_piece.shape[0]
    key_block_rows = 512

    def one_block(block_number, state_now):
        run_peak, run_mass, context = state_now
        block_start = block_number * key_block_rows
        key_block = lax.dynamic_slice_in_dim(key_piece, block_start, key_block_rows, 0)
        value_block = lax.dynamic_slice_in_dim(value_piece, block_start, key_block_rows, 0)
        segment_block = lax.dynamic_slice_in_dim(segment_piece, block_start, key_block_rows, 0)
        scores = (
            jnp.einsum("qhd,kd->hqk", query_rot, key_block, preferred_element_type=jnp.float32)
            * attend_scale
        )
        key_index = block_start + jnp.arange(key_block_rows, dtype=jnp.int32)
        visible = (key_index[None, :] <= row_index[:, None]) & (
            segment_block[None, :] == segments[:, None]
        )
        masked = jnp.where(visible[None], scores, NEGATIVE_FILL)
        new_peak = jnp.maximum(run_peak, jnp.max(masked, axis=2))
        factor = jnp.exp(run_peak - new_peak)
        raw_weights = jnp.where(visible[None], jnp.exp(masked - new_peak[:, :, None]), 0.0)
        run_mass = run_mass * factor + jnp.sum(raw_weights, axis=2)
        context = context * factor[:, :, None] + jnp.einsum(
            "hqk,kd->hqd",
            raw_weights.astype(jnp.bfloat16),
            value_block,
            preferred_element_type=jnp.float32,
        )
        return (new_peak, run_mass, context)

    run_peak, run_mass, context = lax.fori_loop(0, piece_rows // key_block_rows, one_block, initial)
    context_flat = (
        (context / run_mass[:, :, None])
        .transpose(1, 0, 2)
        .reshape(local_tokens, query_width)
        .astype(jnp.bfloat16)
    )
    width_out = D // tp_count
    moved_out = lax.all_to_all(w_output, "tp", split_axis=0, concat_axis=1, tiled=True)
    row_terms = jnp.dot(
        context_flat,
        lax.all_gather(moved_out, "blk", axis=1, tiled=True),
        preferred_element_type=jnp.float32,
    )
    summed = lax.psum_scatter(
        row_terms.astype(jnp.bfloat16), "tp", scatter_dimension=1, tiled=True
    ).astype(jnp.float32)
    residual_part = lax.dynamic_slice_in_dim(residual_in, tp_index * width_out, width_out, 1)
    return (residual_part.astype(jnp.float32) + summed).astype(jnp.bfloat16)


MESH = pl.DeviceIdType.MESH
BF = jnp.bfloat16
F32 = jnp.float32


def flip(i, mask):
    out = i
    for bit in range(mask.bit_length()):
        if mask >> bit & 1:
            out = out + (1 << bit) * (1 - 2 * ((i // (1 << bit)) % 2))
    return out


def fused_kernel(nb, nt, dm_ref, x_hbm, wq_hbm, wkv_hbm, gain_ref, bq_ref, bkv_ref, wo_hbm, inv_ref,
                 pos_ref, seg_ref, out_ref, x_ref, xo, gq, gkv, wo, kv_all, seg_all, qacc,
                 kvacc, qrot, ctx_all, oacc, gain32, bq32, bkv32, cos_t, sin_t, segq_ref,
                 masks, psend, prec, pss, prs,
                 x_sem, loc_sem, kv1s, kv1r, kvxs, kvxr, kvcs, kvcr, q1s, q1r, qxs, qxr, qcs, qcr,
                 w1s, w1r, wxs, wxr, wcs, wcr, es, er, gs, gr, azs, azr, ays, ayr, wrel, rs, rr, r2s):
    b = lax.axis_index("blk")
    t = lax.axis_index("tp")
    n_tok, width = x_ref.shape
    rows = wq_hbm.shape[0]
    qc, kc = gq.shape[2], gkv.shape[2]
    oc = wo.shape[1]
    bx, bc = flip(b, 2), flip(b, 1)

    barrier = pltpu.get_barrier_semaphore()
    peers = [(b, flip(t, k)) for k in range(1, nt)] + [(flip(b, k), t) for k in range(1, nb)]
    peers += [(bx, flip(t, 1))]
    for peer in peers:
        pl.semaphore_signal(barrier, inc=1, device_id=peer, device_id_type=MESH)
    x_in = pltpu.make_async_copy(x_hbm, x_ref, x_sem)
    x_in.start()
    gain32[...] = gain_ref[...].astype(F32)
    bq32[...] = bq_ref[...].astype(F32)
    bkv32[...] = bkv_ref[...].astype(F32)
    with jax.named_scope("barrier"):
        pl.semaphore_wait(barrier, len(peers))

    def remote(src, dst, ss, rs, dev):
        return pltpu.make_async_remote_copy(src_ref=src, dst_ref=dst, send_sem=ss, recv_sem=rs,
                                            device_id=dev, device_id_type=MESH)

    def slot(bb, k):
        return bb * nt + flip(t, k)

    def stage_one(hbm, buf, width, k, ss, rs, local):
        cols = pl.ds(pl.multiple_of(flip(t, k) * width, 128), width)
        mine = buf.at[b * nt + t]
        if k == 0:
            return pltpu.make_async_copy(hbm.at[:, cols], mine, local)
        return remote(hbm.at[:, cols], mine, ss.at[k], rs.at[k], (b, flip(t, k)))

    def stage_one_in(buf, hbm, width, k, ss, rs, local):
        if k == 0:
            return stage_one(hbm, buf, width, 0, ss, rs, local)
        piece = buf.at[slot(b, k)]
        return remote(piece, piece, ss.at[k], rs.at[k], (b, flip(t, k)))

    def forward(buf, bb, k, ss, rs, i, dev):
        piece = buf.at[slot(bb, k)]
        return remote(piece, piece, ss.at[i], rs.at[i], dev)

    kv_set = (wkv_hbm, gkv, kc, kv1s, kv1r, kvxs, kvxr, kvcs, kvcr, loc_sem.at[0])
    q_set = (wq_hbm, gq, qc, q1s, q1r, qxs, qxr, qcs, qcr, loc_sem.at[1])

    order = [0, 1, 2, 4, 3, 6, 5, 7]

    def across(ws, k):
        hbm, buf, width, s1, r1, xs, xr, cs, cr, loc = ws
        cols = pl.ds(pl.multiple_of(flip(t, k) * width, 128), width)
        return remote(hbm.at[:, cols], buf.at[b * nt + t], xs.at[k], xr.at[k], (bx, flip(t, k)))

    def start_one(ws, k):
        hbm, buf, width, s1, r1, xs, xr, cs, cr, loc = ws
        stage_one(hbm, buf, width, k, s1, r1, loc).start()
        if k < 2:
            across(ws, k).start()

    def gather_step(ws, i):
        k = order[i]
        hbm, buf, width, s1, r1, xs, xr, cs, cr, loc = ws
        arrived = stage_one_in(buf, hbm, width, k, s1, r1, loc)
        if k == 0:
            arrived.wait()
        else:
            arrived.wait_recv()
        if k > 1:
            forward(buf, b, k, xs, xr, k, (bx, t)).start()
        forward(buf, b, k, cs, cr, k, (bc, t)).start()

    def gather_cross(ws, i):
        k = order[i]
        hbm, buf, width, s1, r1, xs, xr, cs, cr, loc = ws
        forward(buf, bx, k, xs, xr, k, (bx, t)).wait_recv()
        forward(buf, bx, k, cs, cr, nt + k, (bc, t)).start()

    def gather_last(ws, i):
        k = order[i]
        hbm, buf, width, s1, r1, xs, xr, cs, cr, loc = ws
        forward(buf, bc, k, cs, cr, k, (bc, t)).wait_recv()
        forward(buf, flip(b, 3), k, cs, cr, nt + k, (bc, t)).wait_recv()

    def gather_sent(ws):
        hbm, buf, width, s1, r1, xs, xr, cs, cr, loc = ws
        for k in range(nt):
            if k:
                stage_one(hbm, buf, width, k, s1, r1, loc).wait_send()
            if k < 2:
                across(ws, k).wait_send()
            else:
                forward(buf, b, k, xs, xr, k, (bx, t)).wait_send()
            forward(buf, b, k, cs, cr, k, (bc, t)).wait_send()
            forward(buf, bx, k, cs, cr, nt + k, (bc, t)).wait_send()

    def multiply(buf, acc, i):
        k = order[i]

        def one(j, _):
            s = slot(j, k)
            acc[...] += jnp.dot(xo[dm_ref[s]], buf[s], preferred_element_type=F32)
            return 0
        lax.fori_loop(0, nb, one, 0)

    issue = [0,2,4,1,6,3,5,7]
    for k in issue:
        start_one(kv_set, k)

    x_in.wait()
    tile = n_tok // nt

    def norm_tile(i):
        toks = slice(i * tile, (i + 1) * tile)
        v = x_ref[toks, :].astype(F32)
        scale = lax.rsqrt(jnp.maximum(jnp.mean(v * v, axis=1, keepdims=True), NORM_FLOOR))

        def spread(g, _):
            per = 4 * rows // 128
            gain = jnp.concatenate([gain32[pl.ds(g * per + i, 1), :] for i in range(per)], axis=1)
            u = x_ref[toks, pl.ds(pl.multiple_of(g * 4 * rows, 128), 4 * rows)].astype(F32)
            u = (u * scale * gain).astype(BF)
            for i in range(4):
                xo[g * 4 + i, toks, :] = u[:, i * rows:(i + 1) * rows]
            return 0

        lax.fori_loop(0, nb * nt // 4, spread, 0)

    def tables():
        pos = jnp.broadcast_to(pos_ref[...].astype(F32), (HD, n_tok)).T
        angles = pos * inv_ref[...]
        cos_t[...] = jnp.cos(angles)
        sign = jnp.where(lax.broadcasted_iota(jnp.int32, (1, HD), 1) < HD // 2, -1.0, 1.0)
        sin_t[...] = jnp.sin(angles) * sign
        segq_ref[...] = jnp.broadcast_to(seg_ref[...].astype(F32), (HD, n_tok)).T[:, :1].astype(jnp.int32)

    zi, yy = t // (nt // 2), t % 2
    k_mine = t % nb
    even_core = b % 2

    def wsrc(c, i):
        return wo_hbm.at[:, pl.ds(pl.multiple_of((c * 2 + i) * qc, 128), qc)]

    def wpiece(slot, k, i):
        return wo.at[slot, pl.ds(pl.multiple_of(k * rows, 16), rows), i * qc:(i + 1) * qc]

    def mine_or_next(side, owner):
        col = owner * 2 + t // nb
        return (even_core, col) if side == 0 else (1 - even_core, flip(col, 2))

    def straight(side, i):
        c, dest = mine_or_next(side, b)
        return dest, wsrc(c, i), wpiece(even_core, k_mine, i), w1s.at[side, i], w1r.at[k_mine, i]

    def to_relay(side, i):
        c, _ = mine_or_next(side, bx)
        return remote(wsrc(2 + c, i), wrel.at[side, i], rs.at[side, i], rr.at[side, i], (bx, t))

    def from_relay(side, i):
        _, dest = mine_or_next(side, bx)
        return dest, wrel.at[side, i], wpiece(2 + even_core, k_mine, i), r2s.at[side, i], w1r.at[k_mine, i]

    def deliver(what):
        dest, src, dst, ss, sr = what

        @pl.when(dest != t)
        def _():
            remote(src, dst, ss, sr, (b, dest)).start()

        @pl.when(dest == t)
        def _():
            pltpu.make_async_copy(src, dst, sr).start()

    def delivered(what):
        dest, src, dst, ss, sr = what

        @pl.when(dest != t)
        def _():
            remote(src, dst, ss, sr, (b, dest)).wait_send()

    def whalf(bb, k, i):
        return wpiece(2 * ((bb // 2 + zi) % 2) + bb % 2, k, i)

    def w_x(bb, k, i):
        return remote(whalf(bb, k, i), whalf(bb, k, i), wxs.at[k, i], wxr.at[k, i], (bx, t))

    def w_c(bb, u, k, i):
        return remote(whalf(bb, k, i), whalf(bb, k, i), wcs.at[u, k, i], wcr.at[u, k, i], (bc, t))

    def w_home(k, i):
        remote(whalf(b, k, i), whalf(b, k, i), w1s.at[0, i], w1r.at[k, i], (bx, t)).wait_recv()
        w_x(b, k, i).start()
        w_c(b, 0, k, i).start()

    def w_cross(k, i):
        w_x(bx, k, i).wait_recv()
        w_c(bx, 1, k, i).start()

    def w_last(k, i):
        w_c(bc, 0, k, i).wait_recv()
        w_c(flip(b, 3), 1, k, i).wait_recv()

    def w_straight():
        for i in range(2):
            for side in range(2):
                deliver(straight(side, i))

    def w_start():
        for i in range(2):
            for side in range(2):
                to_relay(side, i).start()

    def w_relay(side, i):
        to_relay(side, i).wait_recv()
        deliver(from_relay(side, i))

    def relays(i):
        for side in range(2):
            with jax.named_scope(f"wrelay{i}{side}"):
                w_relay(side, i)

    for k in range(nt):
        with jax.named_scope(f"norm{k}"):
            norm_tile(k)
        with jax.named_scope(f"kvstep{k}"):
            gather_step(kv_set, k)
        if k >= 2:
            start_one(q_set, issue[k - 2])
        if k == 5:
            w_start()
        if k:
            with jax.named_scope(f"kvcross{k}"):
                gather_cross(kv_set, k - 1)
    for k in range(nt - 2, nt):
        start_one(q_set, issue[k])
    with jax.named_scope("tables"):
        tables()
    with jax.named_scope("kvcross8"):
        gather_cross(kv_set, nt - 1)

    for e in range(2):
        kvacc[:, e * HD:(e + 1) * HD] = jnp.broadcast_to(bkv32[pl.ds(t * 2 + e, 1), :], (n_tok, HD))
    for k in range(4):
        with jax.named_scope(f"qstep{k}"):
            gather_step(q_set, k)
        if k:
            with jax.named_scope(f"qcross{k}"):
                gather_cross(q_set, k - 1)
    for e in range(qc // HD):
        qacc[:, e * HD:(e + 1) * HD] = jnp.broadcast_to(
            bq32[pl.ds(t * (qc // HD) + e, 1), :], (n_tok, HD))
    for e in range(nt):
        gather_last(kv_set, e)
        with jax.named_scope(f"kvmul{e}"):
            multiply(gkv, kvacc, e)
        if e % 2 and 4 + e // 2 < nt:
            k = 4 + e // 2
            with jax.named_scope(f"qstep{k}"):
                gather_step(q_set, k)
            with jax.named_scope(f"qcross{k}"):
                gather_cross(q_set, k - 1)
            if k == 6:
                w_straight()
            if k == 5:
                relays(0)
            if k == 7:
                relays(1)
            if e > 1:
                gather_last(q_set, e // 2 - 1)
                multiply(gq, qacc, e // 2 - 1)

    def rope(u):
        return u * cos_t[...] + pltpu.roll(u, HD // 2, 1) * sin_t[...]

    kv_all[b, :, :HD] = rope(kvacc[:, :HD]).astype(BF)
    kv_all[b, :, HD:] = kvacc[:, HD:].astype(BF)
    seg_all[b] = seg_ref[...]

    def keys(slot_b, sem, dev):
        return (remote(kv_all.at[slot_b], kv_all.at[slot_b], es.at[sem], er.at[sem], dev),
                remote(seg_all.at[slot_b], seg_all.at[slot_b], gs.at[sem], gr.at[sem], dev))

    low = b < nb // 2
    even = b % 2 == 0

    @pl.when(low)
    def _():
        for c in keys(b, 0, (bx, t)):
            c.start()

    @pl.when(even)
    def _():
        for c in keys(b, 1, (bc, t)):
            c.start()

    for k in range(8, nt):
        with jax.named_scope(f"qstep{k}"):
            gather_step(q_set, k)
        with jax.named_scope(f"qcross{k}"):
            gather_cross(q_set, k - 1)
    for e in range(nt // 2 - 1, nt):
        if e == nt - 3:
            with jax.named_scope("qcross8"):
                gather_cross(q_set, nt - 1)
        with jax.named_scope(f"qlast{e}"):
            gather_last(q_set, e)
        with jax.named_scope(f"qmul{e}"):
            multiply(gq, qacc, e)

    for h in range(qc // HD):
        cols = slice(h * HD, (h + 1) * HD)
        qrot[:, cols] = rope(qacc[:, cols]).astype(BF)

    @pl.when(b >= nb // 2)
    def _():
        for c in keys(bx, 0, (bx, t)):
            c.wait_recv()
        for c in keys(bx, 2, (bc, t)):
            c.start()
        for c in keys(flip(b, 3), 2, (bc, t)):
            c.wait_recv()

    @pl.when(b % 2 == 1)
    def _():
        for c in keys(bc, 1, (bc, t)):
            c.wait_recv()

    n_part = ctx_all.shape[1]
    qrows = n_tok // n_part
    scale = HD ** (-0.5) * LOG2E
    across_qk = (((1,), (1,)), ((), ()))

    def mask_part(part):
        r0 = part * qrows
        sq = segq_ref[r0:r0 + qrows, :]
        seen = r0 + qrows
        ri = r0 + lax.broadcasted_iota(jnp.int32, (qrows, seen), 0)
        ci = lax.broadcasted_iota(jnp.int32, (qrows, seen), 1)
        vis = (ci <= ri) & (seg_all[b][:, :seen] == sq)
        masks[nb - 1, :, :seen] = jnp.where(vis, 0.0, NEGATIVE_FILL)

        def earlier(j, _):
            masks[j] = jnp.where(seg_all[j] == sq, jnp.zeros((qrows, n_tok), F32), NEGATIVE_FILL)
            return 0

        lax.fori_loop(0, b, earlier, 0)

    def attend(h, part):
        r0 = part * qrows
        seen = r0 + qrows
        qh = qrot[r0:r0 + qrows, h * HD:(h + 1) * HD]

        def scored(kb, mask):
            return lax.dot_general(qh, kb, across_qk, preferred_element_type=F32) * scale + mask

        s = scored(kv_all[b, :seen, :HD], masks[nb - 1, :, :seen])
        m = jnp.max(s, axis=1, keepdims=True)
        p = jnp.exp2(s - m)
        l = jnp.sum(p, axis=1, keepdims=True)
        c = jnp.dot(p.astype(BF), kv_all[b, :seen, HD:], preferred_element_type=F32)

        def block(j, st):
            m, l, c = st
            s = scored(kv_all[j, :, :HD], masks[j])
            m2 = jnp.maximum(m, jnp.max(s, axis=1, keepdims=True))
            f = jnp.exp2(m - m2)
            p = jnp.exp2(s - m2)
            l = l * f + jnp.sum(p, axis=1, keepdims=True)
            c = c * f + jnp.dot(p.astype(BF), kv_all[j, :, HD:], preferred_element_type=F32)
            return (m2, l, c)

        m, l, c = lax.fori_loop(0, b, block, (m, l, c))
        return (c / l).astype(BF)

    def cpiece(z_half, y_side, part):
        return ctx_all.at[z_half, part, :, pl.ds(pl.multiple_of(y_side * qc, 128), qc)]

    def az(z_half, part):
        piece = cpiece(z_half, yy, part)
        return remote(piece, piece, azs.at[part], azr.at[part], (b, flip(t, nt // 2)))

    def ay(z_half, y_side, part, i):
        piece = cpiece(z_half, y_side, part)
        return remote(piece, piece, ays.at[part, i], ayr.at[part, i], (b, flip(t, 1)))

    def relay_ctx(part):
        az(1 - zi, part).wait_recv()
        ay(1 - zi, yy, part, 1).start()

    def partial(part, slot_side):
        acc = None
        for zh in range(2):
            one = lax.dot_general(ctx_all[zh, part], wo[2 * zh + slot_side], across_qk,
                                  preferred_element_type=F32)
            acc = one if acc is None else acc + one
        return acc

    z_low = (t // 2) % 2

    def pcopy(part):
        return remote(psend.at[part], prec.at[part], pss.at[part], prs.at[part], (b, flip(t, 2)))

    def project(part):
        psend[part] = partial(part, 1 - z_low).astype(BF)
        pcopy(part).start()
        toks = slice(part * qrows, (part + 1) * qrows)
        resid = x_ref[toks, pl.ds(pl.multiple_of(t * oc, 128), oc)].astype(F32)
        oacc[toks, :] = resid + partial(part, z_low)

    def homes(i):
        for k in range(nb):
            with jax.named_scope(f"whome{i}{k}"):
                w_home(flip(k_mine, k), i)

    def crosses(i):
        for k in range(nb):
            with jax.named_scope(f"wcross{i}{k}"):
                w_cross(flip(k_mine, k), i)

    def head(part, h):
        with jax.named_scope(f"att{part}{h}"):
            col = pl.ds(pl.multiple_of(yy * qc + h * HD, 128), HD)
            ctx_all[zi, part, :, col] = attend(h, part)

    def send_ctx(part):
        az(zi, part).start()
        ay(zi, yy, part, 0).start()

    mask_part(0)
    head(0, 0)
    head(0, 1)
    head(0, 2)
    head(0, 3)
    send_ctx(0)
    homes(0)
    mask_part(1)
    head(1, 0)
    head(1, 1)
    homes(1)
    head(1, 2)
    head(1, 3)
    send_ctx(1)
    crosses(0)
    crosses(1)
    for part in range(n_part):
        with jax.named_scope(f"ctxrelay{part}"):
            relay_ctx(part)
    for k in range(nb):
        with jax.named_scope(f"wlast{k}"):
            for i in range(2):
                w_last(k, i)
    for part in range(n_part):
        with jax.named_scope(f"ctxy{part}"):
            ay(zi, 1 - yy, part, 0).wait_recv()
            ay(1 - zi, 1 - yy, part, 1).wait_recv()
        with jax.named_scope(f"project{part}"):
            project(part)
    for part in range(n_part):
        with jax.named_scope(f"prec{part}"):
            pcopy(part).wait_recv()
        toks = slice(part * qrows, (part + 1) * qrows)
        out_ref[toks, :] = (oacc[toks, :] + prec[part].astype(F32)).astype(BF)

    gather_sent(kv_set)
    gather_sent(q_set)

    @pl.when(low)
    def _():
        for c in keys(b, 0, (bx, t)):
            c.wait_send()

    @pl.when(even)
    def _():
        for c in keys(b, 1, (bc, t)):
            c.wait_send()

    @pl.when(b >= nb // 2)
    def _():
        for c in keys(bx, 2, (bc, t)):
            c.wait_send()

    for i in range(2):
        for side in range(2):
            to_relay(side, i).wait_send()
            delivered(straight(side, i))
            delivered(from_relay(side, i))
        for k in range(nb):
            w_x(b, k, i).wait_send()
            w_c(b, 0, k, i).wait_send()
            w_c(bx, 1, k, i).wait_send()
    for part in range(n_part):
        az(zi, part).wait_send()
        ay(zi, yy, part, 0).wait_send()
        ay(1 - zi, yy, part, 1).wait_send()
        pcopy(part).wait_send()


def fused(nb, nt, residual_in, norm_gain, w_query, w_key_value, query_bias, key_value_bias, w_output,
          device_map, positions, segments):
    n_tok, width = residual_in.shape
    rows = w_query.shape[0]
    qc, kc, oc = w_query.shape[1] // nt, w_key_value.shape[1] // nt, width // nt
    n = nb * nt
    inv = ROPE_BASE ** (-(np.arange(HD // 2, dtype=np.float64) * 2.0) / HD)
    inv = np.concatenate([inv, inv]).astype(np.float32)[None, :]
    any_, vm = pl.BlockSpec(memory_space=pl.ANY), pl.BlockSpec(memory_space=pltpu.VMEM)
    dma = pltpu.SemaphoreType.DMA
    return pl.pallas_call(
        functools.partial(fused_kernel, nb, nt),
        out_shape=jax.ShapeDtypeStruct((n_tok, oc), BF),
        in_specs=[pl.BlockSpec(memory_space=pltpu.SMEM), any_, any_, any_, vm, vm, vm, any_, vm, vm, vm],
        out_specs=vm,
        scratch_shapes=[
            pltpu.VMEM((n_tok, width), BF),
            pltpu.VMEM((n, n_tok, rows), BF),
            pltpu.VMEM((n, rows, qc), BF),
            pltpu.VMEM((n, rows, kc), BF),
            pltpu.VMEM((nb, oc, 2 * qc), BF),
            pltpu.VMEM((nb, n_tok, kc), BF),
            pltpu.VMEM((nb, 1, n_tok), jnp.int32),
            pltpu.VMEM((n_tok, qc), F32),
            pltpu.VMEM((n_tok, kc), F32),
            pltpu.VMEM((n_tok, qc), BF),
            pltpu.VMEM((2, 2, n_tok // 2, 2 * qc), BF),
            pltpu.VMEM((n_tok, oc), F32),
            pltpu.VMEM((width // 128, 128), F32), pltpu.VMEM((qc * nt // HD, HD), F32),
            pltpu.VMEM((kc * nt // HD, HD), F32), pltpu.VMEM((n_tok, HD), F32),
            pltpu.VMEM((n_tok, HD), F32), pltpu.VMEM((n_tok, 1), jnp.int32),
            pltpu.VMEM((nb, n_tok // 2, n_tok), F32), pltpu.VMEM((2, n_tok // 2, oc), BF),
            pltpu.VMEM((2, n_tok // 2, oc), BF), dma((2,)), dma((2,)),
            dma, dma((3,)),
            dma((nt,)), dma((nt,)), dma((nt,)), dma((nt,)), dma((2 * nt,)), dma((2 * nt,)),
            dma((nt,)), dma((nt,)), dma((nt,)), dma((nt,)), dma((2 * nt,)), dma((2 * nt,)),
            dma((2, 2)), dma((nb, 2)), dma((nb, 2)), dma((nb, 2)), dma((2, nb, 2)), dma((2, nb, 2)),
            dma((nb,)), dma((nb,)), dma((nb,)), dma((nb,)),
            dma((2,)), dma((2,)), dma((2, 2)), dma((2, 2)),
            pltpu.VMEM((2, 2, rows, qc), BF), dma((2, 2)), dma((2, 2)), dma((2, 2)),
        ],
        compiler_params=pltpu.CompilerParams(
            collective_id=0, has_side_effects=True, vmem_limit_bytes=63 * 1024 * 1024),
    )(device_map, residual_in, w_query, w_key_value, norm_gain.reshape(-1, 128), query_bias.reshape(-1, HD),
      key_value_bias.reshape(-1, HD), w_output.T, jnp.asarray(inv), positions[None, :], segments[None, :])


def route(shape, *args):
    nb, nt = shape["blk"], shape["tp"]
    n_tok, width = args[0].shape
    rows = args[2].shape[0]
    qc, kc, oc = args[2].shape[1] // nt, args[3].shape[1] // nt, width // nt
    fits = (nb == 4 and nt == KVH and rows % 32 == 0 and rows <= 160 and qc == 4 * HD and kc == 2 * HD
            and oc == nb * rows and oc % 128 == 0 and width % 128 == 0 and n_tok % 256 == 0)
    if fits:
        return fused(nb, nt, *args)
    return per_device(*args)


def solution(mesh):
    in_specs = (
        P("blk", None),
        P(),
        P(("blk", "tp"), None),
        P(("blk", "tp"), None),
        P(),
        P(),
        P(None, ("blk", "tp")),
        P(),
        P("blk"),
        P("blk"),
    )
    out_specs = P("blk", "tp")
    return jax.shard_map(
        functools.partial(route, dict(mesh.shape)), mesh=mesh, in_specs=in_specs, out_specs=out_specs, check_vma=False
    )
```

```python
import functools

import jax
import jax.numpy as jnp
import numpy as np
from jax import lax
from jax.experimental import pallas as pl
from jax.experimental.pallas import tpu as pltpu
from jax.sharding import PartitionSpec as P

D = 5120
KVH = 8
HD = 128


NORM_FLOOR = 0.0625
ROPE_BASE = 1000000.0
NEGATIVE_FILL = -1e30
LOG2E = 1.4426950408889634
PARTS = 4


def for_sending(x):
    return jax.tree.map(lambda a: a.astype(jnp.bfloat16) if a.dtype == jnp.float32 else a, x)


def from_partner(block, axis, bit):
    count = lax.axis_size(axis)
    route = []
    for low in range(count):
        high = low | 1 << bit
        if high != low and high < count:
            route += [(low, high), (high, low)]
    return lax.ppermute(block, axis, route)


def rope_tables(positions, head_width):
    half_width = head_width // 2
    frequency = ROPE_BASE ** (-(jnp.arange(half_width, dtype=jnp.float32) * 2.0) / head_width)
    angles = positions.astype(jnp.float32)[:, None] * frequency[None, :]
    angles = jnp.concatenate([angles, angles], axis=1)
    return (jnp.cos(angles), jnp.sin(angles))


def rotate(values, cosine_table, sine_table):
    half_width = values.shape[-1] // 2
    turned = jnp.concatenate([-values[..., half_width:], values[..., :half_width]], axis=-1)
    return values * cosine_table[:, None, :] + turned * sine_table[:, None, :]


def join_pair(mine_cols, partner, is_lower):
    return jnp.where(
        is_lower,
        jnp.concatenate([mine_cols, partner], axis=1),
        jnp.concatenate([partner, mine_cols], axis=1),
    )


def per_device(
    residual_in,
    norm_gain,
    w_query,
    w_key_value,
    query_bias,
    key_value_bias,
    w_output,
    device_map,
    positions,
    segments,
):
    tp_count = lax.axis_size("tp")
    tp_index = lax.axis_index("tp")
    blk_index = lax.axis_index("blk")
    local_tokens = residual_in.shape[0]
    shard_rows = w_query.shape[0]
    kv_group = tp_count // KVH
    floats = residual_in.astype(jnp.float32)
    square = jnp.maximum(jnp.mean(floats * floats, axis=1, keepdims=True), NORM_FLOOR)
    normed = (floats * lax.rsqrt(square) * norm_gain.astype(jnp.float32)).astype(jnp.bfloat16)
    ordered = jnp.take(
        normed.reshape(local_tokens, device_map.shape[0], shard_rows), device_map, axis=1
    ).reshape(local_tokens, D)
    moved_query, moved_pairs = (
        lax.all_to_all(w_query, "tp", split_axis=1, concat_axis=0, tiled=True),
        lax.all_to_all(w_key_value, "tp", split_axis=1, concat_axis=0, tiled=True),
    )
    for bit_level in range(kv_group.bit_length() - 1):
        partner = from_partner(for_sending(moved_pairs), "tp", bit_level).astype(moved_pairs.dtype)
        moved_pairs = join_pair(moved_pairs, partner, tp_index >> bit_level & 1 == 0)
    queries = jnp.dot(
        ordered,
        lax.all_gather(moved_query, "blk", axis=0, tiled=True),
        preferred_element_type=jnp.float32,
    )
    key_value = jnp.dot(
        ordered,
        lax.all_gather(moved_pairs, "blk", axis=0, tiled=True),
        preferred_element_type=jnp.float32,
    )
    query_width = queries.shape[1]
    heads_here = query_width // HD
    kv_head = tp_index // kv_group
    queries = queries + lax.dynamic_slice_in_dim(
        query_bias, tp_index * query_width, query_width
    ).astype(jnp.float32)
    key_value = key_value + lax.dynamic_slice_in_dim(
        key_value_bias, kv_head * 2 * HD, 2 * HD
    ).astype(jnp.float32)
    cosine_table, sine_table = rope_tables(positions, HD)
    query_rot = rotate(
        queries.reshape(local_tokens, heads_here, HD), cosine_table, sine_table
    ).astype(jnp.bfloat16)
    key_rot = rotate(key_value[:, None, :HD], cosine_table, sine_table)[:, 0, :].astype(
        jnp.bfloat16
    )
    values = key_value[:, HD:].astype(jnp.bfloat16)
    attend_scale = HD ** (-0.5)
    row_index = blk_index * local_tokens + jnp.arange(local_tokens, dtype=jnp.int32)
    initial = (
        jnp.full((heads_here, local_tokens), NEGATIVE_FILL, jnp.float32),
        jnp.zeros((heads_here, local_tokens), jnp.float32),
        jnp.zeros((heads_here, local_tokens, HD), jnp.float32),
    )
    key_piece = lax.all_gather(key_rot, "blk", axis=0, tiled=True)
    value_piece = lax.all_gather(values, "blk", axis=0, tiled=True)
    segment_piece = lax.all_gather(segments, "blk", axis=0, tiled=True)
    piece_rows = key_piece.shape[0]
    key_block_rows = 512

    def one_block(block_number, state_now):
        run_peak, run_mass, context = state_now
        block_start = block_number * key_block_rows
        key_block = lax.dynamic_slice_in_dim(key_piece, block_start, key_block_rows, 0)
        value_block = lax.dynamic_slice_in_dim(value_piece, block_start, key_block_rows, 0)
        segment_block = lax.dynamic_slice_in_dim(segment_piece, block_start, key_block_rows, 0)
        scores = (
            jnp.einsum("qhd,kd->hqk", query_rot, key_block, preferred_element_type=jnp.float32)
            * attend_scale
        )
        key_index = block_start + jnp.arange(key_block_rows, dtype=jnp.int32)
        visible = (key_index[None, :] <= row_index[:, None]) & (
            segment_block[None, :] == segments[:, None]
        )
        masked = jnp.where(visible[None], scores, NEGATIVE_FILL)
        new_peak = jnp.maximum(run_peak, jnp.max(masked, axis=2))
        factor = jnp.exp(run_peak - new_peak)
        raw_weights = jnp.where(visible[None], jnp.exp(masked - new_peak[:, :, None]), 0.0)
        run_mass = run_mass * factor + jnp.sum(raw_weights, axis=2)
        context = context * factor[:, :, None] + jnp.einsum(
            "hqk,kd->hqd",
            raw_weights.astype(jnp.bfloat16),
            value_block,
            preferred_element_type=jnp.float32,
        )
        return (new_peak, run_mass, context)

    run_peak, run_mass, context = lax.fori_loop(0, piece_rows // key_block_rows, one_block, initial)
    context_flat = (
        (context / run_mass[:, :, None])
        .transpose(1, 0, 2)
        .reshape(local_tokens, query_width)
        .astype(jnp.bfloat16)
    )
    width_out = D // tp_count
    moved_out = lax.all_to_all(w_output, "tp", split_axis=0, concat_axis=1, tiled=True)
    row_terms = jnp.dot(
        context_flat,
        lax.all_gather(moved_out, "blk", axis=1, tiled=True),
        preferred_element_type=jnp.float32,
    )
    summed = lax.psum_scatter(
        row_terms.astype(jnp.bfloat16), "tp", scatter_dimension=1, tiled=True
    ).astype(jnp.float32)
    residual_part = lax.dynamic_slice_in_dim(residual_in, tp_index * width_out, width_out, 1)
    return (residual_part.astype(jnp.float32) + summed).astype(jnp.bfloat16)


MESH = pl.DeviceIdType.MESH
BF = jnp.bfloat16
F32 = jnp.float32


def flip(i, mask):
    out = i
    for bit in range(mask.bit_length()):
        if mask >> bit & 1:
            out = out + (1 << bit) * (1 - 2 * ((i // (1 << bit)) % 2))
    return out


def fused_kernel(nb, nt, dm_ref, x_hbm, wq_hbm, wkv_hbm, gain_ref, bq_ref, bkv_ref, wo_hbm, inv_ref,
                 pos_ref, seg_ref, out_ref, x_ref, xo, gq, gkv, wo, kv_all, seg_all, qacc,
                 kvacc, qrot, ctx_all, oacc, gain32, bq32, bkv32, cos_t, sin_t, segq_ref,
                 masks, psend, prec, pss, prs,
                 x_sem, loc_sem, kv1s, kv1r, kvxs, kvxr, kvcs, kvcr, q1s, q1r, qxs, qxr, qcs, qcr,
                 w1s, w1r, wxs, wxr, wcs, wcr, es, er, gs, gr, azs, azr, ays, ayr, wrel, rs, rr, r2s):
    b = lax.axis_index("blk")
    t = lax.axis_index("tp")
    n_tok, width = x_ref.shape
    rows = wq_hbm.shape[0]
    qc, kc = gq.shape[2], gkv.shape[2]
    oc = wo.shape[1]
    bx, bc = flip(b, 2), flip(b, 1)

    barrier = pltpu.get_barrier_semaphore()
    peers = [(b, flip(t, k)) for k in range(1, nt)] + [(flip(b, k), t) for k in range(1, nb)]
    peers += [(bx, flip(t, 1))]
    for peer in peers:
        pl.semaphore_signal(barrier, inc=1, device_id=peer, device_id_type=MESH)
    x_in = pltpu.make_async_copy(x_hbm, x_ref, x_sem)
    x_in.start()
    gain32[...] = gain_ref[...].astype(F32)
    bq32[...] = bq_ref[...].astype(F32)
    bkv32[...] = bkv_ref[...].astype(F32)
    with jax.named_scope("barrier"):
        pl.semaphore_wait(barrier, len(peers))

    def remote(src, dst, ss, rs, dev):
        return pltpu.make_async_remote_copy(src_ref=src, dst_ref=dst, send_sem=ss, recv_sem=rs,
                                            device_id=dev, device_id_type=MESH)

    def slot(bb, k):
        return bb * nt + flip(t, k)

    def stage_one(hbm, buf, width, k, ss, rs, local):
        cols = pl.ds(pl.multiple_of(flip(t, k) * width, 128), width)
        mine = buf.at[b * nt + t]
        if k == 0:
            return pltpu.make_async_copy(hbm.at[:, cols], mine, local)
        return remote(hbm.at[:, cols], mine, ss.at[k], rs.at[k], (b, flip(t, k)))

    def stage_one_in(buf, hbm, width, k, ss, rs, local):
        if k == 0:
            return stage_one(hbm, buf, width, 0, ss, rs, local)
        piece = buf.at[slot(b, k)]
        return remote(piece, piece, ss.at[k], rs.at[k], (b, flip(t, k)))

    def forward(buf, bb, k, ss, rs, i, dev):
        piece = buf.at[slot(bb, k)]
        return remote(piece, piece, ss.at[i], rs.at[i], dev)

    kv_set = (wkv_hbm, gkv, kc, kv1s, kv1r, kvxs, kvxr, kvcs, kvcr, loc_sem.at[0])
    q_set = (wq_hbm, gq, qc, q1s, q1r, qxs, qxr, qcs, qcr, loc_sem.at[1])

    order = [0, 1, 2, 4, 3, 6, 5, 7]

    def across(ws, k):
        hbm, buf, width, s1, r1, xs, xr, cs, cr, loc = ws
        cols = pl.ds(pl.multiple_of(flip(t, k) * width, 128), width)
        return remote(hbm.at[:, cols], buf.at[b * nt + t], xs.at[k], xr.at[k], (bx, flip(t, k)))

    def start_one(ws, k):
        hbm, buf, width, s1, r1, xs, xr, cs, cr, loc = ws
        stage_one(hbm, buf, width, k, s1, r1, loc).start()
        if k < 2:
            across(ws, k).start()

    def gather_step(ws, i):
        k = order[i]
        hbm, buf, width, s1, r1, xs, xr, cs, cr, loc = ws
        arrived = stage_one_in(buf, hbm, width, k, s1, r1, loc)
        if k == 0:
            arrived.wait()
        else:
            arrived.wait_recv()
        if k > 1:
            forward(buf, b, k, xs, xr, k, (bx, t)).start()
        forward(buf, b, k, cs, cr, k, (bc, t)).start()

    def gather_cross(ws, i):
        k = order[i]
        hbm, buf, width, s1, r1, xs, xr, cs, cr, loc = ws
        forward(buf, bx, k, xs, xr, k, (bx, t)).wait_recv()
        forward(buf, bx, k, cs, cr, nt + k, (bc, t)).start()

    def gather_last(ws, i):
        k = order[i]
        hbm, buf, width, s1, r1, xs, xr, cs, cr, loc = ws
        forward(buf, bc, k, cs, cr, k, (bc, t)).wait_recv()
        forward(buf, flip(b, 3), k, cs, cr, nt + k, (bc, t)).wait_recv()

    def gather_sent(ws):
        hbm, buf, width, s1, r1, xs, xr, cs, cr, loc = ws
        for k in range(nt):
            if k:
                stage_one(hbm, buf, width, k, s1, r1, loc).wait_send()
            if k < 2:
                across(ws, k).wait_send()
            else:
                forward(buf, b, k, xs, xr, k, (bx, t)).wait_send()
            forward(buf, b, k, cs, cr, k, (bc, t)).wait_send()
            forward(buf, bx, k, cs, cr, nt + k, (bc, t)).wait_send()

    def multiply(buf, acc, i):
        k = order[i]

        def one(j, _):
            s = slot(j, k)
            acc[...] += jnp.dot(xo[dm_ref[s]], buf[s], preferred_element_type=F32)
            return 0
        lax.fori_loop(0, nb, one, 0)

    issue = [0,2,4,1,6,3,5,7]
    for k in issue:
        start_one(kv_set, k)

    x_in.wait()
    tile = n_tok // nt

    def norm_tile(i):
        toks = slice(i * tile, (i + 1) * tile)
        v = x_ref[toks, :].astype(F32)
        scale = lax.rsqrt(jnp.maximum(jnp.mean(v * v, axis=1, keepdims=True), NORM_FLOOR))

        def spread(g, _):
            per = 4 * rows // 128
            gain = jnp.concatenate([gain32[pl.ds(g * per + i, 1), :] for i in range(per)], axis=1)
            u = x_ref[toks, pl.ds(pl.multiple_of(g * 4 * rows, 128), 4 * rows)].astype(F32)
            u = (u * scale * gain).astype(BF)
            for i in range(4):
                xo[g * 4 + i, toks, :] = u[:, i * rows:(i + 1) * rows]
            return 0

        lax.fori_loop(0, nb * nt // 4, spread, 0)

    def tables():
        pos = jnp.broadcast_to(pos_ref[...].astype(F32), (HD, n_tok)).T
        angles = pos * inv_ref[...]
        cos_t[...] = jnp.cos(angles)
        sign = jnp.where(lax.broadcasted_iota(jnp.int32, (1, HD), 1) < HD // 2, -1.0, 1.0)
        sin_t[...] = jnp.sin(angles) * sign
        segq_ref[...] = jnp.broadcast_to(seg_ref[...].astype(F32), (HD, n_tok)).T[:, :1].astype(jnp.int32)

    zi, yy = t // (nt // 2), t % 2
    k_mine = t % nb
    even_core = b % 2

    def wsrc(c, i):
        return wo_hbm.at[:, pl.ds(pl.multiple_of((c * 2 + i) * qc, 128), qc)]

    def wpiece(slot, k, i):
        return wo.at[slot, pl.ds(pl.multiple_of(k * rows, 16), rows), i * qc:(i + 1) * qc]

    def mine_or_next(side, owner):
        col = owner * 2 + t // nb
        return (even_core, col) if side == 0 else (1 - even_core, flip(col, 2))

    def straight(side, i):
        c, dest = mine_or_next(side, b)
        return dest, wsrc(c, i), wpiece(even_core, k_mine, i), w1s.at[side, i], w1r.at[k_mine, i]

    def to_relay(side, i):
        c, _ = mine_or_next(side, bx)
        return remote(wsrc(2 + c, i), wrel.at[side, i], rs.at[side, i], rr.at[side, i], (bx, t))

    def from_relay(side, i):
        _, dest = mine_or_next(side, bx)
        return dest, wrel.at[side, i], wpiece(2 + even_core, k_mine, i), r2s.at[side, i], w1r.at[k_mine, i]

    def deliver(what):
        dest, src, dst, ss, sr = what

        @pl.when(dest != t)
        def _():
            remote(src, dst, ss, sr, (b, dest)).start()

        @pl.when(dest == t)
        def _():
            pltpu.make_async_copy(src, dst, sr).start()

    def delivered(what):
        dest, src, dst, ss, sr = what

        @pl.when(dest != t)
        def _():
            remote(src, dst, ss, sr, (b, dest)).wait_send()

    def whalf(bb, k, i):
        return wpiece(2 * ((bb // 2 + zi) % 2) + bb % 2, k, i)

    def w_x(bb, k, i):
        return remote(whalf(bb, k, i), whalf(bb, k, i), wxs.at[k, i], wxr.at[k, i], (bx, t))

    def w_c(bb, u, k, i):
        return remote(whalf(bb, k, i), whalf(bb, k, i), wcs.at[u, k, i], wcr.at[u, k, i], (bc, t))

    def w_home(k, i):
        remote(whalf(b, k, i), whalf(b, k, i), w1s.at[0, i], w1r.at[k, i], (bx, t)).wait_recv()
        w_x(b, k, i).start()
        w_c(b, 0, k, i).start()

    def w_cross(k, i):
        w_x(bx, k, i).wait_recv()
        w_c(bx, 1, k, i).start()

    def w_last(k, i):
        w_c(bc, 0, k, i).wait_recv()
        w_c(flip(b, 3), 1, k, i).wait_recv()

    def w_straight(side):
        for i in range(2):
            deliver(straight(side, i))

    def w_start(side):
        for i in range(2):
            to_relay(side, i).start()

    def w_relay(side, i):
        to_relay(side, i).wait_recv()
        deliver(from_relay(side, i))

    def relays(side):
        for i in range(2):
            with jax.named_scope(f"wrelay{i}{side}"):
                w_relay(side, i)

    for k in range(nt):
        with jax.named_scope(f"norm{k}"):
            norm_tile(k)
        with jax.named_scope(f"kvstep{k}"):
            gather_step(kv_set, k)
        if k >= 2:
            start_one(q_set, issue[k - 2])
        if k == 5:
            w_start(1)
            w_start(0)
        if k:
            with jax.named_scope(f"kvcross{k}"):
                gather_cross(kv_set, k - 1)
    for k in range(nt - 2, nt):
        start_one(q_set, issue[k])
    with jax.named_scope("tables"):
        tables()
    with jax.named_scope("kvcross8"):
        gather_cross(kv_set, nt - 1)

    for e in range(2):
        kvacc[:, e * HD:(e + 1) * HD] = jnp.broadcast_to(bkv32[pl.ds(t * 2 + e, 1), :], (n_tok, HD))
    for k in range(4):
        with jax.named_scope(f"qstep{k}"):
            gather_step(q_set, k)
        if k:
            with jax.named_scope(f"qcross{k}"):
                gather_cross(q_set, k - 1)
    for e in range(qc // HD):
        qacc[:, e * HD:(e + 1) * HD] = jnp.broadcast_to(
            bq32[pl.ds(t * (qc // HD) + e, 1), :], (n_tok, HD))
    for e in range(nt):
        gather_last(kv_set, e)
        with jax.named_scope(f"kvmul{e}"):
            multiply(gkv, kvacc, e)
        if e % 2 and 4 + e // 2 < nt:
            k = 4 + e // 2
            with jax.named_scope(f"qstep{k}"):
                gather_step(q_set, k)
            with jax.named_scope(f"qcross{k}"):
                gather_cross(q_set, k - 1)
            if k == 4:
                w_straight(1)
            if k == 5:
                w_straight(0)
            if k == 5:
                relays(1)
            if k == 7:
                relays(0)
            if e > 1:
                gather_last(q_set, e // 2 - 1)
                multiply(gq, qacc, e // 2 - 1)

    def rope(u):
        return u * cos_t[...] + pltpu.roll(u, HD // 2, 1) * sin_t[...]

    kv_all[b, :, :HD] = rope(kvacc[:, :HD]).astype(BF)
    kv_all[b, :, HD:] = kvacc[:, HD:].astype(BF)
    seg_all[b] = seg_ref[...]

    def keys(slot_b, sem, dev):
        return (remote(kv_all.at[slot_b], kv_all.at[slot_b], es.at[sem], er.at[sem], dev),
                remote(seg_all.at[slot_b], seg_all.at[slot_b], gs.at[sem], gr.at[sem], dev))

    low = b < nb // 2
    even = b % 2 == 0

    @pl.when(low)
    def _():
        for c in keys(b, 0, (bx, t)):
            c.start()

    @pl.when(even)
    def _():
        for c in keys(b, 1, (bc, t)):
            c.start()

    for k in range(8, nt):
        with jax.named_scope(f"qstep{k}"):
            gather_step(q_set, k)
        with jax.named_scope(f"qcross{k}"):
            gather_cross(q_set, k - 1)
    for e in range(nt // 2 - 1, nt):
        if e == nt - 3:
            with jax.named_scope("qcross8"):
                gather_cross(q_set, nt - 1)
        with jax.named_scope(f"qlast{e}"):
            gather_last(q_set, e)
        with jax.named_scope(f"qmul{e}"):
            multiply(gq, qacc, e)

    n_part = ctx_all.shape[1]
    qrows = n_tok // n_part
    for h in range(qc // HD):
        turned = rope(qacc[:, h * HD:(h + 1) * HD]).astype(BF)
        for part in range(n_part):
            qrot[part, h * qrows:(h + 1) * qrows, :] = turned[part * qrows:(part + 1) * qrows, :]

    @pl.when(b >= nb // 2)
    def _():
        for c in keys(bx, 0, (bx, t)):
            c.wait_recv()
        for c in keys(bx, 2, (bc, t)):
            c.start()
        for c in keys(flip(b, 3), 2, (bc, t)):
            c.wait_recv()

    @pl.when(b % 2 == 1)
    def _():
        for c in keys(bc, 1, (bc, t)):
            c.wait_recv()

    scale = HD ** (-0.5) * LOG2E
    across_qk = (((1,), (1,)), ((), ()))

    def mask_part(part):
        r0 = part * qrows
        sq = segq_ref[r0:r0 + qrows, :]
        seen = r0 + qrows
        ri = r0 + lax.broadcasted_iota(jnp.int32, (qrows, seen), 0)
        ci = lax.broadcasted_iota(jnp.int32, (qrows, seen), 1)
        vis = (ci <= ri) & (seg_all[b][:, :seen] == sq)
        masks[nb - 1, :, :seen] = jnp.where(vis, 0.0, NEGATIVE_FILL)

        def earlier(j, _):
            masks[j] = jnp.where(seg_all[j] == sq, jnp.zeros((qrows, n_tok), F32), NEGATIVE_FILL)
            return 0

        lax.fori_loop(0, b, earlier, 0)

    group = 4

    def attend(g, part):
        seen = (part + 1) * qrows
        rows_here = group * qrows
        qh = qrot[part, g * rows_here:(g + 1) * rows_here, :]

        def scored(kb, mask):
            s = lax.dot_general(qh, kb, across_qk, preferred_element_type=F32) * scale
            return (s.reshape(group, qrows, -1) + mask[None]).reshape(rows_here, -1)

        s = scored(kv_all[b, :seen, :HD], masks[nb - 1, :, :seen])
        m = jnp.max(s, axis=1, keepdims=True)
        p = jnp.exp2(s - m)
        l = jnp.sum(p, axis=1, keepdims=True)
        c = jnp.dot(p.astype(BF), kv_all[b, :seen, HD:], preferred_element_type=F32)

        def block(j, st):
            m, l, c = st
            s = scored(kv_all[j, :, :HD], masks[j])
            m2 = jnp.maximum(m, jnp.max(s, axis=1, keepdims=True))
            f = jnp.exp2(m - m2)
            p = jnp.exp2(s - m2)
            l = l * f + jnp.sum(p, axis=1, keepdims=True)
            c = c * f + jnp.dot(p.astype(BF), kv_all[j, :, HD:], preferred_element_type=F32)
            return (m2, l, c)

        m, l, c = lax.fori_loop(0, b, block, (m, l, c))
        return (c / l).astype(BF)

    def cpiece(z_half, y_side, part):
        return ctx_all.at[z_half, part, :, pl.ds(pl.multiple_of(y_side * qc, 128), qc)]

    def az(z_half, part):
        piece = cpiece(z_half, yy, part)
        return remote(piece, piece, azs.at[part], azr.at[part], (b, flip(t, nt // 2)))

    def ay(z_half, y_side, part, i):
        piece = cpiece(z_half, y_side, part)
        return remote(piece, piece, ays.at[part, i], ayr.at[part, i], (b, flip(t, 1)))

    def relay_ctx(part):
        az(1 - zi, part).wait_recv()
        ay(1 - zi, yy, part, 1).start()

    def partial(part, slot_side):
        acc = None
        for zh in range(2):
            one = lax.dot_general(ctx_all[zh, part], wo[2 * zh + slot_side], across_qk,
                                  preferred_element_type=F32)
            acc = one if acc is None else acc + one
        return acc

    z_low = (t // 2) % 2

    def pcopy(part):
        return remote(psend.at[part], prec.at[part], pss.at[part], prs.at[part], (b, flip(t, 2)))

    def homes(i):
        for k in range(nb):
            with jax.named_scope(f"whome{i}{k}"):
                w_home(flip(k_mine, k), i)

    def crosses(i):
        for k in range(nb):
            with jax.named_scope(f"wcross{i}{k}"):
                w_cross(flip(k_mine, k), i)

    def heads(part, g):
        with jax.named_scope(f"att{part}{g}"):
            both = attend(g, part)
            for e in range(group):
                col = pl.ds(pl.multiple_of(yy * qc + (g * group + e) * HD, 128), HD)
                ctx_all[zi, part, :, col] = both[e * qrows:(e + 1) * qrows, :]

    def send_ctx(part):
        az(zi, part).start()
        ay(zi, yy, part, 0).start()

    next_first = even_core != z_low

    def on(which, *steps):
        @pl.when(which)
        def _():
            for step in steps:
                step()

    def attention(part):
        mask_part(part)
        for g in range(qc // HD // group):
            heads(part, g)
        send_ctx(part)

    def last():
        with jax.named_scope("wlast"):
            for i in range(2):
                for k in range(nb):
                    w_last(flip(k_mine, k), i)

    def next_part(part):
        with jax.named_scope(f"ctxy{part}"):
            ay(zi, 1 - yy, part, 0).wait_recv()
            ay(1 - zi, 1 - yy, part, 1).wait_recv()
        with jax.named_scope(f"next{part}"):
            psend[part] = partial(part, 1 - z_low).astype(BF)
        pcopy(part).start()

    def own_part(part):
        toks = slice(part * qrows, (part + 1) * qrows)
        resid = x_ref[toks, pl.ds(pl.multiple_of(t * oc, 128), oc)].astype(F32)
        with jax.named_scope(f"own{part}"):
            oacc[toks, :] = resid + partial(part, z_low)

    def ctx_turn(part):
        with jax.named_scope(f"ctxrelay{part}"):
            relay_ctx(part)

    own_first = even_core == z_low
    middle = n_part // 2
    on(next_first, lambda: homes(0))
    for part in range(middle):
        attention(part)
    on(next_first, lambda: homes(1))
    for part in range(middle, n_part):
        attention(part)
    on(own_first, lambda: homes(0))
    for part in range(middle):
        ctx_turn(part)
    on(own_first, lambda: homes(1))
    on(next_first, lambda: crosses(0), lambda: crosses(1))
    for part in range(middle, n_part - 1):
        ctx_turn(part)
    on(own_first, last)
    next_part(0)
    ctx_turn(n_part - 1)
    for part in range(1, n_part):
        next_part(part)
    on(own_first, lambda: crosses(0), lambda: crosses(1))
    on(next_first, last)
    for part in range(n_part):
        own_part(part)
    for part in range(n_part):
        with jax.named_scope(f"prec{part}"):
            pcopy(part).wait_recv()
        toks = slice(part * qrows, (part + 1) * qrows)
        out_ref[toks, :] = (oacc[toks, :] + prec[part].astype(F32)).astype(BF)

    gather_sent(kv_set)
    gather_sent(q_set)

    @pl.when(low)
    def _():
        for c in keys(b, 0, (bx, t)):
            c.wait_send()

    @pl.when(even)
    def _():
        for c in keys(b, 1, (bc, t)):
            c.wait_send()

    @pl.when(b >= nb // 2)
    def _():
        for c in keys(bx, 2, (bc, t)):
            c.wait_send()

    for i in range(2):
        for side in range(2):
            to_relay(side, i).wait_send()
            delivered(straight(side, i))
            delivered(from_relay(side, i))
        for k in range(nb):
            w_x(b, k, i).wait_send()
            w_c(b, 0, k, i).wait_send()
            w_c(bx, 1, k, i).wait_send()
    for part in range(n_part):
        az(zi, part).wait_send()
        ay(zi, yy, part, 0).wait_send()
        ay(1 - zi, yy, part, 1).wait_send()
        pcopy(part).wait_send()


def fused(nb, nt, residual_in, norm_gain, w_query, w_key_value, query_bias, key_value_bias, w_output,
          device_map, positions, segments):
    n_tok, width = residual_in.shape
    rows = w_query.shape[0]
    qc, kc, oc = w_query.shape[1] // nt, w_key_value.shape[1] // nt, width // nt
    n = nb * nt
    inv = ROPE_BASE ** (-(np.arange(HD // 2, dtype=np.float64) * 2.0) / HD)
    inv = np.concatenate([inv, inv]).astype(np.float32)[None, :]
    any_, vm = pl.BlockSpec(memory_space=pl.ANY), pl.BlockSpec(memory_space=pltpu.VMEM)
    dma = pltpu.SemaphoreType.DMA
    return pl.pallas_call(
        functools.partial(fused_kernel, nb, nt),
        out_shape=jax.ShapeDtypeStruct((n_tok, oc), BF),
        in_specs=[pl.BlockSpec(memory_space=pltpu.SMEM), any_, any_, any_, vm, vm, vm, any_, vm, vm, vm],
        out_specs=vm,
        scratch_shapes=[
            pltpu.VMEM((n_tok, width), BF),
            pltpu.VMEM((n, n_tok, rows), BF),
            pltpu.VMEM((n, rows, qc), BF),
            pltpu.VMEM((n, rows, kc), BF),
            pltpu.VMEM((nb, oc, 2 * qc), BF),
            pltpu.VMEM((nb, n_tok, kc), BF),
            pltpu.VMEM((nb, 1, n_tok), jnp.int32),
            pltpu.VMEM((n_tok, qc), F32),
            pltpu.VMEM((n_tok, kc), F32),
            pltpu.VMEM((PARTS, n_tok // PARTS * (qc // HD), HD), BF),
            pltpu.VMEM((2, PARTS, n_tok // PARTS, 2 * qc), BF),
            pltpu.VMEM((n_tok, oc), F32),
            pltpu.VMEM((width // 128, 128), F32), pltpu.VMEM((qc * nt // HD, HD), F32),
            pltpu.VMEM((kc * nt // HD, HD), F32), pltpu.VMEM((n_tok, HD), F32),
            pltpu.VMEM((n_tok, HD), F32), pltpu.VMEM((n_tok, 1), jnp.int32),
            pltpu.VMEM((nb, n_tok // PARTS, n_tok), F32), pltpu.VMEM((PARTS, n_tok // PARTS, oc), BF),
            pltpu.VMEM((PARTS, n_tok // PARTS, oc), BF), dma((PARTS,)), dma((PARTS,)),
            dma, dma((3,)),
            dma((nt,)), dma((nt,)), dma((nt,)), dma((nt,)), dma((2 * nt,)), dma((2 * nt,)),
            dma((nt,)), dma((nt,)), dma((nt,)), dma((nt,)), dma((2 * nt,)), dma((2 * nt,)),
            dma((2, 2)), dma((nb, 2)), dma((nb, 2)), dma((nb, 2)), dma((2, nb, 2)), dma((2, nb, 2)),
            dma((nb,)), dma((nb,)), dma((nb,)), dma((nb,)),
            dma((PARTS,)), dma((PARTS,)), dma((PARTS, 2)), dma((PARTS, 2)),
            pltpu.VMEM((2, 2, rows, qc), BF), dma((2, 2)), dma((2, 2)), dma((2, 2)),
        ],
        compiler_params=pltpu.CompilerParams(
            collective_id=0, has_side_effects=True, vmem_limit_bytes=63 * 1024 * 1024),
    )(device_map, residual_in, w_query, w_key_value, norm_gain.reshape(-1, 128), query_bias.reshape(-1, HD),
      key_value_bias.reshape(-1, HD), w_output.T, jnp.asarray(inv), positions[None, :], segments[None, :])


def route(shape, *args):
    nb, nt = shape["blk"], shape["tp"]
    n_tok, width = args[0].shape
    rows = args[2].shape[0]
    qc, kc, oc = args[2].shape[1] // nt, args[3].shape[1] // nt, width // nt
    fits = (nb == 4 and nt == KVH and rows % 32 == 0 and rows <= 160 and qc == 4 * HD and kc == 2 * HD
            and oc == nb * rows and oc % 128 == 0 and width % 128 == 0 and n_tok % 256 == 0)
    if fits:
        return fused(nb, nt, *args)
    return per_device(*args)


def solution(mesh):
    in_specs = (
        P("blk", None),
        P(),
        P(("blk", "tp"), None),
        P(("blk", "tp"), None),
        P(),
        P(),
        P(None, ("blk", "tp")),
        P(),
        P("blk"),
        P("blk"),
    )
    out_specs = P("blk", "tp")
    return jax.shard_map(
        functools.partial(route, dict(mesh.shape)), mesh=mesh, in_specs=in_specs, out_specs=out_specs, check_vma=False
    )
```

```python
import functools

import jax
import jax.numpy as jnp
import numpy as np
from jax import lax
from jax.experimental import pallas as pl
from jax.experimental.pallas import tpu as pltpu
from jax.sharding import PartitionSpec as P

D = 5120
KVH = 8
HD = 128


NORM_FLOOR = 0.0625
ROPE_BASE = 1000000.0
NEGATIVE_FILL = -1e30
LOG2E = 1.4426950408889634
PARTS = 4


def for_sending(x):
    return jax.tree.map(lambda a: a.astype(jnp.bfloat16) if a.dtype == jnp.float32 else a, x)


def from_partner(block, axis, bit):
    count = lax.axis_size(axis)
    route = []
    for low in range(count):
        high = low | 1 << bit
        if high != low and high < count:
            route += [(low, high), (high, low)]
    return lax.ppermute(block, axis, route)


def rope_tables(positions, head_width):
    half_width = head_width // 2
    frequency = ROPE_BASE ** (-(jnp.arange(half_width, dtype=jnp.float32) * 2.0) / head_width)
    angles = positions.astype(jnp.float32)[:, None] * frequency[None, :]
    angles = jnp.concatenate([angles, angles], axis=1)
    return (jnp.cos(angles), jnp.sin(angles))


def rotate(values, cosine_table, sine_table):
    half_width = values.shape[-1] // 2
    turned = jnp.concatenate([-values[..., half_width:], values[..., :half_width]], axis=-1)
    return values * cosine_table[:, None, :] + turned * sine_table[:, None, :]


def join_pair(mine_cols, partner, is_lower):
    return jnp.where(
        is_lower,
        jnp.concatenate([mine_cols, partner], axis=1),
        jnp.concatenate([partner, mine_cols], axis=1),
    )


def per_device(
    residual_in,
    norm_gain,
    w_query,
    w_key_value,
    query_bias,
    key_value_bias,
    w_output,
    device_map,
    positions,
    segments,
):
    tp_count = lax.axis_size("tp")
    tp_index = lax.axis_index("tp")
    blk_index = lax.axis_index("blk")
    local_tokens = residual_in.shape[0]
    shard_rows = w_query.shape[0]
    kv_group = tp_count // KVH
    floats = residual_in.astype(jnp.float32)
    square = jnp.maximum(jnp.mean(floats * floats, axis=1, keepdims=True), NORM_FLOOR)
    normed = (floats * lax.rsqrt(square) * norm_gain.astype(jnp.float32)).astype(jnp.bfloat16)
    ordered = jnp.take(
        normed.reshape(local_tokens, device_map.shape[0], shard_rows), device_map, axis=1
    ).reshape(local_tokens, D)
    moved_query, moved_pairs = (
        lax.all_to_all(w_query, "tp", split_axis=1, concat_axis=0, tiled=True),
        lax.all_to_all(w_key_value, "tp", split_axis=1, concat_axis=0, tiled=True),
    )
    for bit_level in range(kv_group.bit_length() - 1):
        partner = from_partner(for_sending(moved_pairs), "tp", bit_level).astype(moved_pairs.dtype)
        moved_pairs = join_pair(moved_pairs, partner, tp_index >> bit_level & 1 == 0)
    queries = jnp.dot(
        ordered,
        lax.all_gather(moved_query, "blk", axis=0, tiled=True),
        preferred_element_type=jnp.float32,
    )
    key_value = jnp.dot(
        ordered,
        lax.all_gather(moved_pairs, "blk", axis=0, tiled=True),
        preferred_element_type=jnp.float32,
    )
    query_width = queries.shape[1]
    heads_here = query_width // HD
    kv_head = tp_index // kv_group
    queries = queries + lax.dynamic_slice_in_dim(
        query_bias, tp_index * query_width, query_width
    ).astype(jnp.float32)
    key_value = key_value + lax.dynamic_slice_in_dim(
        key_value_bias, kv_head * 2 * HD, 2 * HD
    ).astype(jnp.float32)
    cosine_table, sine_table = rope_tables(positions, HD)
    query_rot = rotate(
        queries.reshape(local_tokens, heads_here, HD), cosine_table, sine_table
    ).astype(jnp.bfloat16)
    key_rot = rotate(key_value[:, None, :HD], cosine_table, sine_table)[:, 0, :].astype(
        jnp.bfloat16
    )
    values = key_value[:, HD:].astype(jnp.bfloat16)
    attend_scale = HD ** (-0.5)
    row_index = blk_index * local_tokens + jnp.arange(local_tokens, dtype=jnp.int32)
    initial = (
        jnp.full((heads_here, local_tokens), NEGATIVE_FILL, jnp.float32),
        jnp.zeros((heads_here, local_tokens), jnp.float32),
        jnp.zeros((heads_here, local_tokens, HD), jnp.float32),
    )
    key_piece = lax.all_gather(key_rot, "blk", axis=0, tiled=True)
    value_piece = lax.all_gather(values, "blk", axis=0, tiled=True)
    segment_piece = lax.all_gather(segments, "blk", axis=0, tiled=True)
    piece_rows = key_piece.shape[0]
    key_block_rows = 512

    def one_block(block_number, state_now):
        run_peak, run_mass, context = state_now
        block_start = block_number * key_block_rows
        key_block = lax.dynamic_slice_in_dim(key_piece, block_start, key_block_rows, 0)
        value_block = lax.dynamic_slice_in_dim(value_piece, block_start, key_block_rows, 0)
        segment_block = lax.dynamic_slice_in_dim(segment_piece, block_start, key_block_rows, 0)
        scores = (
            jnp.einsum("qhd,kd->hqk", query_rot, key_block, preferred_element_type=jnp.float32)
            * attend_scale
        )
        key_index = block_start + jnp.arange(key_block_rows, dtype=jnp.int32)
        visible = (key_index[None, :] <= row_index[:, None]) & (
            segment_block[None, :] == segments[:, None]
        )
        masked = jnp.where(visible[None], scores, NEGATIVE_FILL)
        new_peak = jnp.maximum(run_peak, jnp.max(masked, axis=2))
        factor = jnp.exp(run_peak - new_peak)
        raw_weights = jnp.where(visible[None], jnp.exp(masked - new_peak[:, :, None]), 0.0)
        run_mass = run_mass * factor + jnp.sum(raw_weights, axis=2)
        context = context * factor[:, :, None] + jnp.einsum(
            "hqk,kd->hqd",
            raw_weights.astype(jnp.bfloat16),
            value_block,
            preferred_element_type=jnp.float32,
        )
        return (new_peak, run_mass, context)

    run_peak, run_mass, context = lax.fori_loop(0, piece_rows // key_block_rows, one_block, initial)
    context_flat = (
        (context / run_mass[:, :, None])
        .transpose(1, 0, 2)
        .reshape(local_tokens, query_width)
        .astype(jnp.bfloat16)
    )
    width_out = D // tp_count
    moved_out = lax.all_to_all(w_output, "tp", split_axis=0, concat_axis=1, tiled=True)
    row_terms = jnp.dot(
        context_flat,
        lax.all_gather(moved_out, "blk", axis=1, tiled=True),
        preferred_element_type=jnp.float32,
    )
    summed = lax.psum_scatter(
        row_terms.astype(jnp.bfloat16), "tp", scatter_dimension=1, tiled=True
    ).astype(jnp.float32)
    residual_part = lax.dynamic_slice_in_dim(residual_in, tp_index * width_out, width_out, 1)
    return (residual_part.astype(jnp.float32) + summed).astype(jnp.bfloat16)


MESH = pl.DeviceIdType.MESH
BF = jnp.bfloat16
F32 = jnp.float32


def flip(i, mask):
    out = i
    for bit in range(mask.bit_length()):
        if mask >> bit & 1:
            out = out + (1 << bit) * (1 - 2 * ((i // (1 << bit)) % 2))
    return out


def fused_kernel(nb, nt, dm_ref, x_hbm, wq_hbm, wkv_hbm, gain_ref, bq_ref, bkv_ref, wo_hbm, inv_ref,
                 pos_ref, seg_ref, out_ref, x_ref, xo, gq, gkv, wo, kv_all, seg_all, qacc,
                 kvacc, qrot, ctx_all, oacc, gain32, bq32, bkv32, cos_t, sin_t, segq_ref,
                 masks, psend, prec, pss, prs,
                 x_sem, loc_sem, kv1s, kv1r, kvxs, kvxr, kvcs, kvcr, q1s, q1r, qxs, qxr, qcs, qcr,
                 w1s, w1r, wxs, wxr, wcs, wcr, es, er, gs, gr, azs, azr, ays, ayr, wrel, rs, rr, r2s):
    b = lax.axis_index("blk")
    t = lax.axis_index("tp")
    n_tok, width = x_ref.shape
    rows = wq_hbm.shape[0]
    qc, kc = gq.shape[2], gkv.shape[2]
    oc = wo.shape[1]
    bx, bc = flip(b, 2), flip(b, 1)

    barrier = pltpu.get_barrier_semaphore()
    peers = [(b, flip(t, k)) for k in range(1, nt)] + [(flip(b, k), t) for k in range(1, nb)]
    peers += [(bx, flip(t, 1))]
    for peer in peers:
        pl.semaphore_signal(barrier, inc=1, device_id=peer, device_id_type=MESH)
    x_in = pltpu.make_async_copy(x_hbm, x_ref, x_sem)
    x_in.start()
    gain32[...] = gain_ref[...].astype(F32)
    bq32[...] = bq_ref[...].astype(F32)
    bkv32[...] = bkv_ref[...].astype(F32)
    with jax.named_scope("barrier"):
        pl.semaphore_wait(barrier, len(peers))

    def remote(src, dst, ss, rs, dev):
        return pltpu.make_async_remote_copy(src_ref=src, dst_ref=dst, send_sem=ss, recv_sem=rs,
                                            device_id=dev, device_id_type=MESH)

    def slot(bb, k):
        return bb * nt + flip(t, k)

    def stage_one(hbm, buf, width, k, ss, rs, local):
        cols = pl.ds(pl.multiple_of(flip(t, k) * width, 128), width)
        mine = buf.at[b * nt + t]
        if k == 0:
            return pltpu.make_async_copy(hbm.at[:, cols], mine, local)
        return remote(hbm.at[:, cols], mine, ss.at[k], rs.at[k], (b, flip(t, k)))

    def stage_one_in(buf, hbm, width, k, ss, rs, local):
        if k == 0:
            return stage_one(hbm, buf, width, 0, ss, rs, local)
        piece = buf.at[slot(b, k)]
        return remote(piece, piece, ss.at[k], rs.at[k], (b, flip(t, k)))

    def forward(buf, bb, k, ss, rs, i, dev):
        piece = buf.at[slot(bb, k)]
        return remote(piece, piece, ss.at[i], rs.at[i], dev)

    kv_set = (wkv_hbm, gkv, kc, kv1s, kv1r, kvxs, kvxr, kvcs, kvcr, loc_sem.at[0])
    q_set = (wq_hbm, gq, qc, q1s, q1r, qxs, qxr, qcs, qcr, loc_sem.at[1])

    order = [0, 1, 2, 4, 3, 6, 5, 7]

    def across(ws, k):
        hbm, buf, width, s1, r1, xs, xr, cs, cr, loc = ws
        cols = pl.ds(pl.multiple_of(flip(t, k) * width, 128), width)
        return remote(hbm.at[:, cols], buf.at[b * nt + t], xs.at[k], xr.at[k], (bx, flip(t, k)))

    def start_one(ws, k):
        hbm, buf, width, s1, r1, xs, xr, cs, cr, loc = ws
        stage_one(hbm, buf, width, k, s1, r1, loc).start()
        if k < 2:
            across(ws, k).start()

    def gather_step(ws, i):
        k = order[i]
        hbm, buf, width, s1, r1, xs, xr, cs, cr, loc = ws
        arrived = stage_one_in(buf, hbm, width, k, s1, r1, loc)
        if k == 0:
            arrived.wait()
        else:
            arrived.wait_recv()
        if k > 1:
            forward(buf, b, k, xs, xr, k, (bx, t)).start()
        forward(buf, b, k, cs, cr, k, (bc, t)).start()

    def gather_cross(ws, i):
        k = order[i]
        hbm, buf, width, s1, r1, xs, xr, cs, cr, loc = ws
        forward(buf, bx, k, xs, xr, k, (bx, t)).wait_recv()
        forward(buf, bx, k, cs, cr, nt + k, (bc, t)).start()

    def gather_last(ws, i):
        k = order[i]
        hbm, buf, width, s1, r1, xs, xr, cs, cr, loc = ws
        forward(buf, bc, k, cs, cr, k, (bc, t)).wait_recv()
        forward(buf, flip(b, 3), k, cs, cr, nt + k, (bc, t)).wait_recv()

    def gather_sent(ws):
        hbm, buf, width, s1, r1, xs, xr, cs, cr, loc = ws
        for k in range(nt):
            if k:
                stage_one(hbm, buf, width, k, s1, r1, loc).wait_send()
            if k < 2:
                across(ws, k).wait_send()
            else:
                forward(buf, b, k, xs, xr, k, (bx, t)).wait_send()
            forward(buf, b, k, cs, cr, k, (bc, t)).wait_send()
            forward(buf, bx, k, cs, cr, nt + k, (bc, t)).wait_send()

    def multiply(buf, acc, i):
        k = order[i]

        def one(j, _):
            s = slot(j, k)
            acc[...] += jnp.dot(xo[dm_ref[s]], buf[s], preferred_element_type=F32)
            return 0
        lax.fori_loop(0, nb, one, 0)

    issue = [0,2,4,1,6,3,5,7]
    for k in issue:
        start_one(kv_set, k)

    x_in.wait()
    tile = n_tok // nt

    def norm_tile(i):
        toks = slice(i * tile, (i + 1) * tile)
        v = x_ref[toks, :].astype(F32)
        scale = lax.rsqrt(jnp.maximum(jnp.mean(v * v, axis=1, keepdims=True), NORM_FLOOR))

        def spread(g, _):
            per = 4 * rows // 128
            gain = jnp.concatenate([gain32[pl.ds(g * per + i, 1), :] for i in range(per)], axis=1)
            u = x_ref[toks, pl.ds(pl.multiple_of(g * 4 * rows, 128), 4 * rows)].astype(F32)
            u = (u * scale * gain).astype(BF)
            for i in range(4):
                xo[g * 4 + i, toks, :] = u[:, i * rows:(i + 1) * rows]
            return 0

        lax.fori_loop(0, nb * nt // 4, spread, 0)

    def tables():
        pos = jnp.broadcast_to(pos_ref[...].astype(F32), (HD, n_tok)).T
        angles = pos * inv_ref[...]
        cos_t[...] = jnp.cos(angles)
        sign = jnp.where(lax.broadcasted_iota(jnp.int32, (1, HD), 1) < HD // 2, -1.0, 1.0)
        sin_t[...] = jnp.sin(angles) * sign
        segq_ref[...] = jnp.broadcast_to(seg_ref[...].astype(F32), (HD, n_tok)).T[:, :1].astype(jnp.int32)

    zi, yy = t // (nt // 2), t % 2
    k_mine = t % nb
    even_core = b % 2

    def wsrc(c, i):
        return wo_hbm.at[:, pl.ds(pl.multiple_of((c * 2 + i) * qc, 128), qc)]

    def wpiece(slot, k, i):
        return wo.at[slot, pl.ds(pl.multiple_of(k * rows, 16), rows), i * qc:(i + 1) * qc]

    def mine_or_next(side, owner):
        col = owner * 2 + t // nb
        return (even_core, col) if side == 0 else (1 - even_core, flip(col, 2))

    def straight(side, i):
        c, dest = mine_or_next(side, b)
        return dest, wsrc(c, i), wpiece(even_core, k_mine, i), w1s.at[side, i], w1r.at[k_mine, i]

    def to_relay(side, i):
        c, _ = mine_or_next(side, bx)
        return remote(wsrc(2 + c, i), wrel.at[side, i], rs.at[side, i], rr.at[side, i], (bx, t))

    def from_relay(side, i):
        _, dest = mine_or_next(side, bx)
        return dest, wrel.at[side, i], wpiece(2 + even_core, k_mine, i), r2s.at[side, i], w1r.at[k_mine, i]

    def deliver(what):
        dest, src, dst, ss, sr = what

        @pl.when(dest != t)
        def _():
            remote(src, dst, ss, sr, (b, dest)).start()

        @pl.when(dest == t)
        def _():
            pltpu.make_async_copy(src, dst, sr).start()

    def delivered(what):
        dest, src, dst, ss, sr = what

        @pl.when(dest != t)
        def _():
            remote(src, dst, ss, sr, (b, dest)).wait_send()

    def whalf(bb, k, i):
        return wpiece(2 * ((bb // 2 + zi) % 2) + bb % 2, k, i)

    def w_x(bb, k, i):
        return remote(whalf(bb, k, i), whalf(bb, k, i), wxs.at[k, i], wxr.at[k, i], (bx, t))

    def w_c(bb, u, k, i):
        return remote(whalf(bb, k, i), whalf(bb, k, i), wcs.at[u, k, i], wcr.at[u, k, i], (bc, t))

    def w_home(k, i):
        remote(whalf(b, k, i), whalf(b, k, i), w1s.at[0, i], w1r.at[k, i], (bx, t)).wait_recv()
        w_x(b, k, i).start()
        w_c(b, 0, k, i).start()

    def w_cross(k, i):
        w_x(bx, k, i).wait_recv()
        w_c(bx, 1, k, i).start()

    def w_last(k, i):
        w_c(bc, 0, k, i).wait_recv()
        w_c(flip(b, 3), 1, k, i).wait_recv()

    def w_straight(side):
        for i in range(2):
            deliver(straight(side, i))

    def w_start(side):
        for i in range(2):
            to_relay(side, i).start()

    def w_relay(side, i):
        to_relay(side, i).wait_recv()
        deliver(from_relay(side, i))

    def relays(side):
        for i in range(2):
            with jax.named_scope(f"wrelay{i}{side}"):
                w_relay(side, i)

    for k in range(nt):
        with jax.named_scope(f"norm{k}"):
            norm_tile(k)
        with jax.named_scope(f"kvstep{k}"):
            gather_step(kv_set, k)
        if k >= 2:
            start_one(q_set, issue[k - 2])
        if k == 4:
            w_start(1)
        if k == 6:
            w_start(0)
        if k:
            with jax.named_scope(f"kvcross{k}"):
                gather_cross(kv_set, k - 1)
    for k in range(nt - 2, nt):
        start_one(q_set, issue[k])
    with jax.named_scope("tables"):
        tables()
    with jax.named_scope("kvcross8"):
        gather_cross(kv_set, nt - 1)

    for e in range(2):
        kvacc[:, e * HD:(e + 1) * HD] = jnp.broadcast_to(bkv32[pl.ds(t * 2 + e, 1), :], (n_tok, HD))
    for k in range(4):
        with jax.named_scope(f"qstep{k}"):
            gather_step(q_set, k)
        if k:
            with jax.named_scope(f"qcross{k}"):
                gather_cross(q_set, k - 1)
    for e in range(qc // HD):
        qacc[:, e * HD:(e + 1) * HD] = jnp.broadcast_to(
            bq32[pl.ds(t * (qc // HD) + e, 1), :], (n_tok, HD))
    for e in range(nt):
        gather_last(kv_set, e)
        with jax.named_scope(f"kvmul{e}"):
            multiply(gkv, kvacc, e)
        if e % 2 and 4 + e // 2 < nt:
            k = 4 + e // 2
            with jax.named_scope(f"qstep{k}"):
                gather_step(q_set, k)
            with jax.named_scope(f"qcross{k}"):
                gather_cross(q_set, k - 1)
            if k == 4:
                w_straight(1)
            if k == 5:
                w_straight(0)
            if k == 5:
                relays(1)
            if k == 7:
                relays(0)
            if e > 1:
                gather_last(q_set, e // 2 - 1)
                multiply(gq, qacc, e // 2 - 1)

    def rope(u):
        return u * cos_t[...] + pltpu.roll(u, HD // 2, 1) * sin_t[...]

    kv_all[b, :, :HD] = rope(kvacc[:, :HD]).astype(BF)
    kv_all[b, :, HD:] = kvacc[:, HD:].astype(BF)
    seg_all[b] = seg_ref[...]

    def keys(slot_b, sem, dev):
        return (remote(kv_all.at[slot_b], kv_all.at[slot_b], es.at[sem], er.at[sem], dev),
                remote(seg_all.at[slot_b], seg_all.at[slot_b], gs.at[sem], gr.at[sem], dev))

    low = b < nb // 2
    even = b % 2 == 0

    @pl.when(low)
    def _():
        for c in keys(b, 0, (bx, t)):
            c.start()

    @pl.when(even)
    def _():
        for c in keys(b, 1, (bc, t)):
            c.start()

    for k in range(8, nt):
        with jax.named_scope(f"qstep{k}"):
            gather_step(q_set, k)
        with jax.named_scope(f"qcross{k}"):
            gather_cross(q_set, k - 1)
    for e in range(nt // 2 - 1, nt):
        if e == nt - 3:
            with jax.named_scope("qcross8"):
                gather_cross(q_set, nt - 1)
        with jax.named_scope(f"qlast{e}"):
            gather_last(q_set, e)
        with jax.named_scope(f"qmul{e}"):
            multiply(gq, qacc, e)

    n_part = ctx_all.shape[1]
    qrows = n_tok // n_part
    for h in range(qc // HD):
        turned = rope(qacc[:, h * HD:(h + 1) * HD]).astype(BF)
        for part in range(n_part):
            qrot[part, h * qrows:(h + 1) * qrows, :] = turned[part * qrows:(part + 1) * qrows, :]

    @pl.when(b >= nb // 2)
    def _():
        for c in keys(bx, 0, (bx, t)):
            c.wait_recv()
        for c in keys(bx, 2, (bc, t)):
            c.start()
        for c in keys(flip(b, 3), 2, (bc, t)):
            c.wait_recv()

    @pl.when(b % 2 == 1)
    def _():
        for c in keys(bc, 1, (bc, t)):
            c.wait_recv()

    scale = HD ** (-0.5) * LOG2E
    across_qk = (((1,), (1,)), ((), ()))

    def mask_part(part):
        r0 = part * qrows
        sq = segq_ref[r0:r0 + qrows, :]
        seen = r0 + qrows
        ri = r0 + lax.broadcasted_iota(jnp.int32, (qrows, seen), 0)
        ci = lax.broadcasted_iota(jnp.int32, (qrows, seen), 1)
        vis = (ci <= ri) & (seg_all[b][:, :seen] == sq)
        masks[nb - 1, :, :seen] = jnp.where(vis, 0.0, NEGATIVE_FILL)

        def earlier(j, _):
            masks[j] = jnp.where(seg_all[j] == sq, jnp.zeros((qrows, n_tok), F32), NEGATIVE_FILL)
            return 0

        lax.fori_loop(0, b, earlier, 0)

    group = 4

    def attend(g, part):
        seen = (part + 1) * qrows
        rows_here = group * qrows
        qh = qrot[part, g * rows_here:(g + 1) * rows_here, :]

        def scored(kb, mask):
            s = lax.dot_general(qh, kb, across_qk, preferred_element_type=F32) * scale
            return (s.reshape(group, qrows, -1) + mask[None]).reshape(rows_here, -1)

        s = scored(kv_all[b, :seen, :HD], masks[nb - 1, :, :seen])
        m = jnp.max(s, axis=1, keepdims=True)
        p = jnp.exp2(s - m)
        l = jnp.sum(p, axis=1, keepdims=True)
        c = jnp.dot(p.astype(BF), kv_all[b, :seen, HD:], preferred_element_type=F32)

        def block(j, st):
            m, l, c = st
            s = scored(kv_all[j, :, :HD], masks[j])
            m2 = jnp.maximum(m, jnp.max(s, axis=1, keepdims=True))
            f = jnp.exp2(m - m2)
            p = jnp.exp2(s - m2)
            l = l * f + jnp.sum(p, axis=1, keepdims=True)
            c = c * f + jnp.dot(p.astype(BF), kv_all[j, :, HD:], preferred_element_type=F32)
            return (m2, l, c)

        m, l, c = lax.fori_loop(0, b, block, (m, l, c))
        return (c / l).astype(BF)

    def cpiece(z_half, y_side, part):
        return ctx_all.at[z_half, part, :, pl.ds(pl.multiple_of(y_side * qc, 128), qc)]

    def az(z_half, part):
        piece = cpiece(z_half, yy, part)
        return remote(piece, piece, azs.at[part], azr.at[part], (b, flip(t, nt // 2)))

    def ay(z_half, y_side, part, i):
        piece = cpiece(z_half, y_side, part)
        return remote(piece, piece, ays.at[part, i], ayr.at[part, i], (b, flip(t, 1)))

    def relay_ctx(part):
        az(1 - zi, part).wait_recv()
        ay(1 - zi, yy, part, 1).start()

    def partial(part, slot_side):
        acc = None
        for zh in range(2):
            one = lax.dot_general(ctx_all[zh, part], wo[2 * zh + slot_side], across_qk,
                                  preferred_element_type=F32)
            acc = one if acc is None else acc + one
        return acc

    z_low = (t // 2) % 2

    def pcopy(part):
        return remote(psend.at[part], prec.at[part], pss.at[part], prs.at[part], (b, flip(t, 2)))

    def homes(i):
        for k in range(nb):
            with jax.named_scope(f"whome{i}{k}"):
                w_home(flip(k_mine, k), i)

    def crosses(i):
        for k in range(nb):
            with jax.named_scope(f"wcross{i}{k}"):
                w_cross(flip(k_mine, k), i)

    def heads(part, g):
        with jax.named_scope(f"att{part}{g}"):
            both = attend(g, part)
            for e in range(group):
                col = pl.ds(pl.multiple_of(yy * qc + (g * group + e) * HD, 128), HD)
                ctx_all[zi, part, :, col] = both[e * qrows:(e + 1) * qrows, :]

    def send_ctx(part):
        az(zi, part).start()
        ay(zi, yy, part, 0).start()

    next_first = even_core != z_low

    def on(which, *steps):
        @pl.when(which)
        def _():
            for step in steps:
                step()

    def attention(part):
        mask_part(part)
        for g in range(qc // HD // group):
            heads(part, g)
        send_ctx(part)

    def last():
        with jax.named_scope("wlast"):
            for i in range(2):
                for k in range(nb):
                    w_last(flip(k_mine, k), i)

    def next_part(part):
        with jax.named_scope(f"ctxy{part}"):
            ay(zi, 1 - yy, part, 0).wait_recv()
            ay(1 - zi, 1 - yy, part, 1).wait_recv()
        with jax.named_scope(f"next{part}"):
            psend[part] = partial(part, 1 - z_low).astype(BF)
        pcopy(part).start()

    def own_part(part):
        toks = slice(part * qrows, (part + 1) * qrows)
        resid = x_ref[toks, pl.ds(pl.multiple_of(t * oc, 128), oc)].astype(F32)
        with jax.named_scope(f"own{part}"):
            oacc[toks, :] = resid + partial(part, z_low)

    def ctx_turn(part):
        with jax.named_scope(f"ctxrelay{part}"):
            relay_ctx(part)

    own_first = even_core == z_low
    middle = n_part // 2
    on(next_first, lambda: homes(0))
    for part in range(middle):
        attention(part)
    on(next_first, lambda: homes(1))
    for part in range(middle, n_part):
        attention(part)
    near = yy == zi
    on(own_first, lambda: homes(0))
    on(own_first & near, lambda: homes(1))
    for part in range(middle):
        ctx_turn(part)
    on(own_first & (yy != zi), lambda: homes(1))
    on(next_first, lambda: crosses(0), lambda: crosses(1))
    on(own_first, last)
    for part in range(middle, n_part):
        next_part(part - middle)
        ctx_turn(part)
    for part in range(n_part - middle, n_part):
        next_part(part)
    on(own_first, lambda: crosses(0), lambda: crosses(1))
    on(next_first, last)
    for part in range(n_part):
        own_part(part)
    for part in range(n_part):
        with jax.named_scope(f"prec{part}"):
            pcopy(part).wait_recv()
        toks = slice(part * qrows, (part + 1) * qrows)
        out_ref[toks, :] = (oacc[toks, :] + prec[part].astype(F32)).astype(BF)

    gather_sent(kv_set)
    gather_sent(q_set)

    @pl.when(low)
    def _():
        for c in keys(b, 0, (bx, t)):
            c.wait_send()

    @pl.when(even)
    def _():
        for c in keys(b, 1, (bc, t)):
            c.wait_send()

    @pl.when(b >= nb // 2)
    def _():
        for c in keys(bx, 2, (bc, t)):
            c.wait_send()

    for i in range(2):
        for side in range(2):
            to_relay(side, i).wait_send()
            delivered(straight(side, i))
            delivered(from_relay(side, i))
        for k in range(nb):
            w_x(b, k, i).wait_send()
            w_c(b, 0, k, i).wait_send()
            w_c(bx, 1, k, i).wait_send()
    for part in range(n_part):
        az(zi, part).wait_send()
        ay(zi, yy, part, 0).wait_send()
        ay(1 - zi, yy, part, 1).wait_send()
        pcopy(part).wait_send()


def fused(nb, nt, residual_in, norm_gain, w_query, w_key_value, query_bias, key_value_bias, w_output,
          device_map, positions, segments):
    n_tok, width = residual_in.shape
    rows = w_query.shape[0]
    qc, kc, oc = w_query.shape[1] // nt, w_key_value.shape[1] // nt, width // nt
    n = nb * nt
    inv = ROPE_BASE ** (-(np.arange(HD // 2, dtype=np.float64) * 2.0) / HD)
    inv = np.concatenate([inv, inv]).astype(np.float32)[None, :]
    any_, vm = pl.BlockSpec(memory_space=pl.ANY), pl.BlockSpec(memory_space=pltpu.VMEM)
    dma = pltpu.SemaphoreType.DMA
    return pl.pallas_call(
        functools.partial(fused_kernel, nb, nt),
        out_shape=jax.ShapeDtypeStruct((n_tok, oc), BF),
        in_specs=[pl.BlockSpec(memory_space=pltpu.SMEM), any_, any_, any_, vm, vm, vm, any_, vm, vm, vm],
        out_specs=vm,
        scratch_shapes=[
            pltpu.VMEM((n_tok, width), BF),
            pltpu.VMEM((n, n_tok, rows), BF),
            pltpu.VMEM((n, rows, qc), BF),
            pltpu.VMEM((n, rows, kc), BF),
            pltpu.VMEM((nb, oc, 2 * qc), BF),
            pltpu.VMEM((nb, n_tok, kc), BF),
            pltpu.VMEM((nb, 1, n_tok), jnp.int32),
            pltpu.VMEM((n_tok, qc), F32),
            pltpu.VMEM((n_tok, kc), F32),
            pltpu.VMEM((PARTS, n_tok // PARTS * (qc // HD), HD), BF),
            pltpu.VMEM((2, PARTS, n_tok // PARTS, 2 * qc), BF),
            pltpu.VMEM((n_tok, oc), F32),
            pltpu.VMEM((width // 128, 128), F32), pltpu.VMEM((qc * nt // HD, HD), F32),
            pltpu.VMEM((kc * nt // HD, HD), F32), pltpu.VMEM((n_tok, HD), F32),
            pltpu.VMEM((n_tok, HD), F32), pltpu.VMEM((n_tok, 1), jnp.int32),
            pltpu.VMEM((nb, n_tok // PARTS, n_tok), F32), pltpu.VMEM((PARTS, n_tok // PARTS, oc), BF),
            pltpu.VMEM((PARTS, n_tok // PARTS, oc), BF), dma((PARTS,)), dma((PARTS,)),
            dma, dma((3,)),
            dma((nt,)), dma((nt,)), dma((nt,)), dma((nt,)), dma((2 * nt,)), dma((2 * nt,)),
            dma((nt,)), dma((nt,)), dma((nt,)), dma((nt,)), dma((2 * nt,)), dma((2 * nt,)),
            dma((2, 2)), dma((nb, 2)), dma((nb, 2)), dma((nb, 2)), dma((2, nb, 2)), dma((2, nb, 2)),
            dma((nb,)), dma((nb,)), dma((nb,)), dma((nb,)),
            dma((PARTS,)), dma((PARTS,)), dma((PARTS, 2)), dma((PARTS, 2)),
            pltpu.VMEM((2, 2, rows, qc), BF), dma((2, 2)), dma((2, 2)), dma((2, 2)),
        ],
        compiler_params=pltpu.CompilerParams(
            collective_id=0, has_side_effects=True, vmem_limit_bytes=63 * 1024 * 1024),
    )(device_map, residual_in, w_query, w_key_value, norm_gain.reshape(-1, 128), query_bias.reshape(-1, HD),
      key_value_bias.reshape(-1, HD), w_output.T, jnp.asarray(inv), positions[None, :], segments[None, :])


def route(shape, *args):
    nb, nt = shape["blk"], shape["tp"]
    n_tok, width = args[0].shape
    rows = args[2].shape[0]
    qc, kc, oc = args[2].shape[1] // nt, args[3].shape[1] // nt, width // nt
    fits = (nb == 4 and nt == KVH and rows % 32 == 0 and rows <= 160 and qc == 4 * HD and kc == 2 * HD
            and oc == nb * rows and oc % 128 == 0 and width % 128 == 0 and n_tok % 256 == 0)
    if fits:
        return fused(nb, nt, *args)
    return per_device(*args)


def solution(mesh):
    in_specs = (
        P("blk", None),
        P(),
        P(("blk", "tp"), None),
        P(("blk", "tp"), None),
        P(),
        P(),
        P(None, ("blk", "tp")),
        P(),
        P("blk"),
        P("blk"),
    )
    out_specs = P("blk", "tp")
    return jax.shard_map(
        functools.partial(route, dict(mesh.shape)), mesh=mesh, in_specs=in_specs, out_specs=out_specs, check_vma=False
    )
```

```python
import functools

import jax
import jax.numpy as jnp
import numpy as np
from jax import lax
from jax.experimental import pallas as pl
from jax.experimental.pallas import tpu as pltpu
from jax.sharding import PartitionSpec as P

D = 5120
KVH = 8
HD = 128


NORM_FLOOR = 0.0625
ROPE_BASE = 1000000.0
NEGATIVE_FILL = -1e30
LOG2E = 1.4426950408889634
PARTS = 4


def for_sending(x):
    return jax.tree.map(lambda a: a.astype(jnp.bfloat16) if a.dtype == jnp.float32 else a, x)


def from_partner(block, axis, bit):
    count = lax.axis_size(axis)
    route = []
    for low in range(count):
        high = low | 1 << bit
        if high != low and high < count:
            route += [(low, high), (high, low)]
    return lax.ppermute(block, axis, route)


def rope_tables(positions, head_width):
    half_width = head_width // 2
    frequency = ROPE_BASE ** (-(jnp.arange(half_width, dtype=jnp.float32) * 2.0) / head_width)
    angles = positions.astype(jnp.float32)[:, None] * frequency[None, :]
    angles = jnp.concatenate([angles, angles], axis=1)
    return (jnp.cos(angles), jnp.sin(angles))


def rotate(values, cosine_table, sine_table):
    half_width = values.shape[-1] // 2
    turned = jnp.concatenate([-values[..., half_width:], values[..., :half_width]], axis=-1)
    return values * cosine_table[:, None, :] + turned * sine_table[:, None, :]


def join_pair(mine_cols, partner, is_lower):
    return jnp.where(
        is_lower,
        jnp.concatenate([mine_cols, partner], axis=1),
        jnp.concatenate([partner, mine_cols], axis=1),
    )


def per_device(
    residual_in,
    norm_gain,
    w_query,
    w_key_value,
    query_bias,
    key_value_bias,
    w_output,
    device_map,
    positions,
    segments,
):
    tp_count = lax.axis_size("tp")
    tp_index = lax.axis_index("tp")
    blk_index = lax.axis_index("blk")
    local_tokens = residual_in.shape[0]
    shard_rows = w_query.shape[0]
    kv_group = tp_count // KVH
    floats = residual_in.astype(jnp.float32)
    square = jnp.maximum(jnp.mean(floats * floats, axis=1, keepdims=True), NORM_FLOOR)
    normed = (floats * lax.rsqrt(square) * norm_gain.astype(jnp.float32)).astype(jnp.bfloat16)
    ordered = jnp.take(
        normed.reshape(local_tokens, device_map.shape[0], shard_rows), device_map, axis=1
    ).reshape(local_tokens, D)
    moved_query, moved_pairs = (
        lax.all_to_all(w_query, "tp", split_axis=1, concat_axis=0, tiled=True),
        lax.all_to_all(w_key_value, "tp", split_axis=1, concat_axis=0, tiled=True),
    )
    for bit_level in range(kv_group.bit_length() - 1):
        partner = from_partner(for_sending(moved_pairs), "tp", bit_level).astype(moved_pairs.dtype)
        moved_pairs = join_pair(moved_pairs, partner, tp_index >> bit_level & 1 == 0)
    queries = jnp.dot(
        ordered,
        lax.all_gather(moved_query, "blk", axis=0, tiled=True),
        preferred_element_type=jnp.float32,
    )
    key_value = jnp.dot(
        ordered,
        lax.all_gather(moved_pairs, "blk", axis=0, tiled=True),
        preferred_element_type=jnp.float32,
    )
    query_width = queries.shape[1]
    heads_here = query_width // HD
    kv_head = tp_index // kv_group
    queries = queries + lax.dynamic_slice_in_dim(
        query_bias, tp_index * query_width, query_width
    ).astype(jnp.float32)
    key_value = key_value + lax.dynamic_slice_in_dim(
        key_value_bias, kv_head * 2 * HD, 2 * HD
    ).astype(jnp.float32)
    cosine_table, sine_table = rope_tables(positions, HD)
    query_rot = rotate(
        queries.reshape(local_tokens, heads_here, HD), cosine_table, sine_table
    ).astype(jnp.bfloat16)
    key_rot = rotate(key_value[:, None, :HD], cosine_table, sine_table)[:, 0, :].astype(
        jnp.bfloat16
    )
    values = key_value[:, HD:].astype(jnp.bfloat16)
    attend_scale = HD ** (-0.5)
    row_index = blk_index * local_tokens + jnp.arange(local_tokens, dtype=jnp.int32)
    initial = (
        jnp.full((heads_here, local_tokens), NEGATIVE_FILL, jnp.float32),
        jnp.zeros((heads_here, local_tokens), jnp.float32),
        jnp.zeros((heads_here, local_tokens, HD), jnp.float32),
    )
    key_piece = lax.all_gather(key_rot, "blk", axis=0, tiled=True)
    value_piece = lax.all_gather(values, "blk", axis=0, tiled=True)
    segment_piece = lax.all_gather(segments, "blk", axis=0, tiled=True)
    piece_rows = key_piece.shape[0]
    key_block_rows = 512

    def one_block(block_number, state_now):
        run_peak, run_mass, context = state_now
        block_start = block_number * key_block_rows
        key_block = lax.dynamic_slice_in_dim(key_piece, block_start, key_block_rows, 0)
        value_block = lax.dynamic_slice_in_dim(value_piece, block_start, key_block_rows, 0)
        segment_block = lax.dynamic_slice_in_dim(segment_piece, block_start, key_block_rows, 0)
        scores = (
            jnp.einsum("qhd,kd->hqk", query_rot, key_block, preferred_element_type=jnp.float32)
            * attend_scale
        )
        key_index = block_start + jnp.arange(key_block_rows, dtype=jnp.int32)
        visible = (key_index[None, :] <= row_index[:, None]) & (
            segment_block[None, :] == segments[:, None]
        )
        masked = jnp.where(visible[None], scores, NEGATIVE_FILL)
        new_peak = jnp.maximum(run_peak, jnp.max(masked, axis=2))
        factor = jnp.exp(run_peak - new_peak)
        raw_weights = jnp.where(visible[None], jnp.exp(masked - new_peak[:, :, None]), 0.0)
        run_mass = run_mass * factor + jnp.sum(raw_weights, axis=2)
        context = context * factor[:, :, None] + jnp.einsum(
            "hqk,kd->hqd",
            raw_weights.astype(jnp.bfloat16),
            value_block,
            preferred_element_type=jnp.float32,
        )
        return (new_peak, run_mass, context)

    run_peak, run_mass, context = lax.fori_loop(0, piece_rows // key_block_rows, one_block, initial)
    context_flat = (
        (context / run_mass[:, :, None])
        .transpose(1, 0, 2)
        .reshape(local_tokens, query_width)
        .astype(jnp.bfloat16)
    )
    width_out = D // tp_count
    moved_out = lax.all_to_all(w_output, "tp", split_axis=0, concat_axis=1, tiled=True)
    row_terms = jnp.dot(
        context_flat,
        lax.all_gather(moved_out, "blk", axis=1, tiled=True),
        preferred_element_type=jnp.float32,
    )
    summed = lax.psum_scatter(
        row_terms.astype(jnp.bfloat16), "tp", scatter_dimension=1, tiled=True
    ).astype(jnp.float32)
    residual_part = lax.dynamic_slice_in_dim(residual_in, tp_index * width_out, width_out, 1)
    return (residual_part.astype(jnp.float32) + summed).astype(jnp.bfloat16)


MESH = pl.DeviceIdType.MESH
BF = jnp.bfloat16
F32 = jnp.float32


def flip(i, mask):
    out = i
    for bit in range(mask.bit_length()):
        if mask >> bit & 1:
            out = out + (1 << bit) * (1 - 2 * ((i // (1 << bit)) % 2))
    return out


def fused_kernel(nb, nt, dm_ref, x_hbm, wq_hbm, wkv_hbm, gain_ref, bq_ref, bkv_ref, wo_hbm, inv_ref,
                 pos_ref, seg_ref, out_ref, x_ref, xo, gq, gkv, wo, kv_all, seg_all, qacc,
                 kvacc, qrot, ctx_all, oacc, gain32, bq32, bkv32, cos_t, sin_t, segq_ref,
                 masks, psend, prec, pss, prs,
                 x_sem, loc_sem, kv1s, kv1r, kvxs, kvxr, kvcs, kvcr, q1s, q1r, qxs, qxr, qcs, qcr,
                 w1s, w1r, wxs, wxr, wcs, wcr, es, er, gs, gr, azs, azr, ays, ayr, wrel, rs, rr, r2s):
    b = lax.axis_index("blk")
    t = lax.axis_index("tp")
    n_tok, width = x_ref.shape
    rows = wq_hbm.shape[0]
    qc, kc = gq.shape[2], gkv.shape[2]
    oc = wo.shape[1]
    bx, bc = flip(b, 2), flip(b, 1)

    barrier = pltpu.get_barrier_semaphore()
    peers = [(b, flip(t, k)) for k in range(1, nt)] + [(flip(b, k), t) for k in range(1, nb)]
    peers += [(bx, flip(t, 1))]
    for peer in peers:
        pl.semaphore_signal(barrier, inc=1, device_id=peer, device_id_type=MESH)
    x_in = pltpu.make_async_copy(x_hbm, x_ref, x_sem)
    x_in.start()
    gain32[...] = gain_ref[...].astype(F32)
    bq32[...] = bq_ref[...].astype(F32)
    bkv32[...] = bkv_ref[...].astype(F32)
    with jax.named_scope("barrier"):
        pl.semaphore_wait(barrier, len(peers))

    def remote(src, dst, ss, rs, dev):
        return pltpu.make_async_remote_copy(src_ref=src, dst_ref=dst, send_sem=ss, recv_sem=rs,
                                            device_id=dev, device_id_type=MESH)

    def slot(bb, k):
        return bb * nt + flip(t, k)

    def stage_one(hbm, buf, width, k, ss, rs, local):
        cols = pl.ds(pl.multiple_of(flip(t, k) * width, 128), width)
        mine = buf.at[b * nt + t]
        if k == 0:
            return pltpu.make_async_copy(hbm.at[:, cols], mine, local)
        return remote(hbm.at[:, cols], mine, ss.at[k], rs.at[k], (b, flip(t, k)))

    def stage_one_in(buf, hbm, width, k, ss, rs, local):
        if k == 0:
            return stage_one(hbm, buf, width, 0, ss, rs, local)
        piece = buf.at[slot(b, k)]
        return remote(piece, piece, ss.at[k], rs.at[k], (b, flip(t, k)))

    def forward(buf, bb, k, ss, rs, i, dev):
        piece = buf.at[slot(bb, k)]
        return remote(piece, piece, ss.at[i], rs.at[i], dev)

    kv_set = (wkv_hbm, gkv, kc, kv1s, kv1r, kvxs, kvxr, kvcs, kvcr, loc_sem.at[0])
    q_set = (wq_hbm, gq, qc, q1s, q1r, qxs, qxr, qcs, qcr, loc_sem.at[1])

    order = [0, 1, 2, 4, 3, 6, 5, 7]

    def across(ws, k):
        hbm, buf, width, s1, r1, xs, xr, cs, cr, loc = ws
        cols = pl.ds(pl.multiple_of(flip(t, k) * width, 128), width)
        return remote(hbm.at[:, cols], buf.at[b * nt + t], xs.at[k], xr.at[k], (bx, flip(t, k)))

    def start_one(ws, k):
        hbm, buf, width, s1, r1, xs, xr, cs, cr, loc = ws
        stage_one(hbm, buf, width, k, s1, r1, loc).start()
        if k < 2:
            across(ws, k).start()

    def gather_step(ws, i):
        k = order[i]
        hbm, buf, width, s1, r1, xs, xr, cs, cr, loc = ws
        arrived = stage_one_in(buf, hbm, width, k, s1, r1, loc)
        if k == 0:
            arrived.wait()
        else:
            arrived.wait_recv()
        if k > 1:
            forward(buf, b, k, xs, xr, k, (bx, t)).start()
        forward(buf, b, k, cs, cr, k, (bc, t)).start()

    def gather_cross(ws, i):
        k = order[i]
        hbm, buf, width, s1, r1, xs, xr, cs, cr, loc = ws
        forward(buf, bx, k, xs, xr, k, (bx, t)).wait_recv()
        forward(buf, bx, k, cs, cr, nt + k, (bc, t)).start()

    def gather_last(ws, i):
        k = order[i]
        hbm, buf, width, s1, r1, xs, xr, cs, cr, loc = ws
        forward(buf, bc, k, cs, cr, k, (bc, t)).wait_recv()
        forward(buf, flip(b, 3), k, cs, cr, nt + k, (bc, t)).wait_recv()

    def gather_sent(ws):
        hbm, buf, width, s1, r1, xs, xr, cs, cr, loc = ws
        for k in range(nt):
            if k:
                stage_one(hbm, buf, width, k, s1, r1, loc).wait_send()
            if k < 2:
                across(ws, k).wait_send()
            else:
                forward(buf, b, k, xs, xr, k, (bx, t)).wait_send()
            forward(buf, b, k, cs, cr, k, (bc, t)).wait_send()
            forward(buf, bx, k, cs, cr, nt + k, (bc, t)).wait_send()

    def multiply(buf, acc, i):
        k = order[i]

        def one(j, _):
            s = slot(j, k)
            acc[...] += jnp.dot(xo[dm_ref[s]], buf[s], preferred_element_type=F32)
            return 0
        lax.fori_loop(0, nb, one, 0)

    issue = [0,2,4,1,6,3,5,7]
    for k in issue:
        start_one(kv_set, k)

    x_in.wait()
    tile = n_tok // nt

    def norm_tile(i):
        toks = slice(i * tile, (i + 1) * tile)
        v = x_ref[toks, :].astype(F32)
        scale = lax.rsqrt(jnp.maximum(jnp.mean(v * v, axis=1, keepdims=True), NORM_FLOOR))

        def spread(g, _):
            per = 4 * rows // 128
            gain = jnp.concatenate([gain32[pl.ds(g * per + i, 1), :] for i in range(per)], axis=1)
            u = x_ref[toks, pl.ds(pl.multiple_of(g * 4 * rows, 128), 4 * rows)].astype(F32)
            u = (u * scale * gain).astype(BF)
            for i in range(4):
                xo[g * 4 + i, toks, :] = u[:, i * rows:(i + 1) * rows]
            return 0

        lax.fori_loop(0, nb * nt // 4, spread, 0)

    def tables():
        pos = jnp.broadcast_to(pos_ref[...].astype(F32), (HD, n_tok)).T
        angles = pos * inv_ref[...]
        cos_t[...] = jnp.cos(angles)
        sign = jnp.where(lax.broadcasted_iota(jnp.int32, (1, HD), 1) < HD // 2, -1.0, 1.0)
        sin_t[...] = jnp.sin(angles) * sign
        segq_ref[...] = jnp.broadcast_to(seg_ref[...].astype(F32), (HD, n_tok)).T[:, :1].astype(jnp.int32)

    zi, yy = t // (nt // 2), t % 2
    k_mine = t % nb
    even_core = b % 2

    def wsrc(c, i):
        return wo_hbm.at[:, pl.ds(pl.multiple_of((c * 2 + i) * qc, 128), qc)]

    def wpiece(slot, k, i):
        return wo.at[slot, pl.ds(pl.multiple_of(k * rows, 16), rows), i * qc:(i + 1) * qc]

    def mine_or_next(side, owner):
        col = owner * 2 + t // nb
        return (even_core, col) if side == 0 else (1 - even_core, flip(col, 2))

    def straight(side, i):
        c, dest = mine_or_next(side, b)
        return dest, wsrc(c, i), wpiece(even_core, k_mine, i), w1s.at[side, i], w1r.at[k_mine, i]

    def to_relay(side, i):
        c, _ = mine_or_next(side, bx)
        return remote(wsrc(2 + c, i), wrel.at[side, i], rs.at[side, i], rr.at[side, i], (bx, t))

    def from_relay(side, i):
        _, dest = mine_or_next(side, bx)
        return dest, wrel.at[side, i], wpiece(2 + even_core, k_mine, i), r2s.at[side, i], w1r.at[k_mine, i]

    def deliver(what):
        dest, src, dst, ss, sr = what

        @pl.when(dest != t)
        def _():
            remote(src, dst, ss, sr, (b, dest)).start()

        @pl.when(dest == t)
        def _():
            pltpu.make_async_copy(src, dst, sr).start()

    def delivered(what):
        dest, src, dst, ss, sr = what

        @pl.when(dest != t)
        def _():
            remote(src, dst, ss, sr, (b, dest)).wait_send()

    def whalf(bb, k, i):
        return wpiece(2 * ((bb // 2 + zi) % 2) + bb % 2, k, i)

    def w_x(bb, k, i):
        return remote(whalf(bb, k, i), whalf(bb, k, i), wxs.at[k, i], wxr.at[k, i], (bx, t))

    def w_c(bb, u, k, i):
        return remote(whalf(bb, k, i), whalf(bb, k, i), wcs.at[u, k, i], wcr.at[u, k, i], (bc, t))

    def w_home(k, i):
        remote(whalf(b, k, i), whalf(b, k, i), w1s.at[0, i], w1r.at[k, i], (bx, t)).wait_recv()
        w_x(b, k, i).start()
        w_c(b, 0, k, i).start()

    def w_cross(k, i):
        w_x(bx, k, i).wait_recv()
        w_c(bx, 1, k, i).start()

    def w_last(k, i):
        w_c(bc, 0, k, i).wait_recv()
        w_c(flip(b, 3), 1, k, i).wait_recv()

    def w_straight(side):
        for i in range(2):
            deliver(straight(side, i))

    def w_start(side):
        for i in range(2):
            to_relay(side, i).start()

    def w_relay(side, i):
        to_relay(side, i).wait_recv()
        deliver(from_relay(side, i))

    def relays(side):
        for i in range(2):
            with jax.named_scope(f"wrelay{i}{side}"):
                w_relay(side, i)

    for k in range(nt):
        with jax.named_scope(f"norm{k}"):
            norm_tile(k)
        with jax.named_scope(f"kvstep{k}"):
            gather_step(kv_set, k)
        if k >= 2:
            start_one(q_set, issue[k - 2])
        if k == 4:
            w_start(1)
        if k == 6:
            w_start(0)
        if k:
            with jax.named_scope(f"kvcross{k}"):
                gather_cross(kv_set, k - 1)
    for k in range(nt - 2, nt):
        start_one(q_set, issue[k])
    with jax.named_scope("tables"):
        tables()
    with jax.named_scope("kvcross8"):
        gather_cross(kv_set, nt - 1)

    for e in range(2):
        kvacc[:, e * HD:(e + 1) * HD] = jnp.broadcast_to(bkv32[pl.ds(t * 2 + e, 1), :], (n_tok, HD))
    for k in range(4):
        with jax.named_scope(f"qstep{k}"):
            gather_step(q_set, k)
        if k:
            with jax.named_scope(f"qcross{k}"):
                gather_cross(q_set, k - 1)
    for e in range(qc // HD):
        qacc[:, e * HD:(e + 1) * HD] = jnp.broadcast_to(
            bq32[pl.ds(t * (qc // HD) + e, 1), :], (n_tok, HD))
    for e in range(nt):
        gather_last(kv_set, e)
        with jax.named_scope(f"kvmul{e}"):
            multiply(gkv, kvacc, e)
        if e % 2 and 4 + e // 2 < nt:
            k = 4 + e // 2
            with jax.named_scope(f"qstep{k}"):
                gather_step(q_set, k)
            with jax.named_scope(f"qcross{k}"):
                gather_cross(q_set, k - 1)
            if k == 4:
                w_straight(1)
            if k == 5:
                w_straight(0)
            if k == 4:
                relays(1)
            if k == 6:
                relays(0)
            if e > 1:
                gather_last(q_set, e // 2 - 1)
                multiply(gq, qacc, e // 2 - 1)

    def rope(u):
        return u * cos_t[...] + pltpu.roll(u, HD // 2, 1) * sin_t[...]

    kv_all[b, :, :HD] = rope(kvacc[:, :HD]).astype(BF)
    kv_all[b, :, HD:] = kvacc[:, HD:].astype(BF)
    seg_all[b] = seg_ref[...]

    def keys(slot_b, sem, dev):
        return (remote(kv_all.at[slot_b], kv_all.at[slot_b], es.at[sem], er.at[sem], dev),
                remote(seg_all.at[slot_b], seg_all.at[slot_b], gs.at[sem], gr.at[sem], dev))

    low = b < nb // 2
    even = b % 2 == 0

    @pl.when(low)
    def _():
        for c in keys(b, 0, (bx, t)):
            c.start()

    @pl.when(even)
    def _():
        for c in keys(b, 1, (bc, t)):
            c.start()

    for k in range(8, nt):
        with jax.named_scope(f"qstep{k}"):
            gather_step(q_set, k)
        with jax.named_scope(f"qcross{k}"):
            gather_cross(q_set, k - 1)
    for e in range(nt // 2 - 1, nt):
        if e == nt - 3:
            with jax.named_scope("qcross8"):
                gather_cross(q_set, nt - 1)
        with jax.named_scope(f"qlast{e}"):
            gather_last(q_set, e)
        with jax.named_scope(f"qmul{e}"):
            multiply(gq, qacc, e)

    n_part = ctx_all.shape[1]
    qrows = n_tok // n_part
    for h in range(qc // HD):
        turned = rope(qacc[:, h * HD:(h + 1) * HD]).astype(BF)
        for part in range(n_part):
            qrot[part, h * qrows:(h + 1) * qrows, :] = turned[part * qrows:(part + 1) * qrows, :]

    @pl.when(b >= nb // 2)
    def _():
        for c in keys(bx, 0, (bx, t)):
            c.wait_recv()
        for c in keys(bx, 2, (bc, t)):
            c.start()
        for c in keys(flip(b, 3), 2, (bc, t)):
            c.wait_recv()

    @pl.when(b % 2 == 1)
    def _():
        for c in keys(bc, 1, (bc, t)):
            c.wait_recv()

    scale = HD ** (-0.5) * LOG2E
    across_qk = (((1,), (1,)), ((), ()))

    def mask_part(part):
        r0 = part * qrows
        sq = segq_ref[r0:r0 + qrows, :]
        seen = r0 + qrows
        ri = r0 + lax.broadcasted_iota(jnp.int32, (qrows, seen), 0)
        ci = lax.broadcasted_iota(jnp.int32, (qrows, seen), 1)
        vis = (ci <= ri) & (seg_all[b][:, :seen] == sq)
        masks[nb - 1, :, :seen] = jnp.where(vis, 0.0, NEGATIVE_FILL)

        def earlier(j, _):
            masks[j] = jnp.where(seg_all[j] == sq, jnp.zeros((qrows, n_tok), F32), NEGATIVE_FILL)
            return 0

        lax.fori_loop(0, b, earlier, 0)

    group = 4

    def attend(g, part):
        seen = (part + 1) * qrows
        rows_here = group * qrows
        qh = qrot[part, g * rows_here:(g + 1) * rows_here, :]

        def scored(kb, mask):
            s = lax.dot_general(qh, kb, across_qk, preferred_element_type=F32) * scale
            return (s.reshape(group, qrows, -1) + mask[None]).reshape(rows_here, -1)

        s = scored(kv_all[b, :seen, :HD], masks[nb - 1, :, :seen])
        m = jnp.max(s, axis=1, keepdims=True)
        p = jnp.exp2(s - m)
        l = jnp.sum(p, axis=1, keepdims=True)
        c = jnp.dot(p.astype(BF), kv_all[b, :seen, HD:], preferred_element_type=F32)

        def block(j, st):
            m, l, c = st
            s = scored(kv_all[j, :, :HD], masks[j])
            m2 = jnp.maximum(m, jnp.max(s, axis=1, keepdims=True))
            f = jnp.exp2(m - m2)
            p = jnp.exp2(s - m2)
            l = l * f + jnp.sum(p, axis=1, keepdims=True)
            c = c * f + jnp.dot(p.astype(BF), kv_all[j, :, HD:], preferred_element_type=F32)
            return (m2, l, c)

        m, l, c = lax.fori_loop(0, b, block, (m, l, c))
        return (c / l).astype(BF)

    def cpiece(z_half, y_side, part):
        return ctx_all.at[z_half, part, :, pl.ds(pl.multiple_of(y_side * qc, 128), qc)]

    def az(z_half, part):
        piece = cpiece(z_half, yy, part)
        return remote(piece, piece, azs.at[part], azr.at[part], (b, flip(t, nt // 2)))

    def ay(z_half, y_side, part, i):
        piece = cpiece(z_half, y_side, part)
        return remote(piece, piece, ays.at[part, i], ayr.at[part, i], (b, flip(t, 1)))

    def relay_ctx(part):
        az(1 - zi, part).wait_recv()
        ay(1 - zi, yy, part, 1).start()

    def partial(part, slot_side):
        acc = None
        for zh in range(2):
            one = lax.dot_general(ctx_all[zh, part], wo[2 * zh + slot_side], across_qk,
                                  preferred_element_type=F32)
            acc = one if acc is None else acc + one
        return acc

    z_low = (t // 2) % 2

    def pcopy(part):
        return remote(psend.at[part], prec.at[part], pss.at[part], prs.at[part], (b, flip(t, 2)))

    def homes(i):
        for k in range(nb):
            with jax.named_scope(f"whome{i}{k}"):
                w_home(flip(k_mine, k), i)

    def crosses(i):
        for k in range(nb):
            with jax.named_scope(f"wcross{i}{k}"):
                w_cross(flip(k_mine, k), i)

    def heads(part, g):
        with jax.named_scope(f"att{part}{g}"):
            both = attend(g, part)
            for e in range(group):
                col = pl.ds(pl.multiple_of(yy * qc + (g * group + e) * HD, 128), HD)
                ctx_all[zi, part, :, col] = both[e * qrows:(e + 1) * qrows, :]

    def send_ctx(part):
        az(zi, part).start()
        ay(zi, yy, part, 0).start()

    next_first = even_core != z_low

    def on(which, *steps):
        @pl.when(which)
        def _():
            for step in steps:
                step()

    def attention(part):
        mask_part(part)
        for g in range(qc // HD // group):
            heads(part, g)
        send_ctx(part)

    def last():
        with jax.named_scope("wlast"):
            for i in range(2):
                for k in range(nb):
                    w_last(flip(k_mine, k), i)

    def next_part(part):
        with jax.named_scope(f"ctxy{part}"):
            ay(zi, 1 - yy, part, 0).wait_recv()
            ay(1 - zi, 1 - yy, part, 1).wait_recv()
        with jax.named_scope(f"next{part}"):
            psend[part] = partial(part, 1 - z_low).astype(BF)
        pcopy(part).start()

    def own_part(part):
        toks = slice(part * qrows, (part + 1) * qrows)
        resid = x_ref[toks, pl.ds(pl.multiple_of(t * oc, 128), oc)].astype(F32)
        with jax.named_scope(f"own{part}"):
            oacc[toks, :] = resid + partial(part, z_low)

    def ctx_turn(part):
        with jax.named_scope(f"ctxrelay{part}"):
            relay_ctx(part)

    own_first = even_core == z_low
    middle = n_part // 2
    on(next_first, lambda: homes(0))
    for part in range(middle):
        attention(part)
    on(next_first, lambda: homes(1))
    for part in range(middle, n_part):
        attention(part)
    near = yy == zi
    on(own_first, lambda: homes(0))
    on(own_first & near, lambda: homes(1))
    for part in range(middle):
        ctx_turn(part)
    on(own_first & (yy != zi), lambda: homes(1))
    on(next_first, lambda: crosses(0), lambda: crosses(1))
    on(own_first, last)
    for part in range(middle, n_part):
        next_part(part - middle)
        if part - middle == 1:
            on(own_first & near, lambda: crosses(0), lambda: crosses(1))
        ctx_turn(part)
    for part in range(n_part - middle, n_part - 1):
        next_part(part)
    on(own_first & (yy != zi), lambda: crosses(0), lambda: crosses(1))
    next_part(n_part - 1)
    on(next_first, last)
    for part in range(n_part):
        own_part(part)
    for part in range(n_part):
        with jax.named_scope(f"prec{part}"):
            pcopy(part).wait_recv()
        toks = slice(part * qrows, (part + 1) * qrows)
        out_ref[toks, :] = (oacc[toks, :] + prec[part].astype(F32)).astype(BF)

    gather_sent(kv_set)
    gather_sent(q_set)

    @pl.when(low)
    def _():
        for c in keys(b, 0, (bx, t)):
            c.wait_send()

    @pl.when(even)
    def _():
        for c in keys(b, 1, (bc, t)):
            c.wait_send()

    @pl.when(b >= nb // 2)
    def _():
        for c in keys(bx, 2, (bc, t)):
            c.wait_send()

    for i in range(2):
        for side in range(2):
            to_relay(side, i).wait_send()
            delivered(straight(side, i))
            delivered(from_relay(side, i))
        for k in range(nb):
            w_x(b, k, i).wait_send()
            w_c(b, 0, k, i).wait_send()
            w_c(bx, 1, k, i).wait_send()
    for part in range(n_part):
        az(zi, part).wait_send()
        ay(zi, yy, part, 0).wait_send()
        ay(1 - zi, yy, part, 1).wait_send()
        pcopy(part).wait_send()


def fused(nb, nt, residual_in, norm_gain, w_query, w_key_value, query_bias, key_value_bias, w_output,
          device_map, positions, segments):
    n_tok, width = residual_in.shape
    rows = w_query.shape[0]
    qc, kc, oc = w_query.shape[1] // nt, w_key_value.shape[1] // nt, width // nt
    n = nb * nt
    inv = ROPE_BASE ** (-(np.arange(HD // 2, dtype=np.float64) * 2.0) / HD)
    inv = np.concatenate([inv, inv]).astype(np.float32)[None, :]
    any_, vm = pl.BlockSpec(memory_space=pl.ANY), pl.BlockSpec(memory_space=pltpu.VMEM)
    dma = pltpu.SemaphoreType.DMA
    return pl.pallas_call(
        functools.partial(fused_kernel, nb, nt),
        out_shape=jax.ShapeDtypeStruct((n_tok, oc), BF),
        in_specs=[pl.BlockSpec(memory_space=pltpu.SMEM), any_, any_, any_, vm, vm, vm, any_, vm, vm, vm],
        out_specs=vm,
        scratch_shapes=[
            pltpu.VMEM((n_tok, width), BF),
            pltpu.VMEM((n, n_tok, rows), BF),
            pltpu.VMEM((n, rows, qc), BF),
            pltpu.VMEM((n, rows, kc), BF),
            pltpu.VMEM((nb, oc, 2 * qc), BF),
            pltpu.VMEM((nb, n_tok, kc), BF),
            pltpu.VMEM((nb, 1, n_tok), jnp.int32),
            pltpu.VMEM((n_tok, qc), F32),
            pltpu.VMEM((n_tok, kc), F32),
            pltpu.VMEM((PARTS, n_tok // PARTS * (qc // HD), HD), BF),
            pltpu.VMEM((2, PARTS, n_tok // PARTS, 2 * qc), BF),
            pltpu.VMEM((n_tok, oc), F32),
            pltpu.VMEM((width // 128, 128), F32), pltpu.VMEM((qc * nt // HD, HD), F32),
            pltpu.VMEM((kc * nt // HD, HD), F32), pltpu.VMEM((n_tok, HD), F32),
            pltpu.VMEM((n_tok, HD), F32), pltpu.VMEM((n_tok, 1), jnp.int32),
            pltpu.VMEM((nb, n_tok // PARTS, n_tok), F32), pltpu.VMEM((PARTS, n_tok // PARTS, oc), BF),
            pltpu.VMEM((PARTS, n_tok // PARTS, oc), BF), dma((PARTS,)), dma((PARTS,)),
            dma, dma((3,)),
            dma((nt,)), dma((nt,)), dma((nt,)), dma((nt,)), dma((2 * nt,)), dma((2 * nt,)),
            dma((nt,)), dma((nt,)), dma((nt,)), dma((nt,)), dma((2 * nt,)), dma((2 * nt,)),
            dma((2, 2)), dma((nb, 2)), dma((nb, 2)), dma((nb, 2)), dma((2, nb, 2)), dma((2, nb, 2)),
            dma((nb,)), dma((nb,)), dma((nb,)), dma((nb,)),
            dma((PARTS,)), dma((PARTS,)), dma((PARTS, 2)), dma((PARTS, 2)),
            pltpu.VMEM((2, 2, rows, qc), BF), dma((2, 2)), dma((2, 2)), dma((2, 2)),
        ],
        compiler_params=pltpu.CompilerParams(
            collective_id=0, has_side_effects=True, vmem_limit_bytes=63 * 1024 * 1024),
    )(device_map, residual_in, w_query, w_key_value, norm_gain.reshape(-1, 128), query_bias.reshape(-1, HD),
      key_value_bias.reshape(-1, HD), w_output.T, jnp.asarray(inv), positions[None, :], segments[None, :])


def route(shape, *args):
    nb, nt = shape["blk"], shape["tp"]
    n_tok, width = args[0].shape
    rows = args[2].shape[0]
    qc, kc, oc = args[2].shape[1] // nt, args[3].shape[1] // nt, width // nt
    fits = (nb == 4 and nt == KVH and rows % 32 == 0 and rows <= 160 and qc == 4 * HD and kc == 2 * HD
            and oc == nb * rows and oc % 128 == 0 and width % 128 == 0 and n_tok % 256 == 0)
    if fits:
        return fused(nb, nt, *args)
    return per_device(*args)


def solution(mesh):
    in_specs = (
        P("blk", None),
        P(),
        P(("blk", "tp"), None),
        P(("blk", "tp"), None),
        P(),
        P(),
        P(None, ("blk", "tp")),
        P(),
        P("blk"),
        P("blk"),
    )
    out_specs = P("blk", "tp")
    return jax.shard_map(
        functools.partial(route, dict(mesh.shape)), mesh=mesh, in_specs=in_specs, out_specs=out_specs, check_vma=False
    )
```

```python
import functools

import jax
import jax.numpy as jnp
import numpy as np
from jax import lax
from jax.experimental import pallas as pl
from jax.experimental.pallas import tpu as pltpu
from jax.sharding import PartitionSpec as P

D = 5120
KVH = 8
HD = 128


NORM_FLOOR = 0.0625
ROPE_BASE = 1000000.0
NEGATIVE_FILL = -1e30
LOG2E = 1.4426950408889634
PARTS = 4


def for_sending(x):
    return jax.tree.map(lambda a: a.astype(jnp.bfloat16) if a.dtype == jnp.float32 else a, x)


def from_partner(block, axis, bit):
    count = lax.axis_size(axis)
    route = []
    for low in range(count):
        high = low | 1 << bit
        if high != low and high < count:
            route += [(low, high), (high, low)]
    return lax.ppermute(block, axis, route)


def rope_tables(positions, head_width):
    half_width = head_width // 2
    frequency = ROPE_BASE ** (-(jnp.arange(half_width, dtype=jnp.float32) * 2.0) / head_width)
    angles = positions.astype(jnp.float32)[:, None] * frequency[None, :]
    angles = jnp.concatenate([angles, angles], axis=1)
    return (jnp.cos(angles), jnp.sin(angles))


def rotate(values, cosine_table, sine_table):
    half_width = values.shape[-1] // 2
    turned = jnp.concatenate([-values[..., half_width:], values[..., :half_width]], axis=-1)
    return values * cosine_table[:, None, :] + turned * sine_table[:, None, :]


def join_pair(mine_cols, partner, is_lower):
    return jnp.where(
        is_lower,
        jnp.concatenate([mine_cols, partner], axis=1),
        jnp.concatenate([partner, mine_cols], axis=1),
    )


def per_device(
    residual_in,
    norm_gain,
    w_query,
    w_key_value,
    query_bias,
    key_value_bias,
    w_output,
    device_map,
    positions,
    segments,
):
    tp_count = lax.axis_size("tp")
    tp_index = lax.axis_index("tp")
    blk_index = lax.axis_index("blk")
    local_tokens = residual_in.shape[0]
    shard_rows = w_query.shape[0]
    kv_group = tp_count // KVH
    floats = residual_in.astype(jnp.float32)
    square = jnp.maximum(jnp.mean(floats * floats, axis=1, keepdims=True), NORM_FLOOR)
    normed = (floats * lax.rsqrt(square) * norm_gain.astype(jnp.float32)).astype(jnp.bfloat16)
    ordered = jnp.take(
        normed.reshape(local_tokens, device_map.shape[0], shard_rows), device_map, axis=1
    ).reshape(local_tokens, D)
    moved_query, moved_pairs = (
        lax.all_to_all(w_query, "tp", split_axis=1, concat_axis=0, tiled=True),
        lax.all_to_all(w_key_value, "tp", split_axis=1, concat_axis=0, tiled=True),
    )
    for bit_level in range(kv_group.bit_length() - 1):
        partner = from_partner(for_sending(moved_pairs), "tp", bit_level).astype(moved_pairs.dtype)
        moved_pairs = join_pair(moved_pairs, partner, tp_index >> bit_level & 1 == 0)
    queries = jnp.dot(
        ordered,
        lax.all_gather(moved_query, "blk", axis=0, tiled=True),
        preferred_element_type=jnp.float32,
    )
    key_value = jnp.dot(
        ordered,
        lax.all_gather(moved_pairs, "blk", axis=0, tiled=True),
        preferred_element_type=jnp.float32,
    )
    query_width = queries.shape[1]
    heads_here = query_width // HD
    kv_head = tp_index // kv_group
    queries = queries + lax.dynamic_slice_in_dim(
        query_bias, tp_index * query_width, query_width
    ).astype(jnp.float32)
    key_value = key_value + lax.dynamic_slice_in_dim(
        key_value_bias, kv_head * 2 * HD, 2 * HD
    ).astype(jnp.float32)
    cosine_table, sine_table = rope_tables(positions, HD)
    query_rot = rotate(
        queries.reshape(local_tokens, heads_here, HD), cosine_table, sine_table
    ).astype(jnp.bfloat16)
    key_rot = rotate(key_value[:, None, :HD], cosine_table, sine_table)[:, 0, :].astype(
        jnp.bfloat16
    )
    values = key_value[:, HD:].astype(jnp.bfloat16)
    attend_scale = HD ** (-0.5)
    row_index = blk_index * local_tokens + jnp.arange(local_tokens, dtype=jnp.int32)
    initial = (
        jnp.full((heads_here, local_tokens), NEGATIVE_FILL, jnp.float32),
        jnp.zeros((heads_here, local_tokens), jnp.float32),
        jnp.zeros((heads_here, local_tokens, HD), jnp.float32),
    )
    key_piece = lax.all_gather(key_rot, "blk", axis=0, tiled=True)
    value_piece = lax.all_gather(values, "blk", axis=0, tiled=True)
    segment_piece = lax.all_gather(segments, "blk", axis=0, tiled=True)
    piece_rows = key_piece.shape[0]
    key_block_rows = 512

    def one_block(block_number, state_now):
        run_peak, run_mass, context = state_now
        block_start = block_number * key_block_rows
        key_block = lax.dynamic_slice_in_dim(key_piece, block_start, key_block_rows, 0)
        value_block = lax.dynamic_slice_in_dim(value_piece, block_start, key_block_rows, 0)
        segment_block = lax.dynamic_slice_in_dim(segment_piece, block_start, key_block_rows, 0)
        scores = (
            jnp.einsum("qhd,kd->hqk", query_rot, key_block, preferred_element_type=jnp.float32)
            * attend_scale
        )
        key_index = block_start + jnp.arange(key_block_rows, dtype=jnp.int32)
        visible = (key_index[None, :] <= row_index[:, None]) & (
            segment_block[None, :] == segments[:, None]
        )
        masked = jnp.where(visible[None], scores, NEGATIVE_FILL)
        new_peak = jnp.maximum(run_peak, jnp.max(masked, axis=2))
        factor = jnp.exp(run_peak - new_peak)
        raw_weights = jnp.where(visible[None], jnp.exp(masked - new_peak[:, :, None]), 0.0)
        run_mass = run_mass * factor + jnp.sum(raw_weights, axis=2)
        context = context * factor[:, :, None] + jnp.einsum(
            "hqk,kd->hqd",
            raw_weights.astype(jnp.bfloat16),
            value_block,
            preferred_element_type=jnp.float32,
        )
        return (new_peak, run_mass, context)

    run_peak, run_mass, context = lax.fori_loop(0, piece_rows // key_block_rows, one_block, initial)
    context_flat = (
        (context / run_mass[:, :, None])
        .transpose(1, 0, 2)
        .reshape(local_tokens, query_width)
        .astype(jnp.bfloat16)
    )
    width_out = D // tp_count
    moved_out = lax.all_to_all(w_output, "tp", split_axis=0, concat_axis=1, tiled=True)
    row_terms = jnp.dot(
        context_flat,
        lax.all_gather(moved_out, "blk", axis=1, tiled=True),
        preferred_element_type=jnp.float32,
    )
    summed = lax.psum_scatter(
        row_terms.astype(jnp.bfloat16), "tp", scatter_dimension=1, tiled=True
    ).astype(jnp.float32)
    residual_part = lax.dynamic_slice_in_dim(residual_in, tp_index * width_out, width_out, 1)
    return (residual_part.astype(jnp.float32) + summed).astype(jnp.bfloat16)


MESH = pl.DeviceIdType.MESH
BF = jnp.bfloat16
F32 = jnp.float32


def flip(i, mask):
    out = i
    for bit in range(mask.bit_length()):
        if mask >> bit & 1:
            out = out + (1 << bit) * (1 - 2 * ((i // (1 << bit)) % 2))
    return out


def fused_kernel(nb, nt, dm_ref, x_hbm, wq_hbm, wkv_hbm, gain_ref, bq_ref, bkv_ref, wo_hbm, inv_ref,
                 pos_ref, seg_ref, out_ref, x_ref, xo, gq, gkv, wo, kv_all, seg_all, qacc,
                 kvacc, qrot, ctx_all, oacc, gain32, bq32, bkv32, cos_t, sin_t, segq_ref,
                 masks, psend, prec, pss, prs,
                 x_sem, loc_sem, kv1s, kv1r, kvxs, kvxr, kvcs, kvcr, q1s, q1r, qxs, qxr, qcs, qcr,
                 w1s, w1r, wxs, wxr, wcs, wcr, es, er, gs, gr, azs, azr, ays, ayr, wrel, rs, rr, r2s):
    b = lax.axis_index("blk")
    t = lax.axis_index("tp")
    n_tok, width = x_ref.shape
    rows = wq_hbm.shape[0]
    qc, kc = gq.shape[2], gkv.shape[2]
    oc = wo.shape[1]
    bx, bc = flip(b, 2), flip(b, 1)

    barrier = pltpu.get_barrier_semaphore()
    peers = [(b, flip(t, k)) for k in range(1, nt)] + [(flip(b, k), t) for k in range(1, nb)]
    peers += [(bx, flip(t, 1))]
    for peer in peers:
        pl.semaphore_signal(barrier, inc=1, device_id=peer, device_id_type=MESH)
    x_in = pltpu.make_async_copy(x_hbm, x_ref, x_sem)
    x_in.start()
    gain32[...] = gain_ref[...].astype(F32)
    bq32[...] = bq_ref[...].astype(F32)
    bkv32[...] = bkv_ref[...].astype(F32)
    with jax.named_scope("barrier"):
        pl.semaphore_wait(barrier, len(peers))

    def remote(src, dst, ss, rs, dev):
        return pltpu.make_async_remote_copy(src_ref=src, dst_ref=dst, send_sem=ss, recv_sem=rs,
                                            device_id=dev, device_id_type=MESH)

    def slot(bb, k):
        return bb * nt + flip(t, k)

    def stage_one(hbm, buf, width, k, ss, rs, local):
        cols = pl.ds(pl.multiple_of(flip(t, k) * width, 128), width)
        mine = buf.at[b * nt + t]
        if k == 0:
            return pltpu.make_async_copy(hbm.at[:, cols], mine, local)
        return remote(hbm.at[:, cols], mine, ss.at[k], rs.at[k], (b, flip(t, k)))

    def stage_one_in(buf, hbm, width, k, ss, rs, local):
        if k == 0:
            return stage_one(hbm, buf, width, 0, ss, rs, local)
        piece = buf.at[slot(b, k)]
        return remote(piece, piece, ss.at[k], rs.at[k], (b, flip(t, k)))

    def forward(buf, bb, k, ss, rs, i, dev):
        piece = buf.at[slot(bb, k)]
        return remote(piece, piece, ss.at[i], rs.at[i], dev)

    kv_set = (wkv_hbm, gkv, kc, kv1s, kv1r, kvxs, kvxr, kvcs, kvcr, loc_sem.at[0])
    q_set = (wq_hbm, gq, qc, q1s, q1r, qxs, qxr, qcs, qcr, loc_sem.at[1])

    order = [0, 1, 2, 4, 3, 6, 5, 7]

    def across(ws, k):
        hbm, buf, width, s1, r1, xs, xr, cs, cr, loc = ws
        cols = pl.ds(pl.multiple_of(flip(t, k) * width, 128), width)
        return remote(hbm.at[:, cols], buf.at[b * nt + t], xs.at[k], xr.at[k], (bx, flip(t, k)))

    def start_one(ws, k):
        hbm, buf, width, s1, r1, xs, xr, cs, cr, loc = ws
        stage_one(hbm, buf, width, k, s1, r1, loc).start()
        if k < 2:
            across(ws, k).start()

    def gather_step(ws, i):
        k = order[i]
        hbm, buf, width, s1, r1, xs, xr, cs, cr, loc = ws
        arrived = stage_one_in(buf, hbm, width, k, s1, r1, loc)
        if k == 0:
            arrived.wait()
        else:
            arrived.wait_recv()
        if k > 1:
            forward(buf, b, k, xs, xr, k, (bx, t)).start()
        forward(buf, b, k, cs, cr, k, (bc, t)).start()

    def gather_cross(ws, i):
        k = order[i]
        hbm, buf, width, s1, r1, xs, xr, cs, cr, loc = ws
        forward(buf, bx, k, xs, xr, k, (bx, t)).wait_recv()
        forward(buf, bx, k, cs, cr, nt + k, (bc, t)).start()

    def gather_last(ws, i):
        k = order[i]
        hbm, buf, width, s1, r1, xs, xr, cs, cr, loc = ws
        forward(buf, bc, k, cs, cr, k, (bc, t)).wait_recv()
        forward(buf, flip(b, 3), k, cs, cr, nt + k, (bc, t)).wait_recv()

    def gather_sent(ws):
        hbm, buf, width, s1, r1, xs, xr, cs, cr, loc = ws
        for k in range(nt):
            if k:
                stage_one(hbm, buf, width, k, s1, r1, loc).wait_send()
            if k < 2:
                across(ws, k).wait_send()
            else:
                forward(buf, b, k, xs, xr, k, (bx, t)).wait_send()
            forward(buf, b, k, cs, cr, k, (bc, t)).wait_send()
            forward(buf, bx, k, cs, cr, nt + k, (bc, t)).wait_send()

    def multiply(buf, acc, i):
        k = order[i]

        def one(j, _):
            s = slot(j, k)
            acc[...] += jnp.dot(xo[dm_ref[s]], buf[s], preferred_element_type=F32)
            return 0
        lax.fori_loop(0, nb, one, 0)

    issue = [0,2,4,1,6,3,5,7]
    for k in issue:
        start_one(kv_set, k)

    x_in.wait()
    tile = n_tok // nt

    def norm_tile(i):
        toks = slice(i * tile, (i + 1) * tile)
        v = x_ref[toks, :].astype(F32)
        scale = lax.rsqrt(jnp.maximum(jnp.mean(v * v, axis=1, keepdims=True), NORM_FLOOR))

        def spread(g, _):
            per = 4 * rows // 128
            gain = jnp.concatenate([gain32[pl.ds(g * per + i, 1), :] for i in range(per)], axis=1)
            u = x_ref[toks, pl.ds(pl.multiple_of(g * 4 * rows, 128), 4 * rows)].astype(F32)
            u = (u * scale * gain).astype(BF)
            for i in range(4):
                xo[g * 4 + i, toks, :] = u[:, i * rows:(i + 1) * rows]
            return 0

        lax.fori_loop(0, nb * nt // 4, spread, 0)

    def tables():
        pos = jnp.broadcast_to(pos_ref[...].astype(F32), (HD, n_tok)).T
        angles = pos * inv_ref[...]
        cos_t[...] = jnp.cos(angles)
        sign = jnp.where(lax.broadcasted_iota(jnp.int32, (1, HD), 1) < HD // 2, -1.0, 1.0)
        sin_t[...] = jnp.sin(angles) * sign
        segq_ref[...] = jnp.broadcast_to(seg_ref[...].astype(F32), (HD, n_tok)).T[:, :1].astype(jnp.int32)

    zi, yy = t // (nt // 2), t % 2
    k_mine = t % nb
    even_core = b % 2

    def wsrc(c, i):
        return wo_hbm.at[:, pl.ds(pl.multiple_of((c * 2 + i) * qc, 128), qc)]

    def wpiece(slot, k, i):
        return wo.at[slot, pl.ds(pl.multiple_of(k * rows, 16), rows), i * qc:(i + 1) * qc]

    def mine_or_next(side, owner):
        col = owner * 2 + t // nb
        return (even_core, col) if side == 0 else (1 - even_core, flip(col, 2))

    def straight(side, i):
        c, dest = mine_or_next(side, b)
        return dest, wsrc(c, i), wpiece(even_core, k_mine, i), w1s.at[side, i], w1r.at[k_mine, i]

    def to_relay(side, i):
        c, _ = mine_or_next(side, bx)
        return remote(wsrc(2 + c, i), wrel.at[side, i], rs.at[side, i], rr.at[side, i], (bx, t))

    def from_relay(side, i):
        _, dest = mine_or_next(side, bx)
        return dest, wrel.at[side, i], wpiece(2 + even_core, k_mine, i), r2s.at[side, i], w1r.at[k_mine, i]

    def deliver(what):
        dest, src, dst, ss, sr = what

        @pl.when(dest != t)
        def _():
            remote(src, dst, ss, sr, (b, dest)).start()

        @pl.when(dest == t)
        def _():
            pltpu.make_async_copy(src, dst, sr).start()

    def delivered(what):
        dest, src, dst, ss, sr = what

        @pl.when(dest != t)
        def _():
            remote(src, dst, ss, sr, (b, dest)).wait_send()

    def whalf(bb, k, i):
        return wpiece(2 * ((bb // 2 + zi) % 2) + bb % 2, k, i)

    def w_x(bb, k, i):
        return remote(whalf(bb, k, i), whalf(bb, k, i), wxs.at[k, i], wxr.at[k, i], (bx, t))

    def w_c(bb, u, k, i):
        return remote(whalf(bb, k, i), whalf(bb, k, i), wcs.at[u, k, i], wcr.at[u, k, i], (bc, t))

    def w_home(k, i):
        remote(whalf(b, k, i), whalf(b, k, i), w1s.at[0, i], w1r.at[k, i], (bx, t)).wait_recv()
        w_x(b, k, i).start()
        w_c(b, 0, k, i).start()

    def w_cross(k, i):
        w_x(bx, k, i).wait_recv()
        w_c(bx, 1, k, i).start()

    def w_last(k, i):
        w_c(bc, 0, k, i).wait_recv()
        w_c(flip(b, 3), 1, k, i).wait_recv()

    def w_straight(side):
        for i in range(2):
            deliver(straight(side, i))

    def w_start(side):
        for i in range(2):
            to_relay(side, i).start()

    def w_relay(side, i):
        to_relay(side, i).wait_recv()
        deliver(from_relay(side, i))

    def relays(side):
        for i in range(2):
            with jax.named_scope(f"wrelay{i}{side}"):
                w_relay(side, i)

    for k in range(nt):
        with jax.named_scope(f"norm{k}"):
            norm_tile(k)
        with jax.named_scope(f"kvstep{k}"):
            gather_step(kv_set, k)
        if k >= 1:
            start_one(q_set, issue[k - 1])
        if k == 4:
            w_start(1)
        if k == 6:
            w_start(0)
        if k:
            with jax.named_scope(f"kvcross{k}"):
                gather_cross(kv_set, k - 1)
    for k in range(nt - 1, nt):
        start_one(q_set, issue[k])
    with jax.named_scope("tables"):
        tables()
    with jax.named_scope("kvcross8"):
        gather_cross(kv_set, nt - 1)

    for e in range(2):
        kvacc[:, e * HD:(e + 1) * HD] = jnp.broadcast_to(bkv32[pl.ds(t * 2 + e, 1), :], (n_tok, HD))
    for k in range(4):
        with jax.named_scope(f"qstep{k}"):
            gather_step(q_set, k)
        if k:
            with jax.named_scope(f"qcross{k}"):
                gather_cross(q_set, k - 1)
    for e in range(qc // HD):
        qacc[:, e * HD:(e + 1) * HD] = jnp.broadcast_to(
            bq32[pl.ds(t * (qc // HD) + e, 1), :], (n_tok, HD))
    for e in range(nt):
        gather_last(kv_set, e)
        with jax.named_scope(f"kvmul{e}"):
            multiply(gkv, kvacc, e)
        if e % 2 and 4 + e // 2 < nt:
            k = 4 + e // 2
            with jax.named_scope(f"qstep{k}"):
                gather_step(q_set, k)
            with jax.named_scope(f"qcross{k}"):
                gather_cross(q_set, k - 1)
            if k == 4:
                w_straight(1)
            if k == 5:
                w_straight(0)
            if k == 4:
                relays(1)
            if k == 6:
                relays(0)
            if e > 1:
                gather_last(q_set, e // 2 - 1)
                multiply(gq, qacc, e // 2 - 1)

    def rope(u):
        return u * cos_t[...] + pltpu.roll(u, HD // 2, 1) * sin_t[...]

    kv_all[b, :, :HD] = rope(kvacc[:, :HD]).astype(BF)
    kv_all[b, :, HD:] = kvacc[:, HD:].astype(BF)
    seg_all[b] = seg_ref[...]

    def keys(slot_b, sem, dev):
        return (remote(kv_all.at[slot_b], kv_all.at[slot_b], es.at[sem], er.at[sem], dev),
                remote(seg_all.at[slot_b], seg_all.at[slot_b], gs.at[sem], gr.at[sem], dev))

    low = b < nb // 2
    even = b % 2 == 0

    @pl.when(low)
    def _():
        for c in keys(b, 0, (bx, t)):
            c.start()

    @pl.when(even)
    def _():
        for c in keys(b, 1, (bc, t)):
            c.start()

    for k in range(8, nt):
        with jax.named_scope(f"qstep{k}"):
            gather_step(q_set, k)
        with jax.named_scope(f"qcross{k}"):
            gather_cross(q_set, k - 1)
    for e in range(nt // 2 - 1, nt):
        if e == nt - 3:
            with jax.named_scope("qcross8"):
                gather_cross(q_set, nt - 1)
        with jax.named_scope(f"qlast{e}"):
            gather_last(q_set, e)
        with jax.named_scope(f"qmul{e}"):
            multiply(gq, qacc, e)

    n_part = ctx_all.shape[1]
    qrows = n_tok // n_part
    for h in range(qc // HD):
        turned = rope(qacc[:, h * HD:(h + 1) * HD]).astype(BF)
        for part in range(n_part):
            qrot[part, h * qrows:(h + 1) * qrows, :] = turned[part * qrows:(part + 1) * qrows, :]

    @pl.when(b >= nb // 2)
    def _():
        for c in keys(bx, 0, (bx, t)):
            c.wait_recv()
        for c in keys(bx, 2, (bc, t)):
            c.start()
        for c in keys(flip(b, 3), 2, (bc, t)):
            c.wait_recv()

    @pl.when(b % 2 == 1)
    def _():
        for c in keys(bc, 1, (bc, t)):
            c.wait_recv()

    scale = HD ** (-0.5) * LOG2E
    across_qk = (((1,), (1,)), ((), ()))

    def mask_part(part):
        r0 = part * qrows
        sq = segq_ref[r0:r0 + qrows, :]
        seen = r0 + qrows
        ri = r0 + lax.broadcasted_iota(jnp.int32, (qrows, seen), 0)
        ci = lax.broadcasted_iota(jnp.int32, (qrows, seen), 1)
        vis = (ci <= ri) & (seg_all[b][:, :seen] == sq)
        masks[nb - 1, :, :seen] = jnp.where(vis, 0.0, NEGATIVE_FILL)

        def earlier(j, _):
            masks[j] = jnp.where(seg_all[j] == sq, jnp.zeros((qrows, n_tok), F32), NEGATIVE_FILL)
            return 0

        lax.fori_loop(0, b, earlier, 0)

    group = 4

    def attend(g, part):
        seen = (part + 1) * qrows
        rows_here = group * qrows
        qh = qrot[part, g * rows_here:(g + 1) * rows_here, :]

        def scored(kb, mask):
            s = lax.dot_general(qh, kb, across_qk, preferred_element_type=F32) * scale
            return (s.reshape(group, qrows, -1) + mask[None]).reshape(rows_here, -1)

        s = scored(kv_all[b, :seen, :HD], masks[nb - 1, :, :seen])
        m = jnp.max(s, axis=1, keepdims=True)
        p = jnp.exp2(s - m)
        l = jnp.sum(p, axis=1, keepdims=True)
        c = jnp.dot(p.astype(BF), kv_all[b, :seen, HD:], preferred_element_type=F32)

        def block(j, st):
            m, l, c = st
            s = scored(kv_all[j, :, :HD], masks[j])
            m2 = jnp.maximum(m, jnp.max(s, axis=1, keepdims=True))
            f = jnp.exp2(m - m2)
            p = jnp.exp2(s - m2)
            l = l * f + jnp.sum(p, axis=1, keepdims=True)
            c = c * f + jnp.dot(p.astype(BF), kv_all[j, :, HD:], preferred_element_type=F32)
            return (m2, l, c)

        m, l, c = lax.fori_loop(0, b, block, (m, l, c))
        return (c / l).astype(BF)

    def cpiece(z_half, y_side, part):
        return ctx_all.at[z_half, part, :, pl.ds(pl.multiple_of(y_side * qc, 128), qc)]

    def az(z_half, part):
        piece = cpiece(z_half, yy, part)
        return remote(piece, piece, azs.at[part], azr.at[part], (b, flip(t, nt // 2)))

    def ay(z_half, y_side, part, i):
        piece = cpiece(z_half, y_side, part)
        return remote(piece, piece, ays.at[part, i], ayr.at[part, i], (b, flip(t, 1)))

    def relay_ctx(part):
        az(1 - zi, part).wait_recv()
        ay(1 - zi, yy, part, 1).start()

    def partial(part, slot_side):
        acc = None
        for zh in range(2):
            one = lax.dot_general(ctx_all[zh, part], wo[2 * zh + slot_side], across_qk,
                                  preferred_element_type=F32)
            acc = one if acc is None else acc + one
        return acc

    z_low = (t // 2) % 2

    def pcopy(part):
        return remote(psend.at[part], prec.at[part], pss.at[part], prs.at[part], (b, flip(t, 2)))

    def homes(i):
        for k in range(nb):
            with jax.named_scope(f"whome{i}{k}"):
                w_home(flip(k_mine, k), i)

    def crosses(i):
        for k in range(nb):
            with jax.named_scope(f"wcross{i}{k}"):
                w_cross(flip(k_mine, k), i)

    def heads(part, g):
        with jax.named_scope(f"att{part}{g}"):
            both = attend(g, part)
            for e in range(group):
                col = pl.ds(pl.multiple_of(yy * qc + (g * group + e) * HD, 128), HD)
                ctx_all[zi, part, :, col] = both[e * qrows:(e + 1) * qrows, :]

    def send_ctx(part):
        az(zi, part).start()
        ay(zi, yy, part, 0).start()

    next_first = even_core != z_low

    def on(which, *steps):
        @pl.when(which)
        def _():
            for step in steps:
                step()

    def attention(part):
        mask_part(part)
        for g in range(qc // HD // group):
            heads(part, g)
        send_ctx(part)

    def last():
        with jax.named_scope("wlast"):
            for i in range(2):
                for k in range(nb):
                    w_last(flip(k_mine, k), i)

    def next_part(part):
        with jax.named_scope(f"ctxy{part}"):
            ay(zi, 1 - yy, part, 0).wait_recv()
            ay(1 - zi, 1 - yy, part, 1).wait_recv()
        with jax.named_scope(f"next{part}"):
            psend[part] = partial(part, 1 - z_low).astype(BF)
        pcopy(part).start()

    def own_part(part):
        toks = slice(part * qrows, (part + 1) * qrows)
        resid = x_ref[toks, pl.ds(pl.multiple_of(t * oc, 128), oc)].astype(F32)
        with jax.named_scope(f"own{part}"):
            oacc[toks, :] = resid + partial(part, z_low)

    def ctx_turn(part):
        with jax.named_scope(f"ctxrelay{part}"):
            relay_ctx(part)

    own_first = even_core == z_low
    middle = n_part // 2
    on(next_first, lambda: homes(0))
    for part in range(middle):
        attention(part)
    on(next_first, lambda: homes(1))
    for part in range(middle, n_part):
        attention(part)
    near = yy == zi
    on(own_first, lambda: homes(0))
    on(own_first & near, lambda: homes(1))
    for part in range(middle):
        ctx_turn(part)
    on(own_first & (yy != zi), lambda: homes(1))
    on(next_first, lambda: crosses(0), lambda: crosses(1))
    on(own_first, last)
    for part in range(middle, n_part):
        next_part(part - middle)
        if part - middle == 1:
            on(own_first & near, lambda: crosses(0), lambda: crosses(1))
        ctx_turn(part)
    for part in range(n_part - middle, n_part - 1):
        next_part(part)
    on(own_first & (yy != zi), lambda: crosses(0), lambda: crosses(1))
    next_part(n_part - 1)
    on(next_first, last)
    for part in range(n_part):
        own_part(part)
    for part in range(n_part):
        with jax.named_scope(f"prec{part}"):
            pcopy(part).wait_recv()
        toks = slice(part * qrows, (part + 1) * qrows)
        out_ref[toks, :] = (oacc[toks, :] + prec[part].astype(F32)).astype(BF)

    gather_sent(kv_set)
    gather_sent(q_set)

    @pl.when(low)
    def _():
        for c in keys(b, 0, (bx, t)):
            c.wait_send()

    @pl.when(even)
    def _():
        for c in keys(b, 1, (bc, t)):
            c.wait_send()

    @pl.when(b >= nb // 2)
    def _():
        for c in keys(bx, 2, (bc, t)):
            c.wait_send()

    for i in range(2):
        for side in range(2):
            to_relay(side, i).wait_send()
            delivered(straight(side, i))
            delivered(from_relay(side, i))
        for k in range(nb):
            w_x(b, k, i).wait_send()
            w_c(b, 0, k, i).wait_send()
            w_c(bx, 1, k, i).wait_send()
    for part in range(n_part):
        az(zi, part).wait_send()
        ay(zi, yy, part, 0).wait_send()
        ay(1 - zi, yy, part, 1).wait_send()
        pcopy(part).wait_send()


def fused(nb, nt, residual_in, norm_gain, w_query, w_key_value, query_bias, key_value_bias, w_output,
          device_map, positions, segments):
    n_tok, width = residual_in.shape
    rows = w_query.shape[0]
    qc, kc, oc = w_query.shape[1] // nt, w_key_value.shape[1] // nt, width // nt
    n = nb * nt
    inv = ROPE_BASE ** (-(np.arange(HD // 2, dtype=np.float64) * 2.0) / HD)
    inv = np.concatenate([inv, inv]).astype(np.float32)[None, :]
    any_, vm = pl.BlockSpec(memory_space=pl.ANY), pl.BlockSpec(memory_space=pltpu.VMEM)
    dma = pltpu.SemaphoreType.DMA
    return pl.pallas_call(
        functools.partial(fused_kernel, nb, nt),
        out_shape=jax.ShapeDtypeStruct((n_tok, oc), BF),
        in_specs=[pl.BlockSpec(memory_space=pltpu.SMEM), any_, any_, any_, vm, vm, vm, any_, vm, vm, vm],
        out_specs=vm,
        scratch_shapes=[
            pltpu.VMEM((n_tok, width), BF),
            pltpu.VMEM((n, n_tok, rows), BF),
            pltpu.VMEM((n, rows, qc), BF),
            pltpu.VMEM((n, rows, kc), BF),
            pltpu.VMEM((nb, oc, 2 * qc), BF),
            pltpu.VMEM((nb, n_tok, kc), BF),
            pltpu.VMEM((nb, 1, n_tok), jnp.int32),
            pltpu.VMEM((n_tok, qc), F32),
            pltpu.VMEM((n_tok, kc), F32),
            pltpu.VMEM((PARTS, n_tok // PARTS * (qc // HD), HD), BF),
            pltpu.VMEM((2, PARTS, n_tok // PARTS, 2 * qc), BF),
            pltpu.VMEM((n_tok, oc), F32),
            pltpu.VMEM((width // 128, 128), F32), pltpu.VMEM((qc * nt // HD, HD), F32),
            pltpu.VMEM((kc * nt // HD, HD), F32), pltpu.VMEM((n_tok, HD), F32),
            pltpu.VMEM((n_tok, HD), F32), pltpu.VMEM((n_tok, 1), jnp.int32),
            pltpu.VMEM((nb, n_tok // PARTS, n_tok), F32), pltpu.VMEM((PARTS, n_tok // PARTS, oc), BF),
            pltpu.VMEM((PARTS, n_tok // PARTS, oc), BF), dma((PARTS,)), dma((PARTS,)),
            dma, dma((3,)),
            dma((nt,)), dma((nt,)), dma((nt,)), dma((nt,)), dma((2 * nt,)), dma((2 * nt,)),
            dma((nt,)), dma((nt,)), dma((nt,)), dma((nt,)), dma((2 * nt,)), dma((2 * nt,)),
            dma((2, 2)), dma((nb, 2)), dma((nb, 2)), dma((nb, 2)), dma((2, nb, 2)), dma((2, nb, 2)),
            dma((nb,)), dma((nb,)), dma((nb,)), dma((nb,)),
            dma((PARTS,)), dma((PARTS,)), dma((PARTS, 2)), dma((PARTS, 2)),
            pltpu.VMEM((2, 2, rows, qc), BF), dma((2, 2)), dma((2, 2)), dma((2, 2)),
        ],
        compiler_params=pltpu.CompilerParams(
            collective_id=0, has_side_effects=True, vmem_limit_bytes=63 * 1024 * 1024),
    )(device_map, residual_in, w_query, w_key_value, norm_gain.reshape(-1, 128), query_bias.reshape(-1, HD),
      key_value_bias.reshape(-1, HD), w_output.T, jnp.asarray(inv), positions[None, :], segments[None, :])


def route(shape, *args):
    nb, nt = shape["blk"], shape["tp"]
    n_tok, width = args[0].shape
    rows = args[2].shape[0]
    qc, kc, oc = args[2].shape[1] // nt, args[3].shape[1] // nt, width // nt
    fits = (nb == 4 and nt == KVH and rows % 32 == 0 and rows <= 160 and qc == 4 * HD and kc == 2 * HD
            and oc == nb * rows and oc % 128 == 0 and width % 128 == 0 and n_tok % 256 == 0)
    if fits:
        return fused(nb, nt, *args)
    return per_device(*args)


def solution(mesh):
    in_specs = (
        P("blk", None),
        P(),
        P(("blk", "tp"), None),
        P(("blk", "tp"), None),
        P(),
        P(),
        P(None, ("blk", "tp")),
        P(),
        P("blk"),
        P("blk"),
    )
    out_specs = P("blk", "tp")
    return jax.shard_map(
        functools.partial(route, dict(mesh.shape)), mesh=mesh, in_specs=in_specs, out_specs=out_specs, check_vma=False
    )
```
